8 devices in a mesh: dp: 1 (over z), tp: 2 (over y), sp: 4 (over x, core).
Axes of the slice: x: 2, y: 2, z: 1, core: 2. Of those that a mesh axis runs over, the one named last changes fastest.
Arguments:
- hidden: bfloat16 [256, 6144], P('dp')
- norm_w: bfloat16 [6144], replicated
- w_q: bfloat16 [6144, 6144], P(None, 'tp')
- b_q: bfloat16 [6144], P('tp')
- w_k: bfloat16 [6144, 256], P(None, 'tp')
- b_k: bfloat16 [256], P('tp')
- w_v: bfloat16 [6144, 256], P(None, 'tp')
- b_v: bfloat16 [256], P('tp')
- w_o: bfloat16 [6144, 6144], P('tp')
- k_cache: bfloat16 [256, 2048, 2, 128], P('dp', 'sp', 'tp')
- v_cache: bfloat16 [256, 2048, 2, 128], P('dp', 'sp', 'tp')
- positions: int32 [256], P('dp')
- seq_lens: int32 [256], P('dp')
Outputs:
- output 1: bfloat16 [256, 6144], P('dp')
- output 2: bfloat16 [256, 2, 128], P('dp', 'tp')
- output 3: bfloat16 [256, 2, 128], P('dp', 'tp')
All inputs are finite; a program needn't handle non-finite values.
Results may differ from the reference program's by a relative error of at most 0.00769785.
Values sent between devices are 32-bit elements.
A program may use at most 1 GiB of HBM per device.

```python
import jax
import jax.numpy as jnp
from jax import lax

BATCH = 256
SEQ_LEN = 2048
D_MODEL = 6144
N_HEADS = 48
KV_GROUPS = 2
HEAD_DIM = 128
ROT_DIM = HEAD_DIM // 2
PER_GROUP = N_HEADS // KV_GROUPS
Q_COLS = N_HEADS * HEAD_DIM
KV_COLS = KV_GROUPS * HEAD_DIM
RMS_EPS = 1.5625e-7
ROPE_BASE = 10000.0


def normal_draw(key, shape, std):
    return std * jax.random.normal(key, shape, jnp.float32)


def setup_inputs(seed: int = 0, part: int = 0) -> dict:
    shared_keys = jax.random.split(jax.random.key(seed), 8)
    part_keys = jax.random.split(jax.random.fold_in(jax.random.key(seed + 1), part), 5)
    val_scale = (SEQ_LEN ** 0.5) / 4.0
    cache_shape = (BATCH, SEQ_LEN, KV_GROUPS, HEAD_DIM)
    seq_lens = jax.random.randint(part_keys[3], (BATCH,), SEQ_LEN // 8, SEQ_LEN + 1, dtype=jnp.int32)
    seq_lens = seq_lens.at[0].set(SEQ_LEN).at[1].set(SEQ_LEN // 8)
    positions = seq_lens + jax.random.randint(part_keys[4], (BATCH,), 0, SEQ_LEN + 1, dtype=jnp.int32)
    return {
        'hidden': normal_draw(part_keys[0], (BATCH, D_MODEL), 1.0).astype(jnp.bfloat16),
        'norm_w': (1.0 + normal_draw(shared_keys[0], (D_MODEL,), 0.3)).astype(jnp.bfloat16),
        'w_q': normal_draw(shared_keys[1], (D_MODEL, Q_COLS), D_MODEL ** -0.5).astype(jnp.bfloat16),
        'b_q': normal_draw(shared_keys[2], (Q_COLS,), 0.5).astype(jnp.bfloat16),
        'w_k': normal_draw(shared_keys[3], (D_MODEL, KV_COLS), D_MODEL ** -0.5).astype(jnp.bfloat16),
        'b_k': normal_draw(shared_keys[4], (KV_COLS,), 0.5).astype(jnp.bfloat16),
        'w_v': normal_draw(shared_keys[5], (D_MODEL, KV_COLS), D_MODEL ** -0.5).astype(jnp.bfloat16),
        'b_v': normal_draw(shared_keys[6], (KV_COLS,), 0.5).astype(jnp.bfloat16),
        'w_o': normal_draw(shared_keys[7], (Q_COLS, D_MODEL), Q_COLS ** -0.5).astype(jnp.bfloat16),
        'k_cache': normal_draw(part_keys[1], cache_shape, 1.4).astype(jnp.bfloat16),
        'v_cache': normal_draw(part_keys[2], cache_shape, val_scale).astype(jnp.bfloat16),
        'positions': positions,
        'seq_lens': seq_lens,
    }


def apply_rotary(heads_in, positions):
    half_rot = ROT_DIM // 2
    inv_freq = ROPE_BASE ** (-2.0 * jnp.arange(half_rot, dtype=jnp.float32) / ROT_DIM)
    angles = positions.astype(jnp.float32)[:, None, None] * inv_freq
    cos_t = jnp.cos(angles)
    sin_t = jnp.sin(angles)
    rot_pairs = heads_in[..., :ROT_DIM].astype(jnp.float32).reshape(heads_in.shape[:-1] + (half_rot, 2))
    even_part = rot_pairs[..., 0]
    odd_part = rot_pairs[..., 1]
    rotated = jnp.stack([even_part * cos_t - odd_part * sin_t, even_part * sin_t + odd_part * cos_t], axis=-1)
    rotated = rotated.reshape(heads_in.shape[:-1] + (ROT_DIM,)).astype(jnp.bfloat16)
    return jnp.concatenate([rotated, heads_in[..., ROT_DIM:]], axis=-1)


def project(normed, weight, bias_vec):
    return (jnp.dot(normed, weight, preferred_element_type=jnp.float32) + bias_vec.astype(jnp.float32)).astype(jnp.bfloat16)


def reference(hidden, norm_w, w_q, b_q, w_k, b_k, w_v, b_v, w_o, k_cache, v_cache, positions, seq_lens):
    x_f32 = hidden.astype(jnp.float32)
    mean_sq = jnp.mean(x_f32 * x_f32, axis=-1, keepdims=True)
    normed = (x_f32 * lax.rsqrt(mean_sq + RMS_EPS) * norm_w.astype(jnp.float32)).astype(jnp.bfloat16)
    q_rot = apply_rotary(project(normed, w_q, b_q).reshape(BATCH, N_HEADS, HEAD_DIM), positions)
    k_rot = apply_rotary(project(normed, w_k, b_k).reshape(BATCH, KV_GROUPS, HEAD_DIM), positions)
    v_new = project(normed, w_v, b_v).reshape(BATCH, KV_GROUPS, HEAD_DIM)
    attn_scale = HEAD_DIM ** -0.5
    cache_idx = jnp.arange(SEQ_LEN)

    def one_row(row_args):
        q_row, k_row, v_row, k_tok, v_tok, length = row_args
        q_grp = q_row.reshape(KV_GROUPS, PER_GROUP, HEAD_DIM).astype(jnp.float32)
        s_cache = jnp.einsum('gqd,sgd->gqs', q_grp, k_row.astype(jnp.float32)) * attn_scale
        s_cache = jnp.where((cache_idx < length)[None, None, :], s_cache, -jnp.inf)
        s_new = jnp.einsum('gqd,gd->gq', q_grp, k_tok.astype(jnp.float32)) * attn_scale
        m_top = jnp.maximum(jnp.max(s_cache, axis=-1), s_new)
        p_cache = jnp.exp(s_cache - m_top[..., None])
        p_new = jnp.exp(s_new - m_top)
        exp_sum = jnp.sum(p_cache, axis=-1) + p_new
        weighted = jnp.einsum('gqs,sgd->gqd', p_cache, v_row.astype(jnp.float32))
        weighted = weighted + p_new[..., None] * v_tok.astype(jnp.float32)[:, None, :]
        return (weighted / exp_sum[..., None]).reshape(Q_COLS).astype(jnp.bfloat16)

    attn_rows = lax.map(one_row, (q_rot, k_cache, v_cache, k_rot, v_new, seq_lens))
    y_out = (x_f32 + jnp.dot(attn_rows, w_o, preferred_element_type=jnp.float32)).astype(jnp.bfloat16)
    return y_out, k_rot, v_new
```

```python
import functools

import jax
import jax.numpy as jnp
from jax import lax
from jax.experimental import pallas as pl
from jax.experimental.pallas import tpu as pltpu
from jax.sharding import PartitionSpec as P

RMS_EPS = 1.5625e-7
ROPE_BASE = 10000.0
LOG2E = 1.4426950408889634
NEG = -3e38
NEG_FLOOR = -1e38
MESH = pl.DeviceIdType.MESH
VMEM_LIMIT = 67_043_328

NC = 2
BR = 8
NB = 4
TN = 512


def rope_tables(positions, head_dim):
    rot_dim = head_dim // 2
    lane = jnp.arange(head_dim, dtype=jnp.int32)
    freq = ROPE_BASE ** (-2.0 * (lane // 2).astype(jnp.float32) / rot_dim)
    freq = jnp.where(lane < rot_dim, freq, 0.0)
    angles = positions.astype(jnp.float32)[:, None] * freq
    sign = jnp.where(lane % 2 == 0, -1.0, 1.0)
    return jnp.cos(angles), jnp.sin(angles) * sign


def rope(x, cos_t, sin_t, even):
    width = x.shape[-1]
    swapped = jnp.where(even, pltpu.roll(x, width - 1, 1), pltpu.roll(x, 1, 1))
    return (x * cos_t + swapped * sin_t).astype(jnp.bfloat16).astype(jnp.float32)


def qkv_kernel(heads, n_tiles, hid_ref, nw_ref, wq_ref, bq_ref, wk_ref, bk_ref, wv_ref, bv_ref, cos_ref, sin_ref,
               q_ref, kf_ref, vf_ref, kb_ref, vb_ref, normed):
    step = pl.program_id(0)
    n_rows, head_dim = cos_ref.shape

    @pl.when(step == 0)
    def _():
        def norm_rows(i, _):
            rows = pl.ds(pl.multiple_of(i * 32, 32), 32)
            x = hid_ref[rows, :].astype(jnp.float32)
            mean_sq = jnp.mean(x * x, axis=-1, keepdims=True)
            y = x * lax.rsqrt(mean_sq + RMS_EPS) * nw_ref[...].astype(jnp.float32)
            normed[rows, :] = y.astype(jnp.bfloat16)
            return 0
        lax.fori_loop(0, n_rows // 32, norm_rows, 0)

    def even_lanes():
        return lax.broadcasted_iota(jnp.int32, (n_rows, head_dim), 1) % 2 == 0

    def proj(w_ref, b_ref):
        acc = jnp.dot(normed[...], w_ref[...], preferred_element_type=jnp.float32)
        return (acc + b_ref[...].astype(jnp.float32)).astype(jnp.bfloat16).astype(jnp.float32)

    @pl.when(step < n_tiles)
    def _():
        val = proj(wq_ref, bq_ref)
        per_tile = heads // n_tiles
        for h in range(per_tile):
            rot = rope(val[:, h * head_dim:(h + 1) * head_dim], cos_ref[...], sin_ref[...], even_lanes())
            q_ref[pl.ds(step * per_tile + h, n_rows, stride=heads), :] = rot

    @pl.when(step == n_tiles)
    def _():
        k_rot = rope(proj(wk_ref, bk_ref), cos_ref[...], sin_ref[...], even_lanes())
        kf_ref[...] = k_rot
        kb_ref[...] = k_rot.astype(jnp.bfloat16)
        v_new = proj(wv_ref, bv_ref)
        vf_ref[...] = v_new
        vb_ref[...] = v_new.astype(jnp.bfloat16)


def qkv(hidden, norm_w, w_q, b_q, w_k, b_k, w_v, b_v, positions, head_dim):
    n_rows, d_model = hidden.shape
    q_cols = w_q.shape[1]
    heads = q_cols // head_dim
    tile = 512
    n_tiles = q_cols // tile
    cos_t, sin_t = rope_tables(positions, head_dim)

    def whole(shape):
        return pl.BlockSpec(shape, lambda i: (0,) * len(shape))

    return pl.pallas_call(
        functools.partial(qkv_kernel, heads, n_tiles),
        grid=(n_tiles + 1,),
        in_specs=[
            whole((n_rows, d_model)), whole((1, d_model)),
            pl.BlockSpec((d_model, tile), lambda i: (0, jnp.minimum(i, n_tiles - 1))),
            pl.BlockSpec((1, tile), lambda i: (0, jnp.minimum(i, n_tiles - 1))),
            whole((d_model, head_dim)), whole((1, head_dim)), whole((d_model, head_dim)), whole((1, head_dim)),
            whole((n_rows, head_dim)), whole((n_rows, head_dim)),
        ],
        out_specs=[whole((n_rows * heads, head_dim))] + [whole((n_rows, head_dim))] * 4,
        out_shape=[
            jax.ShapeDtypeStruct((n_rows * heads, head_dim), jnp.float32),
            jax.ShapeDtypeStruct((n_rows, head_dim), jnp.float32),
            jax.ShapeDtypeStruct((n_rows, head_dim), jnp.float32),
            jax.ShapeDtypeStruct((n_rows, head_dim), jnp.bfloat16),
            jax.ShapeDtypeStruct((n_rows, head_dim), jnp.bfloat16),
        ],
        scratch_shapes=[pltpu.VMEM((n_rows, d_model), jnp.bfloat16)],
        compiler_params=pltpu.CompilerParams(vmem_limit_bytes=VMEM_LIMIT),
        name="qkv",
    )(hidden, norm_w[None], w_q, b_q[None], w_k, b_k[None], w_v, b_v[None], cos_t, sin_t)


def attn_kernel(seq_ref, q_ref, kf_ref, vf_ref, hid_hbm, k_hbm, v_hbm, wo_hbm, y_ref,
                o_buf, rd, rx, att, lhs, p_buf, p_recv, y_send, y_core, y_chip, y_fwd, wo, hid, kbuf, vbuf,
                k_sem, v_sem, wo_sem, hid_sem, rd_s, rd_r, rx_s, rx_r, at_s, at_r, p_s, p_r,
                yc_s, yc_r, yx_s, yx_r, yf_s, yf_r):
    n_rows, d_model = y_ref.shape
    s_dev, head_dim = kbuf.shape[2], kbuf.shape[3]
    heads = q_ref.shape[0] // n_rows
    half = wo.shape[0] * TN
    n_tiles = wo.shape[0]
    quarter = n_rows // (4 * NC)
    o_rows = quarter * heads
    chip_rows = n_rows // 2
    blk_per_q = quarter // BR
    n_blk = n_rows // BR
    coef = head_dim ** -0.5 * LOG2E

    dp, tp, sp = lax.axis_index("dp"), lax.axis_index("tp"), lax.axis_index("sp")
    chip, core = sp // 2, sp % 2
    to_core = (dp, tp, 2 * chip + (1 - core))
    to_chip = (dp, tp, 2 * (1 - chip) + core)
    to_tp = (dp, 1 - tp, sp)

    def remote(src, dst, s_sem, r_sem, dev):
        return pltpu.make_async_remote_copy(src_ref=src, dst_ref=dst, send_sem=s_sem, recv_sem=r_sem,
                                            device_id=dev, device_id_type=MESH)

    def quarter_row(n, qi):
        far = chip if qi >= 2 else 1 - chip
        owner_core = core if qi % 2 == 1 else 1 - core
        return far * chip_rows + n * 2 * quarter + owner_core * quarter

    def block_row(b):
        n = b // (4 * blk_per_q)
        r = b % (4 * blk_per_q)
        qi = r // blk_per_q
        w = r % blk_per_q
        own_chip = qi // 2
        own_core = qi % 2
        far = own_chip * chip + (1 - own_chip) * (1 - chip)
        o_core = own_core * core + (1 - own_core) * (1 - core)
        return pl.multiple_of(far * chip_rows + n * 2 * quarter + o_core * quarter + w * BR, BR)

    def kv_copies(b):
        slot = b % NB
        rows = pl.ds(block_row(b), BR)
        return (pltpu.make_async_copy(k_hbm.at[rows], kbuf.at[slot], k_sem.at[slot]),
                pltpu.make_async_copy(v_hbm.at[rows], vbuf.at[slot], v_sem.at[slot]))

    def start_kv(b):
        for c in kv_copies(b):
            c.start()

    def wo_copy(t):
        cols = pl.ds(pl.multiple_of(core * half + t * TN, 128), TN)
        return pltpu.make_async_copy(wo_hbm.at[:, cols], wo.at[t], wo_sem.at[t])

    hid_copy = pltpu.make_async_copy(
        hid_hbm.at[pl.ds(pl.multiple_of(chip * chip_rows, 128), chip_rows),
                   pl.ds(pl.multiple_of(core * half, 128), half)], hid, hid_sem)

    for b in range(NB):
        start_kv(b)

    barrier = pltpu.get_barrier_semaphore()
    for dev in (to_core, to_chip, to_tp):
        pl.semaphore_signal(barrier, inc=1, device_id=dev, device_id_type=MESH)
    pl.semaphore_wait(barrier, 3)

    lane = lax.broadcasted_iota(jnp.int32, (heads, head_dim), 1)
    pos = lax.broadcasted_iota(jnp.int32, (heads, s_dev), 1) + sp * s_dev
    is_first = sp == 0
    zeros_q = jnp.zeros((heads, head_dim), jnp.float32)

    def attend_quarter(n, qi):
        slot_o = n * 4 + qi
        base = (n * 4 + qi) * blk_per_q
        row_base = quarter_row(n, qi)

        def block(w, stats):
            m_all, l_all = stats
            b = base + w
            slot = b % NB
            row0 = pl.multiple_of(row_base + w * BR, BR)
            for c in kv_copies(b):
                c.wait()
            k_new = kf_ref[pl.ds(row0, BR), :]
            v_new = vf_ref[pl.ds(row0, BR), :]
            for pair in range(BR // 2):
                r = 2 * pair
                qs = [q_ref[pl.ds(pl.multiple_of((row0 + r + i) * heads, 8), heads), :] for i in range(2)]
                left = jnp.concatenate([qs[0], zeros_q], axis=0)
                right = jnp.concatenate([zeros_q, qs[1]], axis=0)
                q_pair = jnp.concatenate([left, right], axis=1).astype(jnp.bfloat16)
                k_pair = jnp.concatenate([kbuf[slot, r], kbuf[slot, r + 1]], axis=1)
                s_pair = lax.dot_general(q_pair, k_pair, (((1,), (1,)), ((), ())),
                                         preferred_element_type=jnp.float32)
                p_list, pn_list = [], []
                for i in range(2):
                    s = s_pair[i * heads:(i + 1) * heads]
                    s = jnp.where(pos < seq_ref[row0 + r + i], s, NEG)
                    s_new = jnp.sum(qs[i] * k_new[r + i:r + i + 1], axis=-1, keepdims=True)
                    s_new = jnp.where(is_first, s_new, NEG)
                    m = jnp.maximum(jnp.maximum(jnp.max(s, axis=-1, keepdims=True), s_new), NEG_FLOOR)
                    p = jnp.exp2((s - m) * coef)
                    p_new = jnp.exp2((s_new - m) * coef)
                    l = jnp.sum(p, axis=-1, keepdims=True) + p_new
                    here = lane == w * BR + r + i
                    m_all = jnp.where(here, m, m_all)
                    l_all = jnp.where(here, l, l_all)
                    p_list.append(p)
                    pn_list.append(p_new)
                p_pair = jnp.concatenate(p_list, axis=0).astype(jnp.bfloat16)
                v_pair = jnp.concatenate([vbuf[slot, r], vbuf[slot, r + 1]], axis=1)
                o_pair = jnp.dot(p_pair, v_pair, preferred_element_type=jnp.float32)
                for i in range(2):
                    o = o_pair[i * heads:(i + 1) * heads, i * head_dim:(i + 1) * head_dim]
                    o = o + pn_list[i] * v_new[r + i:r + i + 1]
                    o_buf[slot_o, pl.ds(pl.multiple_of((w * BR + r + i) * heads, 8), heads), :] = o

            @pl.when(b + NB < n_blk)
            def _():
                start_kv(b + NB)
            return m_all, l_all

        init = (jnp.zeros((heads, head_dim), jnp.float32), jnp.ones((heads, head_dim), jnp.float32))
        m_all, l_all = lax.fori_loop(0, blk_per_q, block, init)
        o_buf[slot_o, o_rows:o_rows + heads, :] = m_all
        o_buf[slot_o, o_rows + heads:o_rows + 2 * heads, :] = l_all

    def column(vals, j):
        return jnp.sum(jnp.where(lane == j, vals, 0.0), axis=-1, keepdims=True)

    def combine(slot_o, other, dst, final):
        m1 = o_buf[slot_o, o_rows:o_rows + heads, :]
        l1 = o_buf[slot_o, o_rows + heads:o_rows + 2 * heads, :]
        m2 = other[o_rows:o_rows + heads, :]
        l2 = other[o_rows + heads:o_rows + 2 * heads, :]
        m = jnp.maximum(m1, m2)
        f1 = jnp.exp2((m1 - m) * coef)
        f2 = jnp.exp2((m2 - m) * coef)
        l = l1 * f1 + l2 * f2
        if final:
            f1, f2 = f1 / l, f2 / l
        else:
            o_buf[slot_o, o_rows:o_rows + heads, :] = m
            o_buf[slot_o, o_rows + heads:o_rows + 2 * heads, :] = l

        def row(g, _):
            for u in range(4):
                j = g * 4 + u
                rows = pl.ds(pl.multiple_of(j * heads, 8), heads)
                o = o_buf[slot_o, rows, :] * column(f1, j) + other[rows, :] * column(f2, j)
                if final:
                    o = o.astype(jnp.bfloat16).astype(jnp.float32)
                dst[rows, :] = o
            return 0
        lax.fori_loop(0, quarter // 4, row, 0)

    def d2d(n, k):
        return remote(o_buf.at[n * 4 + 2 * k], rd.at[n * 2 + k], rd_s.at[n * 2 + k], rd_r.at[n * 2 + k], to_core)

    def xsend(n):
        return remote(o_buf.at[n * 4 + 1], rx.at[n], rx_s.at[n], rx_r.at[n], to_chip)

    def at_copy(n):
        return remote(att.at[n * 2 + core], att.at[n * 2 + core], at_s.at[n], at_r.at[n], to_core)

    def p_copy(i):
        return remote(p_buf.at[i], p_recv.at[i], p_s.at[i], p_r.at[i], to_tp)

    def yc_copy(i):
        return remote(y_send.at[i], y_core.at[i], yc_s.at[i], yc_r.at[i], to_core)

    def yx_copy(i):
        return remote(y_send.at[i], y_chip.at[i], yx_s.at[i], yx_r.at[i], to_chip)

    def yf_copy(i):
        return remote(y_chip.at[i], y_fwd.at[i], yf_s.at[i], yf_r.at[i], to_core)

    def finish(n):
        xsend(n).wait_recv()
        combine(n * 4 + 3, rx.at[n], att.at[n * 2 + core], True)
        at_copy(n).start()

    def project(n):
        at_copy(n).wait_recv()
        for h in range(heads):
            cols = [att[n * 2 + c, pl.ds(h, quarter, stride=heads), :] for c in range(2)]
            lhs[:, h * head_dim:(h + 1) * head_dim] = jnp.concatenate(cols, axis=0).astype(jnp.bfloat16)
        if n == 0:
            hid_copy.wait()

        def tile(t, _):
            if n == 0:
                wo_copy(t).wait()
            i = n * n_tiles + t
            p_buf[i] = jnp.dot(lhs[...], wo[t], preferred_element_type=jnp.float32)
            p_copy(i).start()
            return 0
        lax.fori_loop(0, n_tiles, tile, 0)

    def out_slice(i, on_chip, on_core):
        n, t = i // n_tiles, i % n_tiles
        rows = pl.ds(pl.multiple_of(on_chip * chip_rows + n * 2 * quarter, 2 * quarter), 2 * quarter)
        cols = pl.ds(pl.multiple_of(on_core * half + t * TN, TN), TN)
        return rows, cols

    def y_tile(i):
        n, t = i // n_tiles, i % n_tiles
        p_copy(i).wait_recv()
        res = hid[pl.ds(pl.multiple_of(n * 2 * quarter, 2 * quarter), 2 * quarter),
                  pl.ds(pl.multiple_of(t * TN, TN), TN)].astype(jnp.float32)
        y = (res + (p_buf[i] + p_recv[i])).astype(jnp.bfloat16)
        y_send[i] = y.astype(jnp.float32)
        rows, cols = out_slice(i, chip, core)
        y_ref[rows, cols] = y
        yx_copy(i).start()
        yc_copy(i).start()

    def y_from_chip(i):
        yx_copy(i).wait_recv()
        yf_copy(i).start()
        rows, cols = out_slice(i, 1 - chip, core)
        y_ref[rows, cols] = y_chip[i].astype(jnp.bfloat16)
        yc_copy(i).wait_recv()
        rows, cols = out_slice(i, chip, 1 - core)
        y_ref[rows, cols] = y_core[i].astype(jnp.bfloat16)

    def y_from_fwd(i):
        yf_copy(i).wait_recv()
        rows, cols = out_slice(i, 1 - chip, 1 - core)
        y_ref[rows, cols] = y_fwd[i].astype(jnp.bfloat16)

    wo_next = 0
    for n in range(NC):
        for qi in range(4):
            attend_quarter(n, qi)
            if qi == 0:
                d2d(n, 0).start()
            elif qi == 1:
                d2d(n, 0).wait_recv()
                combine(n * 4 + 1, rd.at[n * 2], o_buf.at[n * 4 + 1], False)
                xsend(n).start()
            elif qi == 2:
                d2d(n, 1).start()
            else:
                d2d(n, 1).wait_recv()
                combine(n * 4 + 3, rd.at[n * 2 + 1], o_buf.at[n * 4 + 3], False)
            if n == 0 and qi == 0:
                hid_copy.start()
            if wo_next < n_tiles:
                for _ in range(2):
                    wo_copy(wo_next).start()
                    wo_next += 1
            if n > 0 and qi == 1:
                finish(n - 1)
            if n > 0 and qi == 2:
                project(n - 1)
    finish(NC - 1)
    project(NC - 1)

    total = NC * n_tiles
    lag, lag2 = 2, 4

    def step(i, _):
        @pl.when(i < total)
        def _():
            y_tile(i)

        @pl.when(jnp.logical_and(i >= lag, i < total + lag))
        def _():
            y_from_chip(i - lag)

        @pl.when(i >= lag2)
        def _():
            y_from_fwd(i - lag2)
        return 0
    lax.fori_loop(0, total + lag2, step, 0)

    for n in range(NC):
        d2d(n, 0).wait_send()
        d2d(n, 1).wait_send()
        xsend(n).wait_send()
        at_copy(n).wait_send()

    def drain(i, _):
        p_copy(i).wait_send()
        yc_copy(i).wait_send()
        yx_copy(i).wait_send()
        yf_copy(i).wait_send()
        return 0
    lax.fori_loop(0, total, drain, 0)


def attention(seq_lens, q, kf, vf, hidden, k_cache, v_cache, w_o):
    n_rows, d_model = hidden.shape
    s_dev, head_dim = k_cache.shape[1], k_cache.shape[2]
    heads = q.shape[0] // n_rows
    half = d_model // 2
    n_tiles = half // TN
    quarter = n_rows // (4 * NC)
    msg = quarter * heads + 2 * heads
    total = NC * n_tiles
    vmem = pl.BlockSpec(memory_space=pltpu.VMEM)
    hbm = pl.BlockSpec(memory_space=pl.ANY)
    f32, bf16 = jnp.float32, jnp.bfloat16
    dma = pltpu.SemaphoreType.DMA
    tile_f32 = pltpu.VMEM((total, 2 * quarter, TN), f32)
    return pl.pallas_call(
        attn_kernel,
        out_shape=jax.ShapeDtypeStruct((n_rows, d_model), bf16),
        in_specs=[pl.BlockSpec(memory_space=pltpu.SMEM), vmem, vmem, vmem, hbm, hbm, hbm, hbm],
        out_specs=vmem,
        scratch_shapes=[
            pltpu.VMEM((NC * 4, msg, head_dim), f32),
            pltpu.VMEM((NC * 2, msg, head_dim), f32),
            pltpu.VMEM((NC, msg, head_dim), f32),
            pltpu.VMEM((NC * 2, quarter * heads, head_dim), f32),
            pltpu.VMEM((2 * quarter, heads * head_dim), bf16),
            tile_f32, tile_f32, tile_f32, tile_f32, tile_f32, tile_f32,
            pltpu.VMEM((n_tiles, heads * head_dim, TN), bf16),
            pltpu.VMEM((n_rows // 2, half), bf16),
            pltpu.VMEM((NB, BR, s_dev, head_dim), bf16),
            pltpu.VMEM((NB, BR, s_dev, head_dim), bf16),
            dma((NB,)), dma((NB,)), dma((n_tiles,)), dma,
            dma((NC * 2,)), dma((NC * 2,)), dma((NC,)), dma((NC,)), dma((NC,)), dma((NC,)),
            dma((total,)), dma((total,)), dma((total,)), dma((total,)), dma((total,)), dma((total,)),
            dma((total,)), dma((total,)),
        ],
        compiler_params=pltpu.CompilerParams(
            collective_id=0, has_side_effects=True, vmem_limit_bytes=VMEM_LIMIT),
        name="attend",
    )(seq_lens, q, kf, vf, hidden, k_cache, v_cache, w_o)


def solution(mesh):
    def device_step(hidden, norm_w, w_q, b_q, w_k, b_k, w_v, b_v, w_o, k_cache, v_cache, positions, seq_lens):
        n_rows = hidden.shape[0]
        s_dev, head_dim = k_cache.shape[1], k_cache.shape[3]
        q, kf, vf, kb, vb = qkv(hidden, norm_w, w_q, b_q, w_k, b_k, w_v, b_v, positions, head_dim)
        y_out = attention(seq_lens, q, kf, vf, hidden, k_cache.reshape(n_rows, s_dev, head_dim),
                          v_cache.reshape(n_rows, s_dev, head_dim), w_o)
        return y_out, kb.reshape(n_rows, 1, head_dim), vb.reshape(n_rows, 1, head_dim)

    col_spec = P(None, 'tp')
    vec_spec = P('tp')
    cache_spec = P('dp', 'sp', 'tp', None)
    group_spec = P('dp', 'tp', None)
    in_specs = (P('dp', None), P(None), col_spec, vec_spec, col_spec, vec_spec, col_spec, vec_spec,
                P('tp', None), cache_spec, cache_spec, P('dp'), P('dp'))
    out_specs = (P('dp', None), group_spec, group_spec)
    return jax.shard_map(device_step, mesh=mesh, in_specs=in_specs, out_specs=out_specs, check_vma=False)
```

```python
import functools

import jax
import jax.numpy as jnp
from jax import lax
from jax.experimental import pallas as pl
from jax.experimental.pallas import tpu as pltpu
from jax.sharding import PartitionSpec as P

RMS_EPS = 1.5625e-7
ROPE_BASE = 10000.0
LOG2E = 1.4426950408889634
NEG = -3e38
NEG_FLOOR = -1e38
MESH = pl.DeviceIdType.MESH
VMEM_LIMIT = 67_043_328

ATTN_VMEM = 59 * 2 ** 20

NC = 2
BR = 8
NBK, NBV = 4, 6
TN = 512
TS = 256


def rope_tables(positions, head_dim):
    rot_dim = head_dim // 2
    lane = jnp.arange(head_dim, dtype=jnp.int32)
    freq = ROPE_BASE ** (-2.0 * (lane // 2).astype(jnp.float32) / rot_dim)
    freq = jnp.where(lane < rot_dim, freq, 0.0)
    angles = positions.astype(jnp.float32)[:, None] * freq
    sign = jnp.where(lane % 2 == 0, -1.0, 1.0)
    return jnp.cos(angles), jnp.sin(angles) * sign


def rope(x, cos_t, sin_t, even):
    width = x.shape[-1]
    swapped = jnp.where(even, pltpu.roll(x, width - 1, 1), pltpu.roll(x, 1, 1))
    return (x * cos_t + swapped * sin_t).astype(jnp.bfloat16).astype(jnp.float32)


def qkv_kernel(heads, n_tiles, hid_ref, nw_ref, wq_ref, bq_ref, wk_ref, bk_ref, wv_ref, bv_ref, cos_ref, sin_ref,
               q_ref, kf_ref, vf_ref, kb_ref, vb_ref, normed):
    step = pl.program_id(0)
    n_rows, head_dim = cos_ref.shape

    @pl.when(step == 0)
    def _():
        def norm_rows(i, _):
            rows = pl.ds(pl.multiple_of(i * 32, 32), 32)
            x = hid_ref[rows, :].astype(jnp.float32)
            mean_sq = jnp.mean(x * x, axis=-1, keepdims=True)
            y = x * lax.rsqrt(mean_sq + RMS_EPS) * nw_ref[...].astype(jnp.float32)
            normed[rows, :] = y.astype(jnp.bfloat16)
            return 0
        lax.fori_loop(0, n_rows // 32, norm_rows, 0)

    def even_lanes():
        return lax.broadcasted_iota(jnp.int32, (n_rows, head_dim), 1) % 2 == 0

    def proj(w_ref, b_ref):
        acc = jnp.dot(normed[...], w_ref[...], preferred_element_type=jnp.float32)
        return (acc + b_ref[...].astype(jnp.float32)).astype(jnp.bfloat16).astype(jnp.float32)

    @pl.when(step < n_tiles)
    def _():
        val = proj(wq_ref, bq_ref)
        per_tile = heads // n_tiles
        for h in range(per_tile):
            rot = rope(val[:, h * head_dim:(h + 1) * head_dim], cos_ref[...], sin_ref[...], even_lanes())
            q_ref[pl.ds(step * per_tile + h, n_rows, stride=heads), :] = rot

    @pl.when(step == n_tiles)
    def _():
        k_rot = rope(proj(wk_ref, bk_ref), cos_ref[...], sin_ref[...], even_lanes())
        kf_ref[...] = k_rot
        kb_ref[...] = k_rot.astype(jnp.bfloat16)
        v_new = proj(wv_ref, bv_ref)
        vf_ref[...] = v_new
        vb_ref[...] = v_new.astype(jnp.bfloat16)


def qkv(hidden, norm_w, w_q, b_q, w_k, b_k, w_v, b_v, positions, head_dim):
    n_rows, d_model = hidden.shape
    q_cols = w_q.shape[1]
    heads = q_cols // head_dim
    tile = 512
    n_tiles = q_cols // tile
    cos_t, sin_t = rope_tables(positions, head_dim)

    def whole(shape):
        return pl.BlockSpec(shape, lambda i: (0,) * len(shape))

    return pl.pallas_call(
        functools.partial(qkv_kernel, heads, n_tiles),
        grid=(n_tiles + 1,),
        in_specs=[
            whole((n_rows, d_model)), whole((1, d_model)),
            pl.BlockSpec((d_model, tile), lambda i: (0, jnp.minimum(i, n_tiles - 1))),
            pl.BlockSpec((1, tile), lambda i: (0, jnp.minimum(i, n_tiles - 1))),
            whole((d_model, head_dim)), whole((1, head_dim)), whole((d_model, head_dim)), whole((1, head_dim)),
            whole((n_rows, head_dim)), whole((n_rows, head_dim)),
        ],
        out_specs=[whole((n_rows * heads, head_dim))] + [whole((n_rows, head_dim))] * 4,
        out_shape=[
            jax.ShapeDtypeStruct((n_rows * heads, head_dim), jnp.float32),
            jax.ShapeDtypeStruct((n_rows, head_dim), jnp.float32),
            jax.ShapeDtypeStruct((n_rows, head_dim), jnp.float32),
            jax.ShapeDtypeStruct((n_rows, head_dim), jnp.bfloat16),
            jax.ShapeDtypeStruct((n_rows, head_dim), jnp.bfloat16),
        ],
        scratch_shapes=[pltpu.VMEM((n_rows, d_model), jnp.bfloat16)],
        compiler_params=pltpu.CompilerParams(vmem_limit_bytes=VMEM_LIMIT),
        name="qkv",
    )(hidden, norm_w[None], w_q, b_q[None], w_k, b_k[None], w_v, b_v[None], cos_t, sin_t)


def attn_kernel(seq_ref, q_ref, kf_ref, vf_ref, hid_hbm, k_hbm, v_hbm, wo_hbm, y_ref,
                o_buf, rd, rx, att, lhs, s_sc, p_sc, new_sc, p_buf, p_recv, y_send, y_core, y_chip, y_fwd, wo, hid,
                kbuf, vbuf, k_sem, v_sem, wo_sem, hid_sem, rd_s, rd_r, rx_s, rx_r, at_s, at_r, p_s, p_r,
                yc_s, yc_r, yx_s, yx_r, yf_s, yf_r):
    n_rows, d_model = y_ref.shape
    s_dev, head_dim = kbuf.shape[2], kbuf.shape[3]
    heads = q_ref.shape[0] // n_rows
    n_tiles = wo.shape[0]
    half = n_tiles * TN
    quarter = n_rows // (4 * NC)
    o_rows = quarter * heads
    chip_rows = n_rows // 2
    bq = quarter // BR
    n_blk = n_rows // BR
    coef = head_dim ** -0.5 * LOG2E

    dp, tp, sp = lax.axis_index("dp"), lax.axis_index("tp"), lax.axis_index("sp")
    chip, core = sp // 2, sp % 2
    to_core = (dp, tp, 2 * chip + (1 - core))
    to_chip = (dp, tp, 2 * (1 - chip) + core)
    to_tp = (dp, 1 - tp, sp)

    def remote(src, dst, s_sem, r_sem, dev):
        return pltpu.make_async_remote_copy(src_ref=src, dst_ref=dst, send_sem=s_sem, recv_sem=r_sem,
                                            device_id=dev, device_id_type=MESH)

    def group_row(u):
        near = u // (2 * NC)
        own = u % 2
        n = (u % (2 * NC)) // 2
        on_chip = near * chip + (1 - near) * (1 - chip)
        on_core = own * core + (1 - own) * (1 - core)
        return on_chip * chip_rows + n * 2 * quarter + on_core * quarter

    def block_row(b):
        return pl.multiple_of(group_row(b // bq) + (b % bq) * BR, BR)

    def k_copy(b):
        return pltpu.make_async_copy(k_hbm.at[pl.ds(block_row(b), BR)], kbuf.at[b % NBK], k_sem.at[b % NBK])

    def v_copy(b):
        return pltpu.make_async_copy(v_hbm.at[pl.ds(block_row(b), BR)], vbuf.at[b % NBV], v_sem.at[b % NBV])

    def wo_copy(t):
        cols = pl.ds(pl.multiple_of(core * half + t * TN, 128), TN)
        return pltpu.make_async_copy(wo_hbm.at[:, cols], wo.at[t], wo_sem.at[t])

    hid_copy = pltpu.make_async_copy(
        hid_hbm.at[pl.ds(pl.multiple_of(chip * chip_rows, 128), chip_rows),
                   pl.ds(pl.multiple_of(core * half, 128), half)], hid, hid_sem)

    for b in range(NBV):
        if b < NBK:
            k_copy(b).start()
        v_copy(b).start()

    barrier = pltpu.get_barrier_semaphore()
    for dev in (to_core, to_chip, to_tp):
        pl.semaphore_signal(barrier, inc=1, device_id=dev, device_id_type=MESH)

    lane = lax.broadcasted_iota(jnp.int32, (heads, head_dim), 1)
    pos = lax.broadcasted_iota(jnp.int32, (heads, s_dev), 1) + sp * s_dev
    zeros_q = jnp.zeros((heads, head_dim), jnp.float32)

    def q_rows(row):
        return q_ref[pl.ds(pl.multiple_of(row * heads, 8), heads), :]

    def new_scores(n):
        row0 = chip * chip_rows + n * 2 * quarter + core * quarter

        def rows8(g, acc):
            base = pl.multiple_of(row0 + g * 8, 8)
            k_new = kf_ref[pl.ds(base, 8), :]
            for r in range(8):
                s_new = jnp.sum(q_rows(base + r) * k_new[r:r + 1], axis=-1, keepdims=True)
                acc = jnp.where(lane == g * 8 + r, s_new, acc)
            return acc
        new_sc[n] = lax.fori_loop(0, quarter // 8, rows8, zeros_q)

    for n in range(NC):
        new_scores(n)
    pl.semaphore_wait(barrier, 3)

    def column(vals, j):
        return jnp.sum(jnp.where(lane == j, vals, 0.0), axis=-1, keepdims=True)

    def d2d(k):
        return remote(o_buf.at[2 * k], rd.at[k], rd_s.at[k], rd_r.at[k], to_core)

    def xsend(n):
        return remote(o_buf.at[2 * n + 1], rx.at[n], rx_s.at[n], rx_r.at[n], to_chip)

    def at_copy(n):
        return remote(att.at[n * 2 + core], att.at[n * 2 + core], at_s.at[n], at_r.at[n], to_core)

    def merge_core(u):
        k = u // 2
        m1 = o_buf[u, o_rows:o_rows + heads, :]
        l1 = o_buf[u, o_rows + heads:o_rows + 2 * heads, :]
        m2 = rd[k, o_rows:o_rows + heads, :]
        l2 = rd[k, o_rows + heads:o_rows + 2 * heads, :]
        m = jnp.maximum(m1, m2)
        f1 = jnp.exp2((m1 - m) * coef)
        f2 = jnp.exp2((m2 - m) * coef)
        o_buf[u, o_rows:o_rows + heads, :] = m
        o_buf[u, o_rows + heads:o_rows + 2 * heads, :] = l1 * f1 + l2 * f2

        def rows8(g, _):
            for r in range(8):
                j = g * 8 + r
                rows = pl.ds(pl.multiple_of(j * heads, 8), heads)
                o_buf[u, rows, :] = o_buf[u, rows, :] * column(f1, j) + rd[k, rows, :] * column(f2, j)
            return 0
        lax.fori_loop(0, quarter // 8, rows8, 0)

    def finish(n):
        u = 2 * NC + 2 * n + 1
        row0 = chip * chip_rows + n * 2 * quarter + core * quarter
        m1 = o_buf[u, o_rows:o_rows + heads, :]
        l1 = o_buf[u, o_rows + heads:o_rows + 2 * heads, :]
        m2 = rx[n, o_rows:o_rows + heads, :]
        l2 = rx[n, o_rows + heads:o_rows + 2 * heads, :]
        m3 = new_sc[n]
        m = jnp.maximum(jnp.maximum(m1, m2), m3)
        f1 = jnp.exp2((m1 - m) * coef)
        f2 = jnp.exp2((m2 - m) * coef)
        f3 = jnp.exp2((m3 - m) * coef)
        l = l1 * f1 + l2 * f2 + f3
        f1, f2, f3 = f1 / l, f2 / l, f3 / l

        def rows8(g, _):
            v_new = vf_ref[pl.ds(pl.multiple_of(row0 + g * 8, 8), 8), :]
            for r in range(8):
                j = g * 8 + r
                rows = pl.ds(pl.multiple_of(j * heads, 8), heads)
                o = o_buf[u, rows, :] * column(f1, j) + rx[n, rows, :] * column(f2, j)
                o = o + column(f3, j) * v_new[r:r + 1]
                att[n * 2 + core, rows, :] = o.astype(jnp.bfloat16).astype(jnp.float32)
            return 0
        lax.fori_loop(0, quarter // 8, rows8, 0)

    def block(b, _):
        @pl.when(b < n_blk)
        def _():
            k_copy(b).wait()

        b1 = jnp.minimum(b, n_blk - 1)
        b2 = jnp.clip(b - 1, 0, n_blk - 1)
        b3 = jnp.clip(b - 2, 0, n_blk - 1)

        @pl.when(jnp.logical_or(b == 0, b >= 3))
        def _():
            v_copy(b3).wait()

        u3, vslot = b3 // bq, b3 % NBV
        for pair in range(BR // 2):
            r = 2 * pair
            v_pair = jnp.concatenate([vbuf[vslot, r], vbuf[vslot, r + 1]], axis=1)
            o_pair = jnp.dot(p_sc[pair], v_pair, preferred_element_type=jnp.float32)
            for i in range(2):
                o = o_pair[i * heads:(i + 1) * heads, i * head_dim:(i + 1) * head_dim]
                o_buf[u3, pl.ds(pl.multiple_of(((b3 % bq) * BR + r + i) * heads, 8), heads), :] = o
        u2, row2 = b2 // bq, block_row(b2)
        m_all = o_buf[u2, o_rows:o_rows + heads, :]
        l_all = o_buf[u2, o_rows + heads:o_rows + 2 * heads, :]
        for pair in range(BR // 2):
            p_list = []
            for i in range(2):
                r = 2 * pair + i
                s = s_sc[pair, i * heads:(i + 1) * heads, :]
                s = jnp.where(pos < seq_ref[row2 + r], s, NEG)
                m = jnp.maximum(jnp.max(s, axis=-1, keepdims=True), NEG_FLOOR)
                p = jnp.exp2((s - m) * coef)
                l = jnp.sum(p, axis=-1, keepdims=True)
                here = lane == (b2 % bq) * BR + r
                m_all = jnp.where(here, m, m_all)
                l_all = jnp.where(here, l, l_all)
                p_list.append(p)
            p_sc[pair] = jnp.concatenate(p_list, axis=0).astype(jnp.bfloat16)
        o_buf[u2, o_rows:o_rows + heads, :] = m_all
        o_buf[u2, o_rows + heads:o_rows + 2 * heads, :] = l_all
        row1, kslot = block_row(b1), b1 % NBK
        for pair in range(BR // 2):
            r = 2 * pair
            left = jnp.concatenate([q_rows(row1 + r), zeros_q], axis=0)
            right = jnp.concatenate([zeros_q, q_rows(row1 + r + 1)], axis=0)
            q_pair = jnp.concatenate([left, right], axis=1).astype(jnp.bfloat16)
            k_pair = jnp.concatenate([kbuf[kslot, r], kbuf[kslot, r + 1]], axis=1)
            s_sc[pair] = lax.dot_general(q_pair, k_pair, (((1,), (1,)), ((), ())),
                                         preferred_element_type=jnp.float32)

        @pl.when(b + NBK < n_blk)
        def _():
            k_copy(b + NBK).start()

        @pl.when(jnp.logical_and(b >= 2, b - 2 + NBV < n_blk))
        def _():
            v_copy(b - 2 + NBV).start()

        done = jnp.logical_and(b >= 2, (b - 2) % bq == bq - 1)
        u = b3 // bq

        @pl.when(jnp.logical_and(done, u % 2 == 0))
        def _():
            d2d(u // 2).start()

        @pl.when(jnp.logical_and(done, u % 2 == 1))
        def _():
            d2d(u // 2).wait_recv()
            merge_core(u)

            @pl.when(u < 2 * NC)
            def _():
                xsend(u // 2).start()
        return 0

    lax.fori_loop(0, n_blk + 2, block, 0)
    for t in range(n_tiles):
        wo_copy(t).start()
        if t == 0:
            hid_copy.start()

    def finish_step(n, _):
        xsend(n).wait_recv()
        finish(n)
        at_copy(n).start()
        return 0
    lax.fori_loop(0, NC, finish_step, 0)

    def p_copy(i):
        return remote(p_buf.at[i], p_recv.at[i], p_s.at[i], p_r.at[i], to_tp)

    def yc_copy(i):
        return remote(y_send.at[i], y_core.at[i], yc_s.at[i], yc_r.at[i], to_core)

    def yx_copy(i):
        return remote(y_send.at[i], y_chip.at[i], yx_s.at[i], yx_r.at[i], to_chip)

    def yf_copy(i):
        return remote(y_chip.at[i], y_fwd.at[i], yf_s.at[i], yf_r.at[i], to_core)

    for n in range(NC):
        at_copy(n).wait_recv()
        for h in range(heads):
            cols = [att[n * 2 + c, pl.ds(h, quarter, stride=heads), :] for c in range(2)]
            lhs[n * 2 * quarter:(n + 1) * 2 * quarter, h * head_dim:(h + 1) * head_dim] = (
                jnp.concatenate(cols, axis=0).astype(jnp.bfloat16))
    hid_copy.wait()
    per = TN // TS

    def project(t, _):
        wo_copy(t).wait()
        res = jnp.dot(lhs[...], wo[t], preferred_element_type=jnp.float32)
        for s in range(per):
            i = t * per + s
            p_buf[i] = res[:, s * TS:(s + 1) * TS]
            p_copy(i).start()
        return 0

    def out_cols(i, on_core):
        return pl.ds(pl.multiple_of(on_core * half + i * TS, TS), TS)

    def out_rows(on_chip):
        return pl.ds(pl.multiple_of(on_chip * chip_rows, chip_rows), chip_rows)

    def y_tile(i):
        p_copy(i).wait_recv()
        res = hid[:, pl.ds(pl.multiple_of(i * TS, TS), TS)].astype(jnp.float32)
        y = (res + (p_buf[i] + p_recv[i])).astype(jnp.bfloat16)
        y_send[i] = y.astype(jnp.float32)
        y_ref[out_rows(chip), out_cols(i, core)] = y
        yx_copy(i).start()
        yc_copy(i).start()

    def y_from_chip(i):
        yx_copy(i).wait_recv()
        yf_copy(i).start()
        y_ref[out_rows(1 - chip), out_cols(i, core)] = y_chip[i].astype(jnp.bfloat16)
        yc_copy(i).wait_recv()
        y_ref[out_rows(chip), out_cols(i, 1 - core)] = y_core[i].astype(jnp.bfloat16)

    def y_from_fwd(i):
        yf_copy(i).wait_recv()
        y_ref[out_rows(1 - chip), out_cols(i, 1 - core)] = y_fwd[i].astype(jnp.bfloat16)

    total = n_tiles * per
    lead = 2
    for t in range(lead):
        project(t, 0)
    lag, lag2 = 2, 3

    def step(i, _):
        @pl.when(jnp.logical_and(i % per == 0, i // per + lead < n_tiles))
        def _():
            project(i // per + lead, 0)

        @pl.when(i < total)
        def _():
            y_tile(i)

        @pl.when(jnp.logical_and(i >= lag, i < total + lag))
        def _():
            y_from_chip(i - lag)

        @pl.when(i >= lag2)
        def _():
            y_from_fwd(i - lag2)
        return 0
    lax.fori_loop(0, total + lag2, step, 0)

    for k in range(2 * NC):
        d2d(k).wait_send()
    for n in range(NC):
        xsend(n).wait_send()
        at_copy(n).wait_send()

    def drain(i, _):
        p_copy(i).wait_send()
        yc_copy(i).wait_send()
        yx_copy(i).wait_send()
        yf_copy(i).wait_send()
        return 0
    lax.fori_loop(0, total, drain, 0)


def attention(seq_lens, q, kf, vf, hidden, k_cache, v_cache, w_o):
    n_rows, d_model = hidden.shape
    s_dev, head_dim = k_cache.shape[1], k_cache.shape[2]
    heads = q.shape[0] // n_rows
    half = d_model // 2
    n_tiles = half // TN
    quarter = n_rows // (4 * NC)
    msg = quarter * heads + 2 * heads
    total = half // TS
    vmem = pl.BlockSpec(memory_space=pltpu.VMEM)
    hbm = pl.BlockSpec(memory_space=pl.ANY)
    f32, bf16 = jnp.float32, jnp.bfloat16
    dma = pltpu.SemaphoreType.DMA
    tile_f32 = pltpu.VMEM((total, n_rows // 2, TS), f32)
    return pl.pallas_call(
        attn_kernel,
        out_shape=jax.ShapeDtypeStruct((n_rows, d_model), bf16),
        in_specs=[pl.BlockSpec(memory_space=pltpu.SMEM), vmem, vmem, vmem, hbm, hbm, hbm, hbm],
        out_specs=vmem,
        scratch_shapes=[
            pltpu.VMEM((NC * 4, msg, head_dim), f32),
            pltpu.VMEM((NC * 2, msg, head_dim), f32),
            pltpu.VMEM((NC, msg, head_dim), f32),
            pltpu.VMEM((NC * 2, quarter * heads, head_dim), f32),
            pltpu.VMEM((n_rows // 2, heads * head_dim), bf16),
            pltpu.VMEM((BR // 2, 2 * heads, s_dev), f32),
            pltpu.VMEM((BR // 2, 2 * heads, s_dev), bf16),
            pltpu.VMEM((NC, heads, head_dim), f32),
            tile_f32, tile_f32, tile_f32, tile_f32, tile_f32, tile_f32,
            pltpu.VMEM((n_tiles, heads * head_dim, TN), bf16),
            pltpu.VMEM((n_rows // 2, half), bf16),
            pltpu.VMEM((NBK, BR, s_dev, head_dim), bf16),
            pltpu.VMEM((NBV, BR, s_dev, head_dim), bf16),
            dma((NBK,)), dma((NBV,)), dma((n_tiles,)), dma,
            dma((NC * 2,)), dma((NC * 2,)), dma((NC,)), dma((NC,)), dma((NC,)), dma((NC,)),
            dma((total,)), dma((total,)), dma((total,)), dma((total,)), dma((total,)), dma((total,)),
            dma((total,)), dma((total,)),
        ],
        compiler_params=pltpu.CompilerParams(
            collective_id=0, has_side_effects=True, vmem_limit_bytes=ATTN_VMEM),
        name="attend",
    )(seq_lens, q, kf, vf, hidden, k_cache, v_cache, w_o)


def solution(mesh):
    def device_step(hidden, norm_w, w_q, b_q, w_k, b_k, w_v, b_v, w_o, k_cache, v_cache, positions, seq_lens):
        n_rows = hidden.shape[0]
        s_dev, head_dim = k_cache.shape[1], k_cache.shape[3]
        q, kf, vf, kb, vb = qkv(hidden, norm_w, w_q, b_q, w_k, b_k, w_v, b_v, positions, head_dim)
        y_out = attention(seq_lens, q, kf, vf, hidden, k_cache.reshape(n_rows, s_dev, head_dim),
                          v_cache.reshape(n_rows, s_dev, head_dim), w_o)
        return y_out, kb.reshape(n_rows, 1, head_dim), vb.reshape(n_rows, 1, head_dim)

    col_spec = P(None, 'tp')
    vec_spec = P('tp')
    cache_spec = P('dp', 'sp', 'tp', None)
    group_spec = P('dp', 'tp', None)
    in_specs = (P('dp', None), P(None), col_spec, vec_spec, col_spec, vec_spec, col_spec, vec_spec,
                P('tp', None), cache_spec, cache_spec, P('dp'), P('dp'))
    out_specs = (P('dp', None), group_spec, group_spec)
    return jax.shard_map(device_step, mesh=mesh, in_specs=in_specs, out_specs=out_specs, check_vma=False)
```

```python
import functools

import jax
import jax.numpy as jnp
from jax import lax
from jax.experimental import pallas as pl
from jax.experimental.pallas import tpu as pltpu
from jax.sharding import PartitionSpec as P

RMS_EPS = 1.5625e-7
ROPE_BASE = 10000.0
LOG2E = 1.4426950408889634
NEG = -3e38
NEG_FLOOR = -1e38
MESH = pl.DeviceIdType.MESH
VMEM_LIMIT = 67_043_328


NC = 2
BR = 8
NBK, NBV = 4, 6
TN = 512
TS = 256


def rope_tables(positions, head_dim):
    rot_dim = head_dim // 2
    lane = jnp.arange(head_dim, dtype=jnp.int32)
    freq = ROPE_BASE ** (-2.0 * (lane // 2).astype(jnp.float32) / rot_dim)
    freq = jnp.where(lane < rot_dim, freq, 0.0)
    angles = positions.astype(jnp.float32)[:, None] * freq
    sign = jnp.where(lane % 2 == 0, -1.0, 1.0)
    return jnp.cos(angles), jnp.sin(angles) * sign


def rope(x, cos_t, sin_t, even):
    width = x.shape[-1]
    swapped = jnp.where(even, pltpu.roll(x, width - 1, 1), pltpu.roll(x, 1, 1))
    return (x * cos_t + swapped * sin_t).astype(jnp.bfloat16).astype(jnp.float32)


def attn_kernel(seq_ref, cos_ref, sin_ref, nw_ref, bq_ref, bk_ref, bv_ref, hid_hbm, wq_hbm, wk_hbm, wv_hbm,
                k_hbm, v_hbm, wo_hbm, y_ref, kb_ref, vb_ref,
                q_ref, q_send, q_recv, wkv, bqf, kf_ref, vf_ref, in_sem, wkv_sem, q_s, q_r, o_buf, rd, rx, att, lhs, s_sc, p_sc, new_sc, p_buf, p_recv, y_send, y_core, y_chip, y_fwd, wo, hid,
                kbuf, vbuf, k_sem, v_sem, wo_sem, hid_sem, rd_s, rd_r, rx_s, rx_r, at_s, at_r, p_s, p_r,
                yc_s, yc_r, yx_s, yx_r, yf_s, yf_r):
    n_rows, d_model = y_ref.shape
    s_dev, head_dim = kbuf.shape[2], kbuf.shape[3]
    heads = q_ref.shape[0] // n_rows
    n_tiles = wo.shape[0]
    half = n_tiles * TN
    quarter = n_rows // (4 * NC)
    o_rows = quarter * heads
    chip_rows = n_rows // 2
    bq = quarter // BR
    n_blk = n_rows // BR
    coef = head_dim ** -0.5 * LOG2E

    dp, tp, sp = lax.axis_index("dp"), lax.axis_index("tp"), lax.axis_index("sp")
    chip, core = sp // 2, sp % 2
    to_core = (dp, tp, 2 * chip + (1 - core))
    to_chip = (dp, tp, 2 * (1 - chip) + core)
    to_tp = (dp, 1 - tp, sp)

    def remote(src, dst, s_sem, r_sem, dev):
        return pltpu.make_async_remote_copy(src_ref=src, dst_ref=dst, send_sem=s_sem, recv_sem=r_sem,
                                            device_id=dev, device_id_type=MESH)

    def group_row(u):
        near = u // (2 * NC)
        own = u % 2
        n = (u % (2 * NC)) // 2
        on_chip = near * chip + (1 - near) * (1 - chip)
        on_core = own * core + (1 - own) * (1 - core)
        return on_chip * chip_rows + n * 2 * quarter + on_core * quarter

    def block_row(b):
        return pl.multiple_of(group_row(b // bq) + (b % bq) * BR, BR)

    def k_copy(b):
        return pltpu.make_async_copy(k_hbm.at[pl.ds(block_row(b), BR)], kbuf.at[b % NBK], k_sem.at[b % NBK])

    def v_copy(b):
        return pltpu.make_async_copy(v_hbm.at[pl.ds(block_row(b), BR)], vbuf.at[b % NBV], v_sem.at[b % NBV])

    def wo_copy(t):
        cols = pl.ds(pl.multiple_of(core * half + t * TN, 128), TN)
        return pltpu.make_async_copy(wo_hbm.at[:, cols], wo.at[t], wo_sem.at[t])

    hid_copy = pltpu.make_async_copy(
        hid_hbm.at[pl.ds(pl.multiple_of(chip * chip_rows, 128), chip_rows),
                   pl.ds(pl.multiple_of(core * half, 128), half)], hid, hid_sem)

    n_q = q_send.shape[0]
    tile_heads = TN // head_dim
    k_half = wo.shape[1]
    in_copy = pltpu.make_async_copy(hid_hbm, y_ref, in_sem)
    wk_copy = pltpu.make_async_copy(wk_hbm, wkv.at[:, :head_dim], wkv_sem.at[0])
    wv_copy = pltpu.make_async_copy(wv_hbm, wkv.at[:, head_dim:], wkv_sem.at[1])

    def wq_copy(i):
        cols = pl.ds(pl.multiple_of((core * n_q + i // 2) * TN, TN), TN)
        return pltpu.make_async_copy(wq_hbm.at[pl.ds((i % 2) * k_half, k_half), cols], wo.at[i], wo_sem.at[i])

    in_copy.start()
    wk_copy.start()
    wv_copy.start()
    for i in range(2 * n_q):
        wq_copy(i).start()

    barrier = pltpu.get_barrier_semaphore()
    for dev in (to_core, to_chip, to_tp):
        pl.semaphore_signal(barrier, inc=1, device_id=dev, device_id_type=MESH)

    bqf[...] = bq_ref[...].astype(jnp.float32)
    in_copy.wait()

    def norm_rows(i, _):
        rows = pl.ds(pl.multiple_of(i * 32, 32), 32)
        sq = jnp.zeros((32, 128), jnp.float32)
        for c in range(d_model // 128):
            x = y_ref[rows, c * 128:(c + 1) * 128].astype(jnp.float32)
            sq = sq + x * x
        inv = lax.rsqrt(jnp.sum(sq, axis=-1, keepdims=True) / d_model + RMS_EPS)
        for c in range(d_model // 128):
            x = y_ref[rows, c * 128:(c + 1) * 128].astype(jnp.float32)
            x = x * inv * nw_ref[c:c + 1, :].astype(jnp.float32)
            y_ref[rows, c * 128:(c + 1) * 128] = x.astype(jnp.bfloat16)
        return 0
    lax.fori_loop(0, n_rows // 32, norm_rows, 0)
    pl.semaphore_wait(barrier, 3)

    even = lax.broadcasted_iota(jnp.int32, (n_rows, head_dim), 1) % 2 == 0

    def round_f32(x):
        return x.astype(jnp.bfloat16).astype(jnp.float32)

    wk_copy.wait()
    wv_copy.wait()
    kv = jnp.dot(y_ref[...], wkv[...], preferred_element_type=jnp.float32)
    k_rot = rope(round_f32(kv[:, :head_dim] + bk_ref[...].astype(jnp.float32)), cos_ref[...], sin_ref[...], even)
    kf_ref[...] = k_rot
    kb_ref[...] = k_rot.astype(jnp.bfloat16)
    v_val = round_f32(kv[:, head_dim:] + bv_ref[...].astype(jnp.float32))
    vf_ref[...] = v_val
    vb_ref[...] = v_val.astype(jnp.bfloat16)

    def q_copy(t):
        return remote(q_send.at[t], q_recv.at[t], q_s.at[t], q_r.at[t], to_core)

    def q_tile(t, _):
        wq_copy(2 * t).wait()
        wq_copy(2 * t + 1).wait()

        @pl.when(t == n_q - 1)
        def _():
            for b in range(NBV):
                if b < NBK:
                    k_copy(b).start()
                v_copy(b).start()
        acc = jnp.dot(y_ref[:, :k_half], wo[2 * t], preferred_element_type=jnp.float32)
        acc = acc + jnp.dot(y_ref[:, k_half:], wo[2 * t + 1], preferred_element_type=jnp.float32)
        for h in range(tile_heads):
            head = core * (heads // 2) + t * tile_heads + h
            val = round_f32(acc[:, h * head_dim:(h + 1) * head_dim] + bqf[pl.ds(head, 1), :])
            val = rope(val, cos_ref[...], sin_ref[...], even)
            q_ref[pl.ds(head, n_rows, stride=heads), :] = val
            q_send[t, pl.ds(h, n_rows, stride=tile_heads), :] = val
        q_copy(t).start()
        return 0
    lax.fori_loop(0, n_q, q_tile, 0)

    def q_take(t, _):
        q_copy(t).wait_recv()
        for h in range(tile_heads):
            head = (1 - core) * (heads // 2) + t * tile_heads + h
            q_ref[pl.ds(head, n_rows, stride=heads), :] = q_recv[t, pl.ds(h, n_rows, stride=tile_heads), :]
        return 0
    lax.fori_loop(0, n_q, q_take, 0)

    lane = lax.broadcasted_iota(jnp.int32, (heads, head_dim), 1)
    pos = lax.broadcasted_iota(jnp.int32, (heads, s_dev), 1) + sp * s_dev
    zeros_q = jnp.zeros((heads, head_dim), jnp.float32)

    def q_rows(row):
        return q_ref[pl.ds(pl.multiple_of(row * heads, 8), heads), :]

    def new_scores(n):
        row0 = chip * chip_rows + n * 2 * quarter + core * quarter

        def rows8(g, acc):
            base = pl.multiple_of(row0 + g * 8, 8)
            k_new = kf_ref[pl.ds(base, 8), :]
            for r in range(8):
                s_new = jnp.sum(q_rows(base + r) * k_new[r:r + 1], axis=-1, keepdims=True)
                acc = jnp.where(lane == g * 8 + r, s_new, acc)
            return acc
        new_sc[n] = lax.fori_loop(0, quarter // 8, rows8, zeros_q)

    for n in range(NC):
        new_scores(n)

    def column(vals, j):
        return jnp.broadcast_to(vals[:, j:j + 1], (heads, head_dim))

    def d2d(k):
        return remote(o_buf.at[2 * k], rd.at[k], rd_s.at[k], rd_r.at[k], to_core)

    def xsend(n):
        return remote(o_buf.at[2 * n + 1], rx.at[n], rx_s.at[n], rx_r.at[n], to_chip)

    def at_copy(n):
        return remote(att.at[n * 2 + core], att.at[n * 2 + core], at_s.at[n], at_r.at[n], to_core)

    def merge_core(u):
        k = u // 2
        m1 = o_buf[u, o_rows:o_rows + heads, :]
        l1 = o_buf[u, o_rows + heads:o_rows + 2 * heads, :]
        m2 = rd[k, o_rows:o_rows + heads, :]
        l2 = rd[k, o_rows + heads:o_rows + 2 * heads, :]
        m = jnp.maximum(m1, m2)
        f1 = jnp.exp2((m1 - m) * coef)
        f2 = jnp.exp2((m2 - m) * coef)
        o_buf[u, o_rows:o_rows + heads, :] = m
        o_buf[u, o_rows + heads:o_rows + 2 * heads, :] = l1 * f1 + l2 * f2

        for j in range(quarter):
            rows = pl.ds(j * heads, heads)
            o_buf[u, rows, :] = o_buf[u, rows, :] * column(f1, j) + rd[k, rows, :] * column(f2, j)

    def finish(n):
        u = 2 * NC + 2 * n + 1
        row0 = chip * chip_rows + n * 2 * quarter + core * quarter
        m1 = o_buf[u, o_rows:o_rows + heads, :]
        l1 = o_buf[u, o_rows + heads:o_rows + 2 * heads, :]
        m2 = rx[n, o_rows:o_rows + heads, :]
        l2 = rx[n, o_rows + heads:o_rows + 2 * heads, :]
        m3 = new_sc[n]
        m = jnp.maximum(jnp.maximum(m1, m2), m3)
        f1 = jnp.exp2((m1 - m) * coef)
        f2 = jnp.exp2((m2 - m) * coef)
        f3 = jnp.exp2((m3 - m) * coef)
        l = l1 * f1 + l2 * f2 + f3
        f1, f2, f3 = f1 / l, f2 / l, f3 / l

        for j in range(quarter):
            if j % 8 == 0:
                v_new = vf_ref[pl.ds(pl.multiple_of(row0 + j, 8), 8), :]
            rows = pl.ds(j * heads, heads)
            o = o_buf[u, rows, :] * column(f1, j) + rx[n, rows, :] * column(f2, j)
            o = o + column(f3, j) * v_new[j % 8:j % 8 + 1]
            att[n * 2 + core, rows, :] = round_f32(o)

    def block(b, _):
        @pl.when(b < n_blk)
        def _():
            k_copy(b).wait()

        b1 = jnp.minimum(b, n_blk - 1)
        b2 = jnp.clip(b - 1, 0, n_blk - 1)
        b3 = jnp.clip(b - 2, 0, n_blk - 1)

        @pl.when(jnp.logical_or(b == 0, b >= 3))
        def _():
            v_copy(b3).wait()

        u3, vslot = b3 // bq, b3 % NBV
        for pair in range(BR // 2):
            r = 2 * pair
            v_pair = jnp.concatenate([vbuf[vslot, r], vbuf[vslot, r + 1]], axis=1)
            o_pair = jnp.dot(p_sc[pair], v_pair, preferred_element_type=jnp.float32)
            for i in range(2):
                o = o_pair[i * heads:(i + 1) * heads, i * head_dim:(i + 1) * head_dim]
                o_buf[u3, pl.ds(pl.multiple_of(((b3 % bq) * BR + r + i) * heads, 8), heads), :] = o
        u2, row2 = b2 // bq, block_row(b2)
        m_all = o_buf[u2, o_rows:o_rows + heads, :]
        l_all = o_buf[u2, o_rows + heads:o_rows + 2 * heads, :]
        for pair in range(BR // 2):
            p_list = []
            for i in range(2):
                r = 2 * pair + i
                s = s_sc[pair, i * heads:(i + 1) * heads, :]
                s = jnp.where(pos < seq_ref[row2 + r], s, NEG)
                m = jnp.maximum(jnp.max(s, axis=-1, keepdims=True), NEG_FLOOR)
                p = jnp.exp2((s - m) * coef)
                l = jnp.sum(p, axis=-1, keepdims=True)
                here = lane == (b2 % bq) * BR + r
                m_all = jnp.where(here, m, m_all)
                l_all = jnp.where(here, l, l_all)
                p_list.append(p)
            p_sc[pair] = jnp.concatenate(p_list, axis=0).astype(jnp.bfloat16)
        o_buf[u2, o_rows:o_rows + heads, :] = m_all
        o_buf[u2, o_rows + heads:o_rows + 2 * heads, :] = l_all
        row1, kslot = block_row(b1), b1 % NBK
        for pair in range(BR // 2):
            r = 2 * pair
            left = jnp.concatenate([q_rows(row1 + r), zeros_q], axis=0)
            right = jnp.concatenate([zeros_q, q_rows(row1 + r + 1)], axis=0)
            q_pair = jnp.concatenate([left, right], axis=1).astype(jnp.bfloat16)
            k_pair = jnp.concatenate([kbuf[kslot, r], kbuf[kslot, r + 1]], axis=1)
            s_sc[pair] = lax.dot_general(q_pair, k_pair, (((1,), (1,)), ((), ())),
                                         preferred_element_type=jnp.float32)

        @pl.when(b + NBK < n_blk)
        def _():
            k_copy(b + NBK).start()

        @pl.when(jnp.logical_and(b >= 2, b - 2 + NBV < n_blk))
        def _():
            v_copy(b - 2 + NBV).start()

        done = jnp.logical_and(b >= 2, (b - 2) % bq == bq - 1)
        u = b3 // bq

        @pl.when(jnp.logical_and(done, u % 2 == 0))
        def _():
            d2d(u // 2).start()

        @pl.when(jnp.logical_and(done, u % 2 == 1))
        def _():
            d2d(u // 2).wait_recv()
            merge_core(u)

            @pl.when(u < 2 * NC)
            def _():
                xsend(u // 2).start()
        return 0

    lax.fori_loop(0, n_blk + 2, block, 0)
    for t in range(n_tiles):
        wo_copy(t).start()
        if t == 0:
            hid_copy.start()

    def finish_step(n, _):
        xsend(n).wait_recv()
        finish(n)
        at_copy(n).start()
        return 0
    lax.fori_loop(0, NC, finish_step, 0)

    def p_copy(i):
        return remote(p_buf.at[i], p_recv.at[i], p_s.at[i], p_r.at[i], to_tp)

    def yc_copy(i):
        return remote(y_send.at[i], y_core.at[i], yc_s.at[i], yc_r.at[i], to_core)

    def yx_copy(i):
        return remote(y_send.at[i], y_chip.at[i], yx_s.at[i], yx_r.at[i], to_chip)

    def yf_copy(i):
        return remote(y_chip.at[i], y_fwd.at[i], yf_s.at[i], yf_r.at[i], to_core)

    for n in range(NC):
        at_copy(n).wait_recv()
        for h in range(heads):
            cols = [att[n * 2 + c, pl.ds(h, quarter, stride=heads), :] for c in range(2)]
            lhs[n * 2 * quarter:(n + 1) * 2 * quarter, h * head_dim:(h + 1) * head_dim] = (
                jnp.concatenate(cols, axis=0).astype(jnp.bfloat16))
    hid_copy.wait()
    per = TN // TS

    def project(t, _):
        wo_copy(t).wait()
        res = jnp.dot(lhs[...], wo[t], preferred_element_type=jnp.float32)
        for s in range(per):
            i = t * per + s
            p_buf[i] = res[:, s * TS:(s + 1) * TS]
            p_copy(i).start()
        return 0

    def out_cols(i, on_core):
        return pl.ds(pl.multiple_of(on_core * half + i * TS, TS), TS)

    def out_rows(on_chip):
        return pl.ds(pl.multiple_of(on_chip * chip_rows, chip_rows), chip_rows)

    def y_tile(i):
        p_copy(i).wait_recv()
        res = hid[:, pl.ds(pl.multiple_of(i * TS, TS), TS)].astype(jnp.float32)
        y = (res + (p_buf[i] + p_recv[i])).astype(jnp.bfloat16)
        y_send[i] = y.astype(jnp.float32)
        y_ref[out_rows(chip), out_cols(i, core)] = y
        yx_copy(i).start()
        yc_copy(i).start()

    def y_from_chip(i):
        yx_copy(i).wait_recv()
        yf_copy(i).start()
        y_ref[out_rows(1 - chip), out_cols(i, core)] = y_chip[i].astype(jnp.bfloat16)
        yc_copy(i).wait_recv()
        y_ref[out_rows(chip), out_cols(i, 1 - core)] = y_core[i].astype(jnp.bfloat16)

    def y_from_fwd(i):
        yf_copy(i).wait_recv()
        y_ref[out_rows(1 - chip), out_cols(i, 1 - core)] = y_fwd[i].astype(jnp.bfloat16)

    total = n_tiles * per
    lead = 2
    for t in range(lead):
        project(t, 0)
    lag, lag2 = 2, 3

    def step(i, _):
        @pl.when(jnp.logical_and(i % per == 0, i // per + lead < n_tiles))
        def _():
            project(i // per + lead, 0)

        @pl.when(i < total)
        def _():
            y_tile(i)

        @pl.when(jnp.logical_and(i >= lag, i < total + lag))
        def _():
            y_from_chip(i - lag)

        @pl.when(i >= lag2)
        def _():
            y_from_fwd(i - lag2)
        return 0
    lax.fori_loop(0, total + lag2, step, 0)

    for t in range(n_q):
        q_copy(t).wait_send()
    for k in range(2 * NC):
        d2d(k).wait_send()
    for n in range(NC):
        xsend(n).wait_send()
        at_copy(n).wait_send()

    def drain(i, _):
        p_copy(i).wait_send()
        yc_copy(i).wait_send()
        yx_copy(i).wait_send()
        yf_copy(i).wait_send()
        return 0
    lax.fori_loop(0, total, drain, 0)


def attention(seq_lens, cos_t, sin_t, norm_w, b_q, b_k, b_v, hidden, w_q, w_k, w_v, k_cache, v_cache, w_o):
    n_rows, d_model = hidden.shape
    s_dev, head_dim = k_cache.shape[1], k_cache.shape[2]
    heads = w_q.shape[1] // head_dim
    half = d_model // 2
    n_tiles = half // TN
    n_q = w_q.shape[1] // (2 * TN)
    quarter = n_rows // (4 * NC)
    msg = quarter * heads + 2 * heads
    total = half // TS
    vmem = pl.BlockSpec(memory_space=pltpu.VMEM)
    hbm = pl.BlockSpec(memory_space=pl.ANY)
    f32, bf16 = jnp.float32, jnp.bfloat16
    dma = pltpu.SemaphoreType.DMA
    tile_f32 = pltpu.VMEM((total, n_rows // 2, TS), f32)
    return pl.pallas_call(
        attn_kernel,
        out_shape=[jax.ShapeDtypeStruct((n_rows, d_model), bf16)] + [jax.ShapeDtypeStruct((n_rows, head_dim), bf16)] * 2,
        in_specs=[pl.BlockSpec(memory_space=pltpu.SMEM)] + [vmem] * 6 + [hbm] * 7,
        out_specs=[vmem] * 3,
        scratch_shapes=[
            pltpu.VMEM((n_rows * heads, head_dim), f32),
            pltpu.VMEM((n_q, n_rows * TN // head_dim, head_dim), f32),
            pltpu.VMEM((n_q, n_rows * TN // head_dim, head_dim), f32),
            pltpu.VMEM((d_model, 2 * head_dim), bf16),
            pltpu.VMEM((heads, head_dim), f32),
            pltpu.VMEM((n_rows, head_dim), f32), pltpu.VMEM((n_rows, head_dim), f32),
            dma, dma((2,)), dma((n_q,)), dma((n_q,)),
            pltpu.VMEM((NC * 4, msg, head_dim), f32),
            pltpu.VMEM((NC * 2, msg, head_dim), f32),
            pltpu.VMEM((NC, msg, head_dim), f32),
            pltpu.VMEM((NC * 2, quarter * heads, head_dim), f32),
            pltpu.VMEM((n_rows // 2, heads * head_dim), bf16),
            pltpu.VMEM((BR // 2, 2 * heads, s_dev), f32),
            pltpu.VMEM((BR // 2, 2 * heads, s_dev), bf16),
            pltpu.VMEM((NC, heads, head_dim), f32),
            tile_f32, tile_f32, tile_f32, tile_f32, tile_f32, tile_f32,
            pltpu.VMEM((n_tiles, heads * head_dim, TN), bf16),
            pltpu.VMEM((n_rows // 2, half), bf16),
            pltpu.VMEM((NBK, BR, s_dev, head_dim), bf16),
            pltpu.VMEM((NBV, BR, s_dev, head_dim), bf16),
            dma((NBK,)), dma((NBV,)), dma((n_tiles,)), dma,
            dma((NC * 2,)), dma((NC * 2,)), dma((NC,)), dma((NC,)), dma((NC,)), dma((NC,)),
            dma((total,)), dma((total,)), dma((total,)), dma((total,)), dma((total,)), dma((total,)),
            dma((total,)), dma((total,)),
        ],
        compiler_params=pltpu.CompilerParams(
            collective_id=0, has_side_effects=True, vmem_limit_bytes=VMEM_LIMIT),
        name="attend",
    )(seq_lens, cos_t, sin_t, norm_w.reshape(-1, 128), b_q.reshape(heads, head_dim), b_k[None], b_v[None], hidden,
      w_q, w_k, w_v, k_cache, v_cache, w_o)


def copy_kernel(parts, y_in, k_in, v_in, y_out, k_out, v_out, buf, kv_buf, in_sem, out_sem):
    rows = y_in.shape[0] // parts
    pairs = [(y_in.at[pl.ds(p * rows, rows)], buf.at[p], y_out.at[pl.ds(p * rows, rows)]) for p in range(parts)]
    pairs += [(k_in, kv_buf.at[0], k_out), (v_in, kv_buf.at[1], v_out)]
    loads = [pltpu.make_async_copy(a, m, in_sem.at[i]) for i, (a, m, _) in enumerate(pairs)]
    stores = [pltpu.make_async_copy(m, z, out_sem.at[i]) for i, (_, m, z) in enumerate(pairs)]
    for c in loads:
        c.start()
    for c, d in zip(loads, stores):
        c.wait()
        d.start()
    for d in stores:
        d.wait()


def copy_out(y, k, v):
    parts = 8
    hbm = pl.BlockSpec(memory_space=pl.ANY)
    dma = pltpu.SemaphoreType.DMA
    return pl.pallas_call(
        functools.partial(copy_kernel, parts),
        out_shape=[jax.ShapeDtypeStruct(a.shape, a.dtype) for a in (y, k, v)],
        in_specs=[hbm] * 3, out_specs=[hbm] * 3,
        scratch_shapes=[pltpu.VMEM((parts, y.shape[0] // parts, y.shape[1]), y.dtype),
                        pltpu.VMEM((2,) + k.shape, k.dtype), dma((parts + 2,)), dma((parts + 2,))],
        name="copy_out",
    )(y, k, v)


def solution(mesh):
    def device_step(hidden, norm_w, w_q, b_q, w_k, b_k, w_v, b_v, w_o, k_cache, v_cache, positions, seq_lens):
        n_rows = hidden.shape[0]
        s_dev, head_dim = k_cache.shape[1], k_cache.shape[3]
        cos_t, sin_t = rope_tables(positions, head_dim)
        outs = attention(seq_lens, cos_t, sin_t, norm_w, b_q, b_k, b_v, hidden, w_q, w_k, w_v,
                         k_cache.reshape(n_rows, s_dev, head_dim), v_cache.reshape(n_rows, s_dev, head_dim), w_o)
        y_out, kb, vb = copy_out(*outs)
        return y_out, kb.reshape(n_rows, 1, head_dim), vb.reshape(n_rows, 1, head_dim)

    col_spec = P(None, 'tp')
    vec_spec = P('tp')
    cache_spec = P('dp', 'sp', 'tp', None)
    group_spec = P('dp', 'tp', None)
    in_specs = (P('dp', None), P(None), col_spec, vec_spec, col_spec, vec_spec, col_spec, vec_spec,
                P('tp', None), cache_spec, cache_spec, P('dp'), P('dp'))
    out_specs = (P('dp', None), group_spec, group_spec)
    return jax.shard_map(device_step, mesh=mesh, in_specs=in_specs, out_specs=out_specs, check_vma=False)
```

```python
import functools

import jax
import jax.numpy as jnp
from jax import lax
from jax.experimental import pallas as pl
from jax.experimental.pallas import tpu as pltpu
from jax.sharding import PartitionSpec as P

RMS_EPS = 1.5625e-7
ROPE_BASE = 10000.0
LOG2E = 1.4426950408889634
NEG = -3e38
NEG_FLOOR = -1e38
MESH = pl.DeviceIdType.MESH
VMEM_LIMIT = 67_043_328


NORM_ROWS = 32
NC = 2
BR = 8
NBK, NBV = 4, 6
TN = 512
TS = 256


def rope_tables(positions, head_dim):
    rot_dim = head_dim // 2
    lane = jnp.arange(head_dim, dtype=jnp.int32)
    freq = ROPE_BASE ** (-2.0 * (lane // 2).astype(jnp.float32) / rot_dim)
    freq = jnp.where(lane < rot_dim, freq, 0.0)
    angles = positions.astype(jnp.float32)[:, None] * freq
    sign = jnp.where(lane % 2 == 0, -1.0, 1.0)
    return jnp.cos(angles), jnp.sin(angles) * sign


def rope(x, cos_t, sin_t, even):
    width = x.shape[-1]
    swapped = jnp.where(even, pltpu.roll(x, width - 1, 1), pltpu.roll(x, 1, 1))
    return (x * cos_t + swapped * sin_t).astype(jnp.bfloat16).astype(jnp.float32)


def attn_kernel(seq_ref, cos_ref, sin_ref, nw_ref, bq_ref, bk_ref, bv_ref, hid_hbm, wq_hbm, wk_hbm, wv_hbm,
                k_hbm, v_hbm, wo_hbm, y_ref, kb_ref, vb_ref,
                q_ref, q_send, q_recv, wkv, bqf, kf_ref, vf_ref, in_sem, wkv_sem, q_s, q_r, o_buf, rd, rx, att, lhs, s_sc, p_sc, new_sc, p_buf, p_recv, y_send, y_core, y_chip, y_fwd, wo, hid,
                kbuf, vbuf, k_sem, v_sem, wo_sem, hid_sem, rd_s, rd_r, rx_s, rx_r, at_s, at_r, p_s, p_r,
                yc_s, yc_r, yx_s, yx_r, yf_s, yf_r):
    n_rows, d_model = y_ref.shape
    s_dev, head_dim = kbuf.shape[2], kbuf.shape[3]
    heads = q_ref.shape[0] // n_rows
    n_tiles = wo.shape[0]
    half = n_tiles * TN
    quarter = n_rows // (4 * NC)
    o_rows = quarter * heads
    chip_rows = n_rows // 2
    bq = quarter // BR
    n_blk = n_rows // BR
    coef = head_dim ** -0.5 * LOG2E

    dp, tp, sp = lax.axis_index("dp"), lax.axis_index("tp"), lax.axis_index("sp")
    chip, core = sp // 2, sp % 2
    to_core = (dp, tp, 2 * chip + (1 - core))
    to_chip = (dp, tp, 2 * (1 - chip) + core)
    to_tp = (dp, 1 - tp, sp)

    def remote(src, dst, s_sem, r_sem, dev):
        return pltpu.make_async_remote_copy(src_ref=src, dst_ref=dst, send_sem=s_sem, recv_sem=r_sem,
                                            device_id=dev, device_id_type=MESH)

    def group_row(u):
        near = u // (2 * NC)
        own = u % 2
        n = (u % (2 * NC)) // 2
        on_chip = near * chip + (1 - near) * (1 - chip)
        on_core = own * core + (1 - own) * (1 - core)
        return on_chip * chip_rows + n * 2 * quarter + on_core * quarter

    def block_row(b):
        return pl.multiple_of(group_row(b // bq) + (b % bq) * BR, BR)

    def k_copy(b):
        return pltpu.make_async_copy(k_hbm.at[pl.ds(block_row(b), BR)], kbuf.at[b % NBK], k_sem.at[b % NBK])

    def v_copy(b):
        return pltpu.make_async_copy(v_hbm.at[pl.ds(block_row(b), BR)], vbuf.at[b % NBV], v_sem.at[b % NBV])

    def wo_copy(t):
        cols = pl.ds(pl.multiple_of(core * half + t * TN, 128), TN)
        return pltpu.make_async_copy(wo_hbm.at[:, cols], wo.at[t], wo_sem.at[t])

    hid_copy = pltpu.make_async_copy(
        hid_hbm.at[pl.ds(pl.multiple_of(chip * chip_rows, 128), chip_rows),
                   pl.ds(pl.multiple_of(core * half, 128), half)], hid, hid_sem)

    n_q = q_send.shape[0]
    tile_heads = TN // head_dim
    k_half = wo.shape[1]

    def in_copy(i):
        rows = pl.ds(pl.multiple_of(i * NORM_ROWS, NORM_ROWS), NORM_ROWS)
        return pltpu.make_async_copy(hid_hbm.at[rows], y_ref.at[rows], in_sem.at[i])

    wk_copy = pltpu.make_async_copy(wk_hbm, wkv.at[:, :head_dim], wkv_sem.at[0])
    wv_copy = pltpu.make_async_copy(wv_hbm, wkv.at[:, head_dim:], wkv_sem.at[1])

    def wq_copy(i):
        cols = pl.ds(pl.multiple_of((core * n_q + i // 2) * TN, TN), TN)
        return pltpu.make_async_copy(wq_hbm.at[pl.ds((i % 2) * k_half, k_half), cols], wo.at[i], wo_sem.at[i])

    n_norm = n_rows // NORM_ROWS
    for i in range(n_norm):
        in_copy(i).start()

    barrier = pltpu.get_barrier_semaphore()
    for dev in (to_core, to_chip, to_tp):
        pl.semaphore_signal(barrier, inc=1, device_id=dev, device_id_type=MESH)

    bqf[...] = bq_ref[...].astype(jnp.float32)

    def norm_rows(i, _):
        rows = pl.ds(pl.multiple_of(i * NORM_ROWS, NORM_ROWS), NORM_ROWS)
        in_copy(i).wait()

        @pl.when(i < 2 * n_q)
        def _():
            wq_copy(i).start()

        @pl.when(i == n_norm - 1)
        def _():
            wk_copy.start()
            wv_copy.start()
        sq = jnp.zeros((NORM_ROWS, 128), jnp.float32)
        for c in range(d_model // 128):
            x = y_ref[rows, c * 128:(c + 1) * 128].astype(jnp.float32)
            sq = sq + x * x
        inv = lax.rsqrt(jnp.sum(sq, axis=-1, keepdims=True) / d_model + RMS_EPS)
        for c in range(d_model // 128):
            x = y_ref[rows, c * 128:(c + 1) * 128].astype(jnp.float32)
            x = x * inv * nw_ref[c:c + 1, :].astype(jnp.float32)
            y_ref[rows, c * 128:(c + 1) * 128] = x.astype(jnp.bfloat16)
        return 0
    lax.fori_loop(0, n_norm, norm_rows, 0)
    pl.semaphore_wait(barrier, 3)

    even = lax.broadcasted_iota(jnp.int32, (n_rows, head_dim), 1) % 2 == 0

    def round_f32(x):
        return x.astype(jnp.bfloat16).astype(jnp.float32)

    def q_copy(t):
        return remote(q_send.at[t], q_recv.at[t], q_s.at[t], q_r.at[t], to_core)

    def q_tile(t, _):
        wq_copy(2 * t).wait()
        wq_copy(2 * t + 1).wait()

        @pl.when(t == n_q - 1)
        def _():
            for b in range(NBV):
                if b < NBK:
                    k_copy(b).start()
                v_copy(b).start()
        acc = jnp.dot(y_ref[:, :k_half], wo[2 * t], preferred_element_type=jnp.float32)
        acc = acc + jnp.dot(y_ref[:, k_half:], wo[2 * t + 1], preferred_element_type=jnp.float32)
        for h in range(tile_heads):
            head = core * (heads // 2) + t * tile_heads + h
            val = round_f32(acc[:, h * head_dim:(h + 1) * head_dim] + bqf[pl.ds(head, 1), :])
            val = rope(val, cos_ref[...], sin_ref[...], even)
            q_ref[pl.ds(head, n_rows, stride=heads), :] = val
            q_send[t, pl.ds(h, n_rows, stride=tile_heads), :] = val
        q_copy(t).start()
        return 0
    lax.fori_loop(0, n_q, q_tile, 0)

    wk_copy.wait()
    wv_copy.wait()
    kv = jnp.dot(y_ref[...], wkv[...], preferred_element_type=jnp.float32)
    k_rot = rope(round_f32(kv[:, :head_dim] + bk_ref[...].astype(jnp.float32)), cos_ref[...], sin_ref[...], even)
    kf_ref[...] = k_rot
    kb_ref[...] = k_rot.astype(jnp.bfloat16)
    v_val = round_f32(kv[:, head_dim:] + bv_ref[...].astype(jnp.float32))
    vf_ref[...] = v_val
    vb_ref[...] = v_val.astype(jnp.bfloat16)

    def q_take(t, _):
        q_copy(t).wait_recv()
        for h in range(tile_heads):
            head = (1 - core) * (heads // 2) + t * tile_heads + h
            q_ref[pl.ds(head, n_rows, stride=heads), :] = q_recv[t, pl.ds(h, n_rows, stride=tile_heads), :]
        return 0
    lax.fori_loop(0, n_q, q_take, 0)

    lane = lax.broadcasted_iota(jnp.int32, (heads, head_dim), 1)
    pos = lax.broadcasted_iota(jnp.int32, (heads, s_dev), 1) + sp * s_dev
    zeros_q = jnp.zeros((heads, head_dim), jnp.float32)

    def q_rows(row):
        return q_ref[pl.ds(pl.multiple_of(row * heads, 8), heads), :]

    def new_scores(n):
        row0 = chip * chip_rows + n * 2 * quarter + core * quarter

        def rows8(g, acc):
            base = pl.multiple_of(row0 + g * 8, 8)
            k_new = kf_ref[pl.ds(base, 8), :]
            for r in range(8):
                s_new = jnp.sum(q_rows(base + r) * k_new[r:r + 1], axis=-1, keepdims=True)
                acc = jnp.where(lane == g * 8 + r, s_new, acc)
            return acc
        new_sc[n] = lax.fori_loop(0, quarter // 8, rows8, zeros_q)

    for n in range(NC):
        new_scores(n)

    def column(vals, j):
        return jnp.broadcast_to(vals[:, j:j + 1], (heads, head_dim))

    def d2d(k):
        return remote(o_buf.at[2 * k], rd.at[k], rd_s.at[k], rd_r.at[k], to_core)

    def xsend(n):
        return remote(o_buf.at[2 * n + 1], rx.at[n], rx_s.at[n], rx_r.at[n], to_chip)

    def at_copy(n):
        return remote(att.at[n * 2 + core], att.at[n * 2 + core], at_s.at[n], at_r.at[n], to_core)

    def merge_core(u):
        k = u // 2
        m1 = o_buf[u, o_rows:o_rows + heads, :]
        l1 = o_buf[u, o_rows + heads:o_rows + 2 * heads, :]
        m2 = rd[k, o_rows:o_rows + heads, :]
        l2 = rd[k, o_rows + heads:o_rows + 2 * heads, :]
        m = jnp.maximum(m1, m2)
        f1 = jnp.exp2((m1 - m) * coef)
        f2 = jnp.exp2((m2 - m) * coef)
        o_buf[u, o_rows:o_rows + heads, :] = m
        o_buf[u, o_rows + heads:o_rows + 2 * heads, :] = l1 * f1 + l2 * f2

        for j in range(quarter):
            rows = pl.ds(j * heads, heads)
            o_buf[u, rows, :] = o_buf[u, rows, :] * column(f1, j) + rd[k, rows, :] * column(f2, j)

    def finish(n):
        u = 2 * NC + 2 * n + 1
        row0 = chip * chip_rows + n * 2 * quarter + core * quarter
        m1 = o_buf[u, o_rows:o_rows + heads, :]
        l1 = o_buf[u, o_rows + heads:o_rows + 2 * heads, :]
        m2 = rx[n, o_rows:o_rows + heads, :]
        l2 = rx[n, o_rows + heads:o_rows + 2 * heads, :]
        m3 = new_sc[n]
        m = jnp.maximum(jnp.maximum(m1, m2), m3)
        f1 = jnp.exp2((m1 - m) * coef)
        f2 = jnp.exp2((m2 - m) * coef)
        f3 = jnp.exp2((m3 - m) * coef)
        l = l1 * f1 + l2 * f2 + f3
        f1, f2, f3 = f1 / l, f2 / l, f3 / l

        for j in range(quarter):
            if j % 8 == 0:
                v_new = vf_ref[pl.ds(pl.multiple_of(row0 + j, 8), 8), :]
            rows = pl.ds(j * heads, heads)
            o = o_buf[u, rows, :] * column(f1, j) + rx[n, rows, :] * column(f2, j)
            o = o + column(f3, j) * v_new[j % 8:j % 8 + 1]
            att[n * 2 + core, rows, :] = round_f32(o)

    def block(b, _):
        @pl.when(b < n_blk)
        def _():
            k_copy(b).wait()

        b1 = jnp.minimum(b, n_blk - 1)
        b2 = jnp.clip(b - 1, 0, n_blk - 1)
        b3 = jnp.clip(b - 2, 0, n_blk - 1)

        @pl.when(jnp.logical_or(b == 0, b >= 3))
        def _():
            v_copy(b3).wait()

        u3, vslot = b3 // bq, b3 % NBV
        for pair in range(BR // 2):
            r = 2 * pair
            v_pair = jnp.concatenate([vbuf[vslot, r], vbuf[vslot, r + 1]], axis=1)
            o_pair = jnp.dot(p_sc[pair], v_pair, preferred_element_type=jnp.float32)
            for i in range(2):
                o = o_pair[i * heads:(i + 1) * heads, i * head_dim:(i + 1) * head_dim]
                o_buf[u3, pl.ds(pl.multiple_of(((b3 % bq) * BR + r + i) * heads, 8), heads), :] = o
        u2, row2 = b2 // bq, block_row(b2)
        m_all = o_buf[u2, o_rows:o_rows + heads, :]
        l_all = o_buf[u2, o_rows + heads:o_rows + 2 * heads, :]
        for pair in range(BR // 2):
            p_list = []
            for i in range(2):
                r = 2 * pair + i
                s = s_sc[pair, i * heads:(i + 1) * heads, :]
                s = jnp.where(pos < seq_ref[row2 + r], s, NEG)
                m = jnp.maximum(jnp.max(s, axis=-1, keepdims=True), NEG_FLOOR)
                p = jnp.exp2((s - m) * coef)
                l = jnp.sum(p, axis=-1, keepdims=True)
                here = lane == (b2 % bq) * BR + r
                m_all = jnp.where(here, m, m_all)
                l_all = jnp.where(here, l, l_all)
                p_list.append(p)
            p_sc[pair] = jnp.concatenate(p_list, axis=0).astype(jnp.bfloat16)
        o_buf[u2, o_rows:o_rows + heads, :] = m_all
        o_buf[u2, o_rows + heads:o_rows + 2 * heads, :] = l_all
        row1, kslot = block_row(b1), b1 % NBK
        for pair in range(BR // 2):
            r = 2 * pair
            left = jnp.concatenate([q_rows(row1 + r), zeros_q], axis=0)
            right = jnp.concatenate([zeros_q, q_rows(row1 + r + 1)], axis=0)
            q_pair = jnp.concatenate([left, right], axis=1).astype(jnp.bfloat16)
            k_pair = jnp.concatenate([kbuf[kslot, r], kbuf[kslot, r + 1]], axis=1)
            s_sc[pair] = lax.dot_general(q_pair, k_pair, (((1,), (1,)), ((), ())),
                                         preferred_element_type=jnp.float32)

        @pl.when(b + NBK < n_blk)
        def _():
            k_copy(b + NBK).start()

        @pl.when(jnp.logical_and(b >= 2, b - 2 + NBV < n_blk))
        def _():
            v_copy(b - 2 + NBV).start()

        done = jnp.logical_and(b >= 2, (b - 2) % bq == bq - 1)
        u = b3 // bq

        @pl.when(jnp.logical_and(done, u % 2 == 0))
        def _():
            d2d(u // 2).start()

        @pl.when(jnp.logical_and(done, u % 2 == 1))
        def _():
            d2d(u // 2).wait_recv()
            merge_core(u)

            @pl.when(u < 2 * NC)
            def _():
                xsend(u // 2).start()
        return 0

    lax.fori_loop(0, n_blk + 2, block, 0)
    for t in range(n_tiles):
        wo_copy(t).start()
        if t == 0:
            hid_copy.start()

    def finish_step(n, _):
        xsend(n).wait_recv()
        finish(n)
        at_copy(n).start()
        return 0
    lax.fori_loop(0, NC, finish_step, 0)

    def p_copy(i):
        return remote(p_buf.at[i], p_recv.at[i], p_s.at[i], p_r.at[i], to_tp)

    def yc_copy(i):
        return remote(y_send.at[i], y_core.at[i], yc_s.at[i], yc_r.at[i], to_core)

    def yx_copy(i):
        return remote(y_send.at[i], y_chip.at[i], yx_s.at[i], yx_r.at[i], to_chip)

    def yf_copy(i):
        return remote(y_chip.at[i], y_fwd.at[i], yf_s.at[i], yf_r.at[i], to_core)

    for n in range(NC):
        at_copy(n).wait_recv()
        for h in range(heads):
            cols = [att[n * 2 + c, pl.ds(h, quarter, stride=heads), :] for c in range(2)]
            lhs[n * 2 * quarter:(n + 1) * 2 * quarter, h * head_dim:(h + 1) * head_dim] = (
                jnp.concatenate(cols, axis=0).astype(jnp.bfloat16))
    hid_copy.wait()
    per = TN // TS

    def project(t, _):
        wo_copy(t).wait()
        res = jnp.dot(lhs[...], wo[t], preferred_element_type=jnp.float32)
        for s in range(per):
            i = t * per + s
            p_buf[i] = res[:, s * TS:(s + 1) * TS]
            p_copy(i).start()
        return 0

    def out_cols(i, on_core):
        return pl.ds(pl.multiple_of(on_core * half + i * TS, TS), TS)

    def out_rows(on_chip):
        return pl.ds(pl.multiple_of(on_chip * chip_rows, chip_rows), chip_rows)

    def y_tile(i):
        p_copy(i).wait_recv()
        res = hid[:, pl.ds(pl.multiple_of(i * TS, TS), TS)].astype(jnp.float32)
        y = (res + (p_buf[i] + p_recv[i])).astype(jnp.bfloat16)
        y_send[i] = y.astype(jnp.float32)
        y_ref[out_rows(chip), out_cols(i, core)] = y
        yx_copy(i).start()
        yc_copy(i).start()

    def y_from_chip(i):
        yx_copy(i).wait_recv()
        yf_copy(i).start()
        y_ref[out_rows(1 - chip), out_cols(i, core)] = y_chip[i].astype(jnp.bfloat16)
        yc_copy(i).wait_recv()
        y_ref[out_rows(chip), out_cols(i, 1 - core)] = y_core[i].astype(jnp.bfloat16)

    def y_from_fwd(i):
        yf_copy(i).wait_recv()
        y_ref[out_rows(1 - chip), out_cols(i, 1 - core)] = y_fwd[i].astype(jnp.bfloat16)

    total = n_tiles * per
    lead = 2
    for t in range(lead):
        project(t, 0)
    lag, lag2 = 2, 3

    def step(i, _):
        @pl.when(jnp.logical_and(i % per == 0, i // per + lead < n_tiles))
        def _():
            project(i // per + lead, 0)

        @pl.when(i < total)
        def _():
            y_tile(i)

        @pl.when(jnp.logical_and(i >= lag, i < total + lag))
        def _():
            y_from_chip(i - lag)

        @pl.when(i >= lag2)
        def _():
            y_from_fwd(i - lag2)
        return 0
    lax.fori_loop(0, total + lag2, step, 0)

    for t in range(n_q):
        q_copy(t).wait_send()
    for k in range(2 * NC):
        d2d(k).wait_send()
    for n in range(NC):
        xsend(n).wait_send()
        at_copy(n).wait_send()

    def drain(i, _):
        p_copy(i).wait_send()
        yc_copy(i).wait_send()
        yx_copy(i).wait_send()
        yf_copy(i).wait_send()
        return 0
    lax.fori_loop(0, total, drain, 0)


def attention(seq_lens, cos_t, sin_t, norm_w, b_q, b_k, b_v, hidden, w_q, w_k, w_v, k_cache, v_cache, w_o):
    n_rows, d_model = hidden.shape
    s_dev, head_dim = k_cache.shape[1], k_cache.shape[2]
    heads = w_q.shape[1] // head_dim
    half = d_model // 2
    n_tiles = half // TN
    n_q = w_q.shape[1] // (2 * TN)
    quarter = n_rows // (4 * NC)
    msg = quarter * heads + 2 * heads
    total = half // TS
    vmem = pl.BlockSpec(memory_space=pltpu.VMEM)
    hbm = pl.BlockSpec(memory_space=pl.ANY)
    f32, bf16 = jnp.float32, jnp.bfloat16
    dma = pltpu.SemaphoreType.DMA
    tile_f32 = pltpu.VMEM((total, n_rows // 2, TS), f32)
    return pl.pallas_call(
        attn_kernel,
        out_shape=[jax.ShapeDtypeStruct((n_rows, d_model), bf16)] + [jax.ShapeDtypeStruct((n_rows, head_dim), bf16)] * 2,
        in_specs=[pl.BlockSpec(memory_space=pltpu.SMEM)] + [vmem] * 6 + [hbm] * 7,
        out_specs=[vmem] * 3,
        scratch_shapes=[
            pltpu.VMEM((n_rows * heads, head_dim), f32),
            pltpu.VMEM((n_q, n_rows * TN // head_dim, head_dim), f32),
            pltpu.VMEM((n_q, n_rows * TN // head_dim, head_dim), f32),
            pltpu.VMEM((d_model, 2 * head_dim), bf16),
            pltpu.VMEM((heads, head_dim), f32),
            pltpu.VMEM((n_rows, head_dim), f32), pltpu.VMEM((n_rows, head_dim), f32),
            dma((n_rows // NORM_ROWS,)), dma((2,)), dma((n_q,)), dma((n_q,)),
            pltpu.VMEM((NC * 4, msg, head_dim), f32),
            pltpu.VMEM((NC * 2, msg, head_dim), f32),
            pltpu.VMEM((NC, msg, head_dim), f32),
            pltpu.VMEM((NC * 2, quarter * heads, head_dim), f32),
            pltpu.VMEM((n_rows // 2, heads * head_dim), bf16),
            pltpu.VMEM((BR // 2, 2 * heads, s_dev), f32),
            pltpu.VMEM((BR // 2, 2 * heads, s_dev), bf16),
            pltpu.VMEM((NC, heads, head_dim), f32),
            tile_f32, tile_f32, tile_f32, tile_f32, tile_f32, tile_f32,
            pltpu.VMEM((n_tiles, heads * head_dim, TN), bf16),
            pltpu.VMEM((n_rows // 2, half), bf16),
            pltpu.VMEM((NBK, BR, s_dev, head_dim), bf16),
            pltpu.VMEM((NBV, BR, s_dev, head_dim), bf16),
            dma((NBK,)), dma((NBV,)), dma((n_tiles,)), dma,
            dma((NC * 2,)), dma((NC * 2,)), dma((NC,)), dma((NC,)), dma((NC,)), dma((NC,)),
            dma((total,)), dma((total,)), dma((total,)), dma((total,)), dma((total,)), dma((total,)),
            dma((total,)), dma((total,)),
        ],
        compiler_params=pltpu.CompilerParams(
            collective_id=0, has_side_effects=True, vmem_limit_bytes=VMEM_LIMIT),
        name="attend",
    )(seq_lens, cos_t, sin_t, norm_w.reshape(-1, 128), b_q.reshape(heads, head_dim), b_k[None], b_v[None], hidden,
      w_q, w_k, w_v, k_cache, v_cache, w_o)


def copy_kernel(parts, y_in, k_in, v_in, y_out, k_out, v_out, buf, kv_buf, in_sem, out_sem):
    rows = y_in.shape[0] // parts
    pairs = [(y_in.at[pl.ds(p * rows, rows)], buf.at[p], y_out.at[pl.ds(p * rows, rows)]) for p in range(parts)]
    pairs += [(k_in, kv_buf.at[0], k_out), (v_in, kv_buf.at[1], v_out)]
    loads = [pltpu.make_async_copy(a, m, in_sem.at[i]) for i, (a, m, _) in enumerate(pairs)]
    stores = [pltpu.make_async_copy(m, z, out_sem.at[i]) for i, (_, m, z) in enumerate(pairs)]
    for c in loads:
        c.start()
    for c, d in zip(loads, stores):
        c.wait()
        d.start()
    for d in stores:
        d.wait()


def copy_out(y, k, v):
    parts = 8
    hbm = pl.BlockSpec(memory_space=pl.ANY)
    dma = pltpu.SemaphoreType.DMA
    return pl.pallas_call(
        functools.partial(copy_kernel, parts),
        out_shape=[jax.ShapeDtypeStruct(a.shape, a.dtype) for a in (y, k, v)],
        in_specs=[hbm] * 3, out_specs=[hbm] * 3,
        scratch_shapes=[pltpu.VMEM((parts, y.shape[0] // parts, y.shape[1]), y.dtype),
                        pltpu.VMEM((2,) + k.shape, k.dtype), dma((parts + 2,)), dma((parts + 2,))],
        name="copy_out",
    )(y, k, v)


def solution(mesh):
    def device_step(hidden, norm_w, w_q, b_q, w_k, b_k, w_v, b_v, w_o, k_cache, v_cache, positions, seq_lens):
        n_rows = hidden.shape[0]
        s_dev, head_dim = k_cache.shape[1], k_cache.shape[3]
        cos_t, sin_t = rope_tables(positions, head_dim)
        outs = attention(seq_lens, cos_t, sin_t, norm_w, b_q, b_k, b_v, hidden, w_q, w_k, w_v,
                         k_cache.reshape(n_rows, s_dev, head_dim), v_cache.reshape(n_rows, s_dev, head_dim), w_o)
        y_out, kb, vb = copy_out(*outs)
        return y_out, kb.reshape(n_rows, 1, head_dim), vb.reshape(n_rows, 1, head_dim)

    col_spec = P(None, 'tp')
    vec_spec = P('tp')
    cache_spec = P('dp', 'sp', 'tp', None)
    group_spec = P('dp', 'tp', None)
    in_specs = (P('dp', None), P(None), col_spec, vec_spec, col_spec, vec_spec, col_spec, vec_spec,
                P('tp', None), cache_spec, cache_spec, P('dp'), P('dp'))
    out_specs = (P('dp', None), group_spec, group_spec)
    return jax.shard_map(device_step, mesh=mesh, in_specs=in_specs, out_specs=out_specs, check_vma=False)
```

```python
import functools

import jax
import jax.numpy as jnp
from jax import lax
from jax.experimental import pallas as pl
from jax.experimental.pallas import tpu as pltpu
from jax.sharding import PartitionSpec as P

RMS_EPS = 1.5625e-7
ROPE_BASE = 10000.0
LOG2E = 1.4426950408889634
NEG = -3e38
NEG_FLOOR = -1e38
MESH = pl.DeviceIdType.MESH
VMEM_LIMIT = 67_043_328


NORM_ROWS = 32
NC = 2
BR = 8
NBK, NBV = 4, 6
TN = 512
TS = 256


def rope_tables(positions, head_dim):
    rot_dim = head_dim // 2
    lane = jnp.arange(head_dim, dtype=jnp.int32)
    freq = ROPE_BASE ** (-2.0 * (lane // 2).astype(jnp.float32) / rot_dim)
    freq = jnp.where(lane < rot_dim, freq, 0.0)
    angles = positions.astype(jnp.float32)[:, None] * freq
    sign = jnp.where(lane % 2 == 0, -1.0, 1.0)
    return jnp.cos(angles), jnp.sin(angles) * sign


def rope(x, cos_t, sin_t, even):
    width = x.shape[-1]
    swapped = jnp.where(even, pltpu.roll(x, width - 1, 1), pltpu.roll(x, 1, 1))
    return (x * cos_t + swapped * sin_t).astype(jnp.bfloat16).astype(jnp.float32)


def attn_kernel(seq_ref, cos_ref, sin_ref, nw_ref, bq_ref, bk_ref, bv_ref, hid_hbm, wq_hbm, wk_hbm, wv_hbm,
                k_hbm, v_hbm, wo_hbm, y_ref, kb_ref, vb_ref,
                q_ref, q_send, q_recv, wkv, bqf, kf_ref, vf_ref, in_sem, wkv_sem, q_s, q_r, o_buf, rd, rx, att, lhs, s_sc, p_sc, new_sc, p_buf, p_recv, y_send, y_core, y_chip, y_fwd, wo, hid,
                kbuf, vbuf, k_sem, v_sem, wo_sem, hid_sem, rd_s, rd_r, rx_s, rx_r, at_s, at_r, p_s, p_r,
                yc_s, yc_r, yx_s, yx_r, yf_s, yf_r):
    n_rows, d_model = y_ref.shape
    s_dev, head_dim = kbuf.shape[2], kbuf.shape[3]
    heads = q_ref.shape[0] // n_rows
    n_tiles = wo.shape[0]
    half = n_tiles * TN
    quarter = n_rows // (4 * NC)
    o_rows = quarter * heads
    chip_rows = n_rows // 2
    bq = quarter // BR
    n_blk = n_rows // BR
    coef = head_dim ** -0.5 * LOG2E

    dp, tp, sp = lax.axis_index("dp"), lax.axis_index("tp"), lax.axis_index("sp")
    chip, core = sp // 2, sp % 2
    to_core = (dp, tp, 2 * chip + (1 - core))
    to_chip = (dp, tp, 2 * (1 - chip) + core)
    to_tp = (dp, 1 - tp, sp)

    def remote(src, dst, s_sem, r_sem, dev):
        return pltpu.make_async_remote_copy(src_ref=src, dst_ref=dst, send_sem=s_sem, recv_sem=r_sem,
                                            device_id=dev, device_id_type=MESH)

    def group_row(u):
        near = u // (2 * NC)
        own = u % 2
        n = (u % (2 * NC)) // 2
        on_chip = near * chip + (1 - near) * (1 - chip)
        on_core = own * core + (1 - own) * (1 - core)
        return on_chip * chip_rows + n * 2 * quarter + on_core * quarter

    def block_row(b):
        return pl.multiple_of(group_row(b // bq) + (b % bq) * BR, BR)

    def k_copy(b):
        return pltpu.make_async_copy(k_hbm.at[pl.ds(block_row(b), BR)], kbuf.at[b % NBK], k_sem.at[b % NBK])

    def v_copy(b):
        return pltpu.make_async_copy(v_hbm.at[pl.ds(block_row(b), BR)], vbuf.at[b % NBV], v_sem.at[b % NBV])

    def wo_copy(t):
        cols = pl.ds(pl.multiple_of(core * half + t * TN, 128), TN)
        return pltpu.make_async_copy(wo_hbm.at[:, cols], wo.at[t], wo_sem.at[t])

    hid_copy = pltpu.make_async_copy(
        hid_hbm.at[pl.ds(pl.multiple_of(chip * chip_rows, 128), chip_rows),
                   pl.ds(pl.multiple_of(core * half, 128), half)], hid, hid_sem)

    n_q = q_send.shape[0]
    tile_heads = TN // head_dim
    k_half = wo.shape[1]

    def in_copy(i):
        rows = pl.ds(pl.multiple_of(i * NORM_ROWS, NORM_ROWS), NORM_ROWS)
        return pltpu.make_async_copy(hid_hbm.at[rows], y_ref.at[rows], in_sem.at[i])

    wk_copy = pltpu.make_async_copy(wk_hbm, wkv.at[:, :head_dim], wkv_sem.at[0])
    wv_copy = pltpu.make_async_copy(wv_hbm, wkv.at[:, head_dim:], wkv_sem.at[1])

    def wq_copy(i):
        cols = pl.ds(pl.multiple_of((core * n_q + i // 2) * TN, TN), TN)
        return pltpu.make_async_copy(wq_hbm.at[pl.ds((i % 2) * k_half, k_half), cols], wo.at[i], wo_sem.at[i])

    n_norm = n_rows // NORM_ROWS
    for i in range(n_norm):
        in_copy(i).start()

    barrier = pltpu.get_barrier_semaphore()
    for dev in (to_core, to_chip, to_tp):
        pl.semaphore_signal(barrier, inc=1, device_id=dev, device_id_type=MESH)

    bqf[...] = bq_ref[...].astype(jnp.float32)

    def norm_rows(i, _):
        rows = pl.ds(pl.multiple_of(i * NORM_ROWS, NORM_ROWS), NORM_ROWS)
        in_copy(i).wait()

        @pl.when(i < 2 * n_q)
        def _():
            wq_copy(i).start()

        @pl.when(i == n_norm - 1)
        def _():
            wk_copy.start()
            wv_copy.start()
        sq = jnp.zeros((NORM_ROWS, 128), jnp.float32)
        for c in range(d_model // 128):
            x = y_ref[rows, c * 128:(c + 1) * 128].astype(jnp.float32)
            sq = sq + x * x
        inv = lax.rsqrt(jnp.sum(sq, axis=-1, keepdims=True) / d_model + RMS_EPS)
        for c in range(d_model // 128):
            x = y_ref[rows, c * 128:(c + 1) * 128].astype(jnp.float32)
            x = x * inv * nw_ref[c:c + 1, :].astype(jnp.float32)
            y_ref[rows, c * 128:(c + 1) * 128] = x.astype(jnp.bfloat16)
        return 0
    lax.fori_loop(0, n_norm, norm_rows, 0)
    pl.semaphore_wait(barrier, 3)

    even = lax.broadcasted_iota(jnp.int32, (n_rows, head_dim), 1) % 2 == 0

    def round_f32(x):
        return x.astype(jnp.bfloat16).astype(jnp.float32)

    def q_copy(t):
        return remote(q_send.at[t], q_recv.at[t], q_s.at[t], q_r.at[t], to_core)

    def q_tile(t, _):
        wq_copy(2 * t).wait()
        wq_copy(2 * t + 1).wait()

        @pl.when(t == n_q - 1)
        def _():
            for b in range(NBV):
                if b < NBK:
                    k_copy(b).start()
                v_copy(b).start()
        acc = jnp.dot(y_ref[:, :k_half], wo[2 * t], preferred_element_type=jnp.float32)
        acc = acc + jnp.dot(y_ref[:, k_half:], wo[2 * t + 1], preferred_element_type=jnp.float32)
        for h in range(tile_heads):
            head = core * (heads // 2) + t * tile_heads + h
            val = round_f32(acc[:, h * head_dim:(h + 1) * head_dim] + bqf[pl.ds(head, 1), :])
            val = rope(val, cos_ref[...], sin_ref[...], even)
            q_ref[pl.ds(head, n_rows, stride=heads), :] = val
            q_send[t, pl.ds(h, n_rows, stride=tile_heads), :] = val
        q_copy(t).start()
        return 0
    lax.fori_loop(0, n_q, q_tile, 0)

    wk_copy.wait()
    wv_copy.wait()
    kv = jnp.dot(y_ref[...], wkv[...], preferred_element_type=jnp.float32)
    k_rot = rope(round_f32(kv[:, :head_dim] + bk_ref[...].astype(jnp.float32)), cos_ref[...], sin_ref[...], even)
    kf_ref[...] = k_rot
    kb_ref[...] = k_rot.astype(jnp.bfloat16)
    v_val = round_f32(kv[:, head_dim:] + bv_ref[...].astype(jnp.float32))
    vf_ref[...] = v_val
    vb_ref[...] = v_val.astype(jnp.bfloat16)

    def q_take(t, _):
        q_copy(t).wait_recv()
        for h in range(tile_heads):
            head = (1 - core) * (heads // 2) + t * tile_heads + h
            q_ref[pl.ds(head, n_rows, stride=heads), :] = q_recv[t, pl.ds(h, n_rows, stride=tile_heads), :]
        return 0
    lax.fori_loop(0, n_q, q_take, 0)

    lane = lax.broadcasted_iota(jnp.int32, (heads, head_dim), 1)
    pos = lax.broadcasted_iota(jnp.int32, (heads, s_dev), 1) + sp * s_dev
    zeros_q = jnp.zeros((heads, head_dim), jnp.float32)

    def q_rows(row):
        return q_ref[pl.ds(pl.multiple_of(row * heads, 8), heads), :]

    def new_scores(n):
        row0 = chip * chip_rows + n * 2 * quarter + core * quarter

        def rows8(g, acc):
            base = pl.multiple_of(row0 + g * 8, 8)
            k_new = kf_ref[pl.ds(base, 8), :]
            for r in range(8):
                s_new = jnp.sum(q_rows(base + r) * k_new[r:r + 1], axis=-1, keepdims=True)
                acc = jnp.where(lane == g * 8 + r, s_new, acc)
            return acc
        new_sc[n] = lax.fori_loop(0, quarter // 8, rows8, zeros_q)

    for n in range(NC):
        new_scores(n)

    def column(vals, j):
        return jnp.broadcast_to(vals[:, j:j + 1], (heads, head_dim))

    def d2d(k):
        return remote(o_buf.at[2 * k], rd.at[k], rd_s.at[k], rd_r.at[k], to_core)

    def xsend(n):
        return remote(o_buf.at[2 * n + 1], rx.at[n], rx_s.at[n], rx_r.at[n], to_chip)

    def at_copy(n):
        return remote(att.at[n * 2 + core], att.at[n * 2 + core], at_s.at[n], at_r.at[n], to_core)

    def merge_core(u):
        k = u // 2
        m1 = o_buf[u, o_rows:o_rows + heads, :]
        l1 = o_buf[u, o_rows + heads:o_rows + 2 * heads, :]
        m2 = rd[k, o_rows:o_rows + heads, :]
        l2 = rd[k, o_rows + heads:o_rows + 2 * heads, :]
        m = jnp.maximum(m1, m2)
        f1 = jnp.exp2((m1 - m) * coef)
        f2 = jnp.exp2((m2 - m) * coef)
        o_buf[u, o_rows:o_rows + heads, :] = m
        o_buf[u, o_rows + heads:o_rows + 2 * heads, :] = l1 * f1 + l2 * f2

        for j in range(quarter):
            rows = pl.ds(j * heads, heads)
            o_buf[u, rows, :] = o_buf[u, rows, :] * column(f1, j) + rd[k, rows, :] * column(f2, j)

    def finish(n):
        u = 2 * NC + 2 * n + 1
        row0 = chip * chip_rows + n * 2 * quarter + core * quarter
        m1 = o_buf[u, o_rows:o_rows + heads, :]
        l1 = o_buf[u, o_rows + heads:o_rows + 2 * heads, :]
        m2 = rx[n, o_rows:o_rows + heads, :]
        l2 = rx[n, o_rows + heads:o_rows + 2 * heads, :]
        m3 = new_sc[n]
        m = jnp.maximum(jnp.maximum(m1, m2), m3)
        f1 = jnp.exp2((m1 - m) * coef)
        f2 = jnp.exp2((m2 - m) * coef)
        f3 = jnp.exp2((m3 - m) * coef)
        l = l1 * f1 + l2 * f2 + f3
        f1, f2, f3 = f1 / l, f2 / l, f3 / l

        for j in range(quarter):
            if j % 8 == 0:
                v_new = vf_ref[pl.ds(pl.multiple_of(row0 + j, 8), 8), :]
            rows = pl.ds(j * heads, heads)
            o = o_buf[u, rows, :] * column(f1, j) + rx[n, rows, :] * column(f2, j)
            o = o + column(f3, j) * v_new[j % 8:j % 8 + 1]
            att[n * 2 + core, rows, :] = round_f32(o)

    def block(b, new, old):
        @pl.when(b < n_blk)
        def _():
            k_copy(b).wait()

        b1 = jnp.minimum(b, n_blk - 1)
        b2 = jnp.clip(b - 1, 0, n_blk - 1)
        b3 = jnp.clip(b - 2, 0, n_blk - 1)

        @pl.when(jnp.logical_or(b == 0, b >= 3))
        def _():
            v_copy(b3).wait()

        u2, row2 = b2 // bq, block_row(b2)
        m_all = o_buf[u2, o_rows:o_rows + heads, :]
        l_all = o_buf[u2, o_rows + heads:o_rows + 2 * heads, :]
        for pair in range(BR // 2):
            p_list = []
            for i in range(2):
                r = 2 * pair + i
                s = s_sc[old, pair, i * heads:(i + 1) * heads, :]
                s = jnp.where(pos < seq_ref[row2 + r], s, NEG)
                m = jnp.maximum(jnp.max(s, axis=-1, keepdims=True), NEG_FLOOR)
                p = jnp.exp2((s - m) * coef)
                l = jnp.sum(p, axis=-1, keepdims=True)
                here = lane == (b2 % bq) * BR + r
                m_all = jnp.where(here, m, m_all)
                l_all = jnp.where(here, l, l_all)
                p_list.append(p)
            p_sc[new, pair] = jnp.concatenate(p_list, axis=0).astype(jnp.bfloat16)
        o_buf[u2, o_rows:o_rows + heads, :] = m_all
        o_buf[u2, o_rows + heads:o_rows + 2 * heads, :] = l_all
        row1, kslot = block_row(b1), b1 % NBK
        for pair in range(BR // 2):
            r = 2 * pair
            left = jnp.concatenate([q_rows(row1 + r), zeros_q], axis=0)
            right = jnp.concatenate([zeros_q, q_rows(row1 + r + 1)], axis=0)
            q_pair = jnp.concatenate([left, right], axis=1).astype(jnp.bfloat16)
            k_pair = jnp.concatenate([kbuf[kslot, r], kbuf[kslot, r + 1]], axis=1)
            s_sc[new, pair] = lax.dot_general(q_pair, k_pair, (((1,), (1,)), ((), ())),
                                         preferred_element_type=jnp.float32)
        u3, vslot = b3 // bq, b3 % NBV
        for pair in range(BR // 2):
            r = 2 * pair
            v_pair = jnp.concatenate([vbuf[vslot, r], vbuf[vslot, r + 1]], axis=1)
            o_pair = jnp.dot(p_sc[old, pair], v_pair, preferred_element_type=jnp.float32)
            for i in range(2):
                o = o_pair[i * heads:(i + 1) * heads, i * head_dim:(i + 1) * head_dim]
                o_buf[u3, pl.ds(pl.multiple_of(((b3 % bq) * BR + r + i) * heads, 8), heads), :] = o

        @pl.when(b + NBK < n_blk)
        def _():
            k_copy(b + NBK).start()

        @pl.when(jnp.logical_and(b >= 2, b - 2 + NBV < n_blk))
        def _():
            v_copy(b - 2 + NBV).start()

        done = jnp.logical_and(b >= 2, (b - 2) % bq == bq - 1)
        u = b3 // bq

        @pl.when(jnp.logical_and(done, u % 2 == 0))
        def _():
            d2d(u // 2).start()

        @pl.when(jnp.logical_and(done, u % 2 == 1))
        def _():
            d2d(u // 2).wait_recv()
            merge_core(u)

            @pl.when(u < 2 * NC)
            def _():
                xsend(u // 2).start()

    def two_blocks(g, _):
        block(2 * g, 0, 1)
        block(2 * g + 1, 1, 0)
        return 0

    lax.fori_loop(0, (n_blk + 2) // 2, two_blocks, 0)
    for t in range(n_tiles):
        wo_copy(t).start()
        if t == 0:
            hid_copy.start()

    def finish_step(n, _):
        xsend(n).wait_recv()
        finish(n)
        at_copy(n).start()
        return 0
    lax.fori_loop(0, NC, finish_step, 0)

    def p_copy(i):
        return remote(p_buf.at[i], p_recv.at[i], p_s.at[i], p_r.at[i], to_tp)

    def yc_copy(i):
        return remote(y_send.at[i], y_core.at[i], yc_s.at[i], yc_r.at[i], to_core)

    def yx_copy(i):
        return remote(y_send.at[i], y_chip.at[i], yx_s.at[i], yx_r.at[i], to_chip)

    def yf_copy(i):
        return remote(y_chip.at[i], y_fwd.at[i], yf_s.at[i], yf_r.at[i], to_core)

    for n in range(NC):
        at_copy(n).wait_recv()
        for h in range(heads):
            cols = [att[n * 2 + c, pl.ds(h, quarter, stride=heads), :] for c in range(2)]
            lhs[n * 2 * quarter:(n + 1) * 2 * quarter, h * head_dim:(h + 1) * head_dim] = (
                jnp.concatenate(cols, axis=0).astype(jnp.bfloat16))
    hid_copy.wait()
    per = TN // TS

    def project(t, _):
        wo_copy(t).wait()
        res = jnp.dot(lhs[...], wo[t], preferred_element_type=jnp.float32)
        for s in range(per):
            i = t * per + s
            p_buf[i] = res[:, s * TS:(s + 1) * TS]
            p_copy(i).start()
        return 0

    def out_cols(i, on_core):
        return pl.ds(pl.multiple_of(on_core * half + i * TS, TS), TS)

    def out_rows(on_chip):
        return pl.ds(pl.multiple_of(on_chip * chip_rows, chip_rows), chip_rows)

    def y_tile(i):
        p_copy(i).wait_recv()
        res = hid[:, pl.ds(pl.multiple_of(i * TS, TS), TS)].astype(jnp.float32)
        y = (res + (p_buf[i] + p_recv[i])).astype(jnp.bfloat16)
        y_send[i] = y.astype(jnp.float32)
        y_ref[out_rows(chip), out_cols(i, core)] = y
        yx_copy(i).start()
        yc_copy(i).start()

    def y_from_chip(i):
        yx_copy(i).wait_recv()
        yf_copy(i).start()
        y_ref[out_rows(1 - chip), out_cols(i, core)] = y_chip[i].astype(jnp.bfloat16)
        yc_copy(i).wait_recv()
        y_ref[out_rows(chip), out_cols(i, 1 - core)] = y_core[i].astype(jnp.bfloat16)

    def y_from_fwd(i):
        yf_copy(i).wait_recv()
        y_ref[out_rows(1 - chip), out_cols(i, 1 - core)] = y_fwd[i].astype(jnp.bfloat16)

    total = n_tiles * per
    lead = 2
    for t in range(lead):
        project(t, 0)
    lag, lag2 = 2, 3

    def step(i, _):
        @pl.when(jnp.logical_and(i % per == 0, i // per + lead < n_tiles))
        def _():
            project(i // per + lead, 0)

        @pl.when(i < total)
        def _():
            y_tile(i)

        @pl.when(jnp.logical_and(i >= lag, i < total + lag))
        def _():
            y_from_chip(i - lag)

        @pl.when(i >= lag2)
        def _():
            y_from_fwd(i - lag2)
        return 0
    lax.fori_loop(0, total + lag2, step, 0)

    for t in range(n_q):
        q_copy(t).wait_send()
    for k in range(2 * NC):
        d2d(k).wait_send()
    for n in range(NC):
        xsend(n).wait_send()
        at_copy(n).wait_send()

    def drain(i, _):
        p_copy(i).wait_send()
        yc_copy(i).wait_send()
        yx_copy(i).wait_send()
        yf_copy(i).wait_send()
        return 0
    lax.fori_loop(0, total, drain, 0)


def attention(seq_lens, cos_t, sin_t, norm_w, b_q, b_k, b_v, hidden, w_q, w_k, w_v, k_cache, v_cache, w_o):
    n_rows, d_model = hidden.shape
    s_dev, head_dim = k_cache.shape[1], k_cache.shape[2]
    heads = w_q.shape[1] // head_dim
    half = d_model // 2
    n_tiles = half // TN
    n_q = w_q.shape[1] // (2 * TN)
    quarter = n_rows // (4 * NC)
    msg = quarter * heads + 2 * heads
    total = half // TS
    vmem = pl.BlockSpec(memory_space=pltpu.VMEM)
    hbm = pl.BlockSpec(memory_space=pl.ANY)
    f32, bf16 = jnp.float32, jnp.bfloat16
    dma = pltpu.SemaphoreType.DMA
    tile_f32 = pltpu.VMEM((total, n_rows // 2, TS), f32)
    return pl.pallas_call(
        attn_kernel,
        out_shape=[jax.ShapeDtypeStruct((n_rows, d_model), bf16)] + [jax.ShapeDtypeStruct((n_rows, head_dim), bf16)] * 2,
        in_specs=[pl.BlockSpec(memory_space=pltpu.SMEM)] + [vmem] * 6 + [hbm] * 7,
        out_specs=[vmem] * 3,
        scratch_shapes=[
            pltpu.VMEM((n_rows * heads, head_dim), f32),
            pltpu.VMEM((n_q, n_rows * TN // head_dim, head_dim), f32),
            pltpu.VMEM((n_q, n_rows * TN // head_dim, head_dim), f32),
            pltpu.VMEM((d_model, 2 * head_dim), bf16),
            pltpu.VMEM((heads, head_dim), f32),
            pltpu.VMEM((n_rows, head_dim), f32), pltpu.VMEM((n_rows, head_dim), f32),
            dma((n_rows // NORM_ROWS,)), dma((2,)), dma((n_q,)), dma((n_q,)),
            pltpu.VMEM((NC * 4, msg, head_dim), f32),
            pltpu.VMEM((NC * 2, msg, head_dim), f32),
            pltpu.VMEM((NC, msg, head_dim), f32),
            pltpu.VMEM((NC * 2, quarter * heads, head_dim), f32),
            pltpu.VMEM((n_rows // 2, heads * head_dim), bf16),
            pltpu.VMEM((2, BR // 2, 2 * heads, s_dev), f32),
            pltpu.VMEM((2, BR // 2, 2 * heads, s_dev), bf16),
            pltpu.VMEM((NC, heads, head_dim), f32),
            tile_f32, tile_f32, tile_f32, tile_f32, tile_f32, tile_f32,
            pltpu.VMEM((n_tiles, heads * head_dim, TN), bf16),
            pltpu.VMEM((n_rows // 2, half), bf16),
            pltpu.VMEM((NBK, BR, s_dev, head_dim), bf16),
            pltpu.VMEM((NBV, BR, s_dev, head_dim), bf16),
            dma((NBK,)), dma((NBV,)), dma((n_tiles,)), dma,
            dma((NC * 2,)), dma((NC * 2,)), dma((NC,)), dma((NC,)), dma((NC,)), dma((NC,)),
            dma((total,)), dma((total,)), dma((total,)), dma((total,)), dma((total,)), dma((total,)),
            dma((total,)), dma((total,)),
        ],
        compiler_params=pltpu.CompilerParams(
            collective_id=0, has_side_effects=True, vmem_limit_bytes=VMEM_LIMIT),
        name="attend",
    )(seq_lens, cos_t, sin_t, norm_w.reshape(-1, 128), b_q.reshape(heads, head_dim), b_k[None], b_v[None], hidden,
      w_q, w_k, w_v, k_cache, v_cache, w_o)


def copy_kernel(parts, y_in, k_in, v_in, y_out, k_out, v_out, buf, kv_buf, in_sem, out_sem):
    rows = y_in.shape[0] // parts
    pairs = [(y_in.at[pl.ds(p * rows, rows)], buf.at[p], y_out.at[pl.ds(p * rows, rows)]) for p in range(parts)]
    pairs += [(k_in, kv_buf.at[0], k_out), (v_in, kv_buf.at[1], v_out)]
    loads = [pltpu.make_async_copy(a, m, in_sem.at[i]) for i, (a, m, _) in enumerate(pairs)]
    stores = [pltpu.make_async_copy(m, z, out_sem.at[i]) for i, (_, m, z) in enumerate(pairs)]
    for c in loads:
        c.start()
    for c, d in zip(loads, stores):
        c.wait()
        d.start()
    for d in stores:
        d.wait()


def copy_out(y, k, v):
    parts = 8
    hbm = pl.BlockSpec(memory_space=pl.ANY)
    dma = pltpu.SemaphoreType.DMA
    return pl.pallas_call(
        functools.partial(copy_kernel, parts),
        out_shape=[jax.ShapeDtypeStruct(a.shape, a.dtype) for a in (y, k, v)],
        in_specs=[hbm] * 3, out_specs=[hbm] * 3,
        scratch_shapes=[pltpu.VMEM((parts, y.shape[0] // parts, y.shape[1]), y.dtype),
                        pltpu.VMEM((2,) + k.shape, k.dtype), dma((parts + 2,)), dma((parts + 2,))],
        name="copy_out",
    )(y, k, v)


def solution(mesh):
    def device_step(hidden, norm_w, w_q, b_q, w_k, b_k, w_v, b_v, w_o, k_cache, v_cache, positions, seq_lens):
        n_rows = hidden.shape[0]
        s_dev, head_dim = k_cache.shape[1], k_cache.shape[3]
        cos_t, sin_t = rope_tables(positions, head_dim)
        outs = attention(seq_lens, cos_t, sin_t, norm_w, b_q, b_k, b_v, hidden, w_q, w_k, w_v,
                         k_cache.reshape(n_rows, s_dev, head_dim), v_cache.reshape(n_rows, s_dev, head_dim), w_o)
        y_out, kb, vb = copy_out(*outs)
        return y_out, kb.reshape(n_rows, 1, head_dim), vb.reshape(n_rows, 1, head_dim)

    col_spec = P(None, 'tp')
    vec_spec = P('tp')
    cache_spec = P('dp', 'sp', 'tp', None)
    group_spec = P('dp', 'tp', None)
    in_specs = (P('dp', None), P(None), col_spec, vec_spec, col_spec, vec_spec, col_spec, vec_spec,
                P('tp', None), cache_spec, cache_spec, P('dp'), P('dp'))
    out_specs = (P('dp', None), group_spec, group_spec)
    return jax.shard_map(device_step, mesh=mesh, in_specs=in_specs, out_specs=out_specs, check_vma=False)
```

```python
import functools

import jax
import jax.numpy as jnp
from jax import lax
from jax.experimental import pallas as pl
from jax.experimental.pallas import tpu as pltpu
from jax.sharding import PartitionSpec as P

RMS_EPS = 1.5625e-7
ROPE_BASE = 10000.0
LOG2E = 1.4426950408889634
NEG = -3e38
NEG_FLOOR = -1e38
MESH = pl.DeviceIdType.MESH
VMEM_LIMIT = 67_043_328


NORM_ROWS = 32
NC = 4
NH = 2
BR = 8
NBK, NBV = 4, 6
TN = 512
G_FINISH, G_PROJECT = 12, 13
WO_FROM = 14


def rope_tables(positions, head_dim):
    rot_dim = head_dim // 2
    lane = jnp.arange(head_dim, dtype=jnp.int32)
    freq = ROPE_BASE ** (-2.0 * (lane // 2).astype(jnp.float32) / rot_dim)
    freq = jnp.where(lane < rot_dim, freq, 0.0)
    angles = positions.astype(jnp.float32)[:, None] * freq
    sign = jnp.where(lane % 2 == 0, -1.0, 1.0)
    return jnp.cos(angles), jnp.sin(angles) * sign


def rope(x, cos_t, sin_t, even):
    width = x.shape[-1]
    swapped = jnp.where(even, pltpu.roll(x, width - 1, 1), pltpu.roll(x, 1, 1))
    return (x * cos_t + swapped * sin_t).astype(jnp.bfloat16).astype(jnp.float32)


def attn_kernel(seq_ref, cos_ref, sin_ref, nw_ref, bq_ref, bk_ref, bv_ref, hid_hbm, wq_hbm, wk_hbm, wv_hbm,
                k_hbm, v_hbm, wo_hbm, y_ref, kb_ref, vb_ref,
                q_ref, q_send, q_recv, wkv, bqf, kf_ref, vf_ref, in_sem, wkv_sem, q_s, q_r, o_buf, rd, rx, att, lhs, s_sc, p_sc, new_sc, p_buf, p_recv, y_send, y_core, y_chip, y_fwd, wo, hid,
                kbuf, vbuf, k_sem, v_sem, wo_sem, hid_sem, rd_s, rd_r, rx_s, rx_r, at_s, at_r, p_s, p_r,
                yc_s, yc_r, yx_s, yx_r, yf_s, yf_r):
    n_rows, d_model = y_ref.shape
    s_dev, head_dim = kbuf.shape[2], kbuf.shape[3]
    heads = q_ref.shape[0] // n_rows
    n_tiles = wo.shape[0]
    half = n_tiles * TN
    quarter = n_rows // (4 * NC)
    o_rows = quarter * heads
    chip_rows = n_rows // 2
    bq = quarter // BR
    n_blk = n_rows // BR
    coef = head_dim ** -0.5 * LOG2E

    dp, tp, sp = lax.axis_index("dp"), lax.axis_index("tp"), lax.axis_index("sp")
    chip, core = sp // 2, sp % 2
    to_core = (dp, tp, 2 * chip + (1 - core))
    to_chip = (dp, tp, 2 * (1 - chip) + core)
    to_tp = (dp, 1 - tp, sp)

    def remote(src, dst, s_sem, r_sem, dev):
        return pltpu.make_async_remote_copy(src_ref=src, dst_ref=dst, send_sem=s_sem, recv_sem=r_sem,
                                            device_id=dev, device_id_type=MESH)

    per_part = NC // NH
    part_rows = chip_rows // NH

    def group_piece(u):
        return (u // (4 * per_part)) * per_part + (u % (2 * per_part)) // 2

    def group_far(u):
        return u % (4 * per_part) < 2 * per_part

    def group_row(u):
        near = (u % (4 * per_part)) // (2 * per_part)
        own = u % 2
        on_chip = near * chip + (1 - near) * (1 - chip)
        on_core = own * core + (1 - own) * (1 - core)
        return on_chip * chip_rows + group_piece(u) * 2 * quarter + on_core * quarter

    def kept_group(n, near):
        return (n // per_part) * 4 * per_part + near * 2 * per_part + 2 * (n % per_part) + 1

    def block_row(b):
        return pl.multiple_of(group_row(b // bq) + (b % bq) * BR, BR)

    def k_copy(b):
        return pltpu.make_async_copy(k_hbm.at[pl.ds(block_row(b), BR)], kbuf.at[b % NBK], k_sem.at[b % NBK])

    def v_copy(b):
        return pltpu.make_async_copy(v_hbm.at[pl.ds(block_row(b), BR)], vbuf.at[b % NBV], v_sem.at[b % NBV])

    def wo_copy(t):
        cols = pl.ds(pl.multiple_of(core * half + t * TN, 128), TN)
        return pltpu.make_async_copy(wo_hbm.at[:, cols], wo.at[t], wo_sem.at[t])

    hid_copy = pltpu.make_async_copy(
        hid_hbm.at[pl.ds(pl.multiple_of(chip * chip_rows, 128), chip_rows),
                   pl.ds(pl.multiple_of(core * half, 128), half)], hid, hid_sem)

    n_q = q_send.shape[0]
    tile_heads = TN // head_dim
    k_half = wo.shape[1]

    def in_copy(i):
        rows = pl.ds(pl.multiple_of(i * NORM_ROWS, NORM_ROWS), NORM_ROWS)
        return pltpu.make_async_copy(hid_hbm.at[rows], y_ref.at[rows], in_sem.at[i])

    wk_copy = pltpu.make_async_copy(wk_hbm, wkv.at[:, :head_dim], wkv_sem.at[0])
    wv_copy = pltpu.make_async_copy(wv_hbm, wkv.at[:, head_dim:], wkv_sem.at[1])

    def wq_copy(i):
        cols = pl.ds(pl.multiple_of((core * n_q + i // 2) * TN, TN), TN)
        return pltpu.make_async_copy(wq_hbm.at[pl.ds((i % 2) * k_half, k_half), cols], wo.at[i], wo_sem.at[i])

    n_norm = n_rows // NORM_ROWS
    for i in range(n_norm):
        in_copy(i).start()

    barrier = pltpu.get_barrier_semaphore()
    for dev in (to_core, to_chip, to_tp):
        pl.semaphore_signal(barrier, inc=1, device_id=dev, device_id_type=MESH)

    bqf[...] = bq_ref[...].astype(jnp.float32)

    def norm_rows(i, _):
        rows = pl.ds(pl.multiple_of(i * NORM_ROWS, NORM_ROWS), NORM_ROWS)
        in_copy(i).wait()

        @pl.when(i < 2 * n_q)
        def _():
            wq_copy(i).start()

        @pl.when(i == n_norm - 1)
        def _():
            wk_copy.start()
            wv_copy.start()
        sq = jnp.zeros((NORM_ROWS, 128), jnp.float32)
        for c in range(d_model // 128):
            x = y_ref[rows, c * 128:(c + 1) * 128].astype(jnp.float32)
            sq = sq + x * x
        inv = lax.rsqrt(jnp.sum(sq, axis=-1, keepdims=True) / d_model + RMS_EPS)
        for c in range(d_model // 128):
            x = y_ref[rows, c * 128:(c + 1) * 128].astype(jnp.float32)
            x = x * inv * nw_ref[c:c + 1, :].astype(jnp.float32)
            y_ref[rows, c * 128:(c + 1) * 128] = x.astype(jnp.bfloat16)
        return 0
    lax.fori_loop(0, n_norm, norm_rows, 0)
    pl.semaphore_wait(barrier, 3)

    even = lax.broadcasted_iota(jnp.int32, (n_rows, head_dim), 1) % 2 == 0

    def round_f32(x):
        return x.astype(jnp.bfloat16).astype(jnp.float32)

    def q_copy(t):
        return remote(q_send.at[t], q_recv.at[t], q_s.at[t], q_r.at[t], to_core)

    def q_tile(t, _):
        wq_copy(2 * t).wait()
        wq_copy(2 * t + 1).wait()

        @pl.when(t == n_q - 1)
        def _():
            for b in range(NBV):
                if b < NBK:
                    k_copy(b).start()
                v_copy(b).start()
        acc = jnp.dot(y_ref[:, :k_half], wo[2 * t], preferred_element_type=jnp.float32)
        acc = acc + jnp.dot(y_ref[:, k_half:], wo[2 * t + 1], preferred_element_type=jnp.float32)
        for h in range(tile_heads):
            head = core * (heads // 2) + t * tile_heads + h
            val = round_f32(acc[:, h * head_dim:(h + 1) * head_dim] + bqf[pl.ds(head, 1), :])
            val = rope(val, cos_ref[...], sin_ref[...], even)
            q_ref[pl.ds(head, n_rows, stride=heads), :] = val
            q_send[t, pl.ds(h, n_rows, stride=tile_heads), :] = val
        q_copy(t).start()
        return 0
    lax.fori_loop(0, n_q, q_tile, 0)

    wk_copy.wait()
    wv_copy.wait()
    kv = jnp.dot(y_ref[...], wkv[...], preferred_element_type=jnp.float32)
    k_rot = rope(round_f32(kv[:, :head_dim] + bk_ref[...].astype(jnp.float32)), cos_ref[...], sin_ref[...], even)
    kf_ref[...] = k_rot
    kb_ref[...] = k_rot.astype(jnp.bfloat16)
    v_val = round_f32(kv[:, head_dim:] + bv_ref[...].astype(jnp.float32))
    vf_ref[...] = v_val
    vb_ref[...] = v_val.astype(jnp.bfloat16)

    def q_take(t, _):
        q_copy(t).wait_recv()
        for h in range(tile_heads):
            head = (1 - core) * (heads // 2) + t * tile_heads + h
            q_ref[pl.ds(head, n_rows, stride=heads), :] = q_recv[t, pl.ds(h, n_rows, stride=tile_heads), :]
        return 0
    lax.fori_loop(0, n_q, q_take, 0)

    lane = lax.broadcasted_iota(jnp.int32, (heads, head_dim), 1)
    pos = lax.broadcasted_iota(jnp.int32, (heads, s_dev), 1) + sp * s_dev
    zeros_q = jnp.zeros((heads, head_dim), jnp.float32)

    def q_rows(row):
        return q_ref[pl.ds(pl.multiple_of(row * heads, 8), heads), :]

    def new_scores(n):
        row0 = chip * chip_rows + n * 2 * quarter + core * quarter

        def rows8(g, acc):
            base = pl.multiple_of(row0 + g * 8, 8)
            k_new = kf_ref[pl.ds(base, 8), :]
            for r in range(8):
                s_new = jnp.sum(q_rows(base + r) * k_new[r:r + 1], axis=-1, keepdims=True)
                acc = jnp.where(lane == g * 8 + r, s_new, acc)
            return acc
        new_sc[n] = lax.fori_loop(0, quarter // 8, rows8, zeros_q)

    for n in range(NC):
        new_scores(n)

    def column(vals, j):
        return jnp.broadcast_to(vals[:, j:j + 1], (heads, head_dim))

    def d2d(k):
        return remote(o_buf.at[2 * k], rd.at[k], rd_s.at[k], rd_r.at[k], to_core)

    def xsend(n):
        return remote(o_buf.at[kept_group(n, 0)], rx.at[n], rx_s.at[n], rx_r.at[n], to_chip)

    def at_copy(n):
        return remote(att.at[n * 2 + core], att.at[n * 2 + core], at_s.at[n], at_r.at[n], to_core)

    def merge_core(u):
        k = u // 2
        m1 = o_buf[u, o_rows:o_rows + heads, :]
        l1 = o_buf[u, o_rows + heads:o_rows + 2 * heads, :]
        m2 = rd[k, o_rows:o_rows + heads, :]
        l2 = rd[k, o_rows + heads:o_rows + 2 * heads, :]
        m = jnp.maximum(m1, m2)
        f1 = jnp.exp2((m1 - m) * coef)
        f2 = jnp.exp2((m2 - m) * coef)
        o_buf[u, o_rows:o_rows + heads, :] = m
        o_buf[u, o_rows + heads:o_rows + 2 * heads, :] = l1 * f1 + l2 * f2

        for j in range(quarter):
            rows = pl.ds(j * heads, heads)
            o_buf[u, rows, :] = o_buf[u, rows, :] * column(f1, j) + rd[k, rows, :] * column(f2, j)

    def finish(n):
        u = kept_group(n, 1)
        row0 = chip * chip_rows + n * 2 * quarter + core * quarter
        m1 = o_buf[u, o_rows:o_rows + heads, :]
        l1 = o_buf[u, o_rows + heads:o_rows + 2 * heads, :]
        m2 = rx[n, o_rows:o_rows + heads, :]
        l2 = rx[n, o_rows + heads:o_rows + 2 * heads, :]
        m3 = new_sc[n]
        m = jnp.maximum(jnp.maximum(m1, m2), m3)
        f1 = jnp.exp2((m1 - m) * coef)
        f2 = jnp.exp2((m2 - m) * coef)
        f3 = jnp.exp2((m3 - m) * coef)
        l = l1 * f1 + l2 * f2 + f3
        f1, f2, f3 = f1 / l, f2 / l, f3 / l

        for j in range(quarter):
            if j % 8 == 0:
                v_new = vf_ref[pl.ds(pl.multiple_of(row0 + j, 8), 8), :]
            rows = pl.ds(j * heads, heads)
            o = o_buf[u, rows, :] * column(f1, j) + rx[n, rows, :] * column(f2, j)
            o = o + column(f3, j) * v_new[j % 8:j % 8 + 1]
            att[n * 2 + core, rows, :] = round_f32(o)

    def block(b, new, old):
        @pl.when(b < n_blk)
        def _():
            k_copy(b).wait()

        b1 = jnp.minimum(b, n_blk - 1)
        b2 = jnp.clip(b - 1, 0, n_blk - 1)
        b3 = jnp.clip(b - 2, 0, n_blk - 1)

        @pl.when(jnp.logical_or(b == 0, b >= 3))
        def _():
            v_copy(b3).wait()

        u2, row2 = b2 // bq, block_row(b2)
        m_all = o_buf[u2, o_rows:o_rows + heads, :]
        l_all = o_buf[u2, o_rows + heads:o_rows + 2 * heads, :]
        for pair in range(BR // 2):
            p_list = []
            for i in range(2):
                r = 2 * pair + i
                s = s_sc[old, pair, i * heads:(i + 1) * heads, :]
                s = jnp.where(pos < seq_ref[row2 + r], s, NEG)
                m = jnp.maximum(jnp.max(s, axis=-1, keepdims=True), NEG_FLOOR)
                p = jnp.exp2((s - m) * coef)
                l = jnp.sum(p, axis=-1, keepdims=True)
                here = lane == (b2 % bq) * BR + r
                m_all = jnp.where(here, m, m_all)
                l_all = jnp.where(here, l, l_all)
                p_list.append(p)
            p_sc[new, pair] = jnp.concatenate(p_list, axis=0).astype(jnp.bfloat16)
        o_buf[u2, o_rows:o_rows + heads, :] = m_all
        o_buf[u2, o_rows + heads:o_rows + 2 * heads, :] = l_all
        row1, kslot = block_row(b1), b1 % NBK
        for pair in range(BR // 2):
            r = 2 * pair
            left = jnp.concatenate([q_rows(row1 + r), zeros_q], axis=0)
            right = jnp.concatenate([zeros_q, q_rows(row1 + r + 1)], axis=0)
            q_pair = jnp.concatenate([left, right], axis=1).astype(jnp.bfloat16)
            k_pair = jnp.concatenate([kbuf[kslot, r], kbuf[kslot, r + 1]], axis=1)
            s_sc[new, pair] = lax.dot_general(q_pair, k_pair, (((1,), (1,)), ((), ())),
                                         preferred_element_type=jnp.float32)
        u3, vslot = b3 // bq, b3 % NBV
        for pair in range(BR // 2):
            r = 2 * pair
            v_pair = jnp.concatenate([vbuf[vslot, r], vbuf[vslot, r + 1]], axis=1)
            o_pair = jnp.dot(p_sc[old, pair], v_pair, preferred_element_type=jnp.float32)
            for i in range(2):
                o = o_pair[i * heads:(i + 1) * heads, i * head_dim:(i + 1) * head_dim]
                o_buf[u3, pl.ds(pl.multiple_of(((b3 % bq) * BR + r + i) * heads, 8), heads), :] = o

        @pl.when(b + NBK < n_blk)
        def _():
            k_copy(b + NBK).start()

        @pl.when(jnp.logical_and(b >= 2, b - 2 + NBV < n_blk))
        def _():
            v_copy(b - 2 + NBV).start()

        w = b - WO_FROM

        @pl.when(jnp.logical_and(w >= 0, jnp.logical_and(w % 2 == 0, w < 2 * n_tiles)))
        def _():
            wo_copy(w // 2).start()

        @pl.when(w == 2 * n_tiles)
        def _():
            hid_copy.start()

        done = jnp.logical_and(b >= 2, (b - 2) % bq == bq - 1)
        u = b3 // bq

        @pl.when(jnp.logical_and(done, u % 2 == 0))
        def _():
            d2d(u // 2).start()

        @pl.when(jnp.logical_and(done, u % 2 == 1))
        def _():
            d2d(u // 2).wait_recv()
            merge_core(u)

            @pl.when(group_far(u))
            def _():
                xsend(group_piece(u)).start()

    def two_blocks(g, _):
        block(2 * g, 0, 1)
        block(2 * g + 1, 1, 0)
        return 0

    def p_copy(i):
        return remote(p_buf.at[i], p_recv.at[i], p_s.at[i], p_r.at[i], to_tp)

    def yc_copy(i):
        return remote(y_send.at[i], y_core.at[i], yc_s.at[i], yc_r.at[i], to_core)

    def yx_copy(i):
        return remote(y_send.at[i], y_chip.at[i], yx_s.at[i], yx_r.at[i], to_chip)

    def yf_copy(i):
        return remote(y_chip.at[i], y_fwd.at[i], yf_s.at[i], yf_r.at[i], to_core)

    def finish_part(h):
        for k in range(per_part):
            n = h * per_part + k
            xsend(n).wait_recv()
            finish(n)
            at_copy(n).start()

    def project_part(h):
        for k in range(per_part):
            n = h * per_part + k
            at_copy(n).wait_recv()
            for hd in range(heads):
                cols = [att[n * 2 + c, pl.ds(hd, quarter, stride=heads), :] for c in range(2)]
                lhs[k * 2 * quarter:(k + 1) * 2 * quarter, hd * head_dim:(hd + 1) * head_dim] = (
                    jnp.concatenate(cols, axis=0).astype(jnp.bfloat16))

        def tile(t, _):
            if h == 0:
                wo_copy(t).wait()
            i = h * n_tiles + t
            p_buf[i] = jnp.dot(lhs[...], wo[t], preferred_element_type=jnp.float32)
            p_copy(i).start()
            return 0
        lax.fori_loop(0, n_tiles, tile, 0)

    def out_cols(i, on_core):
        return pl.ds(pl.multiple_of(on_core * half + (i % n_tiles) * TN, TN), TN)

    def out_rows(i, on_chip):
        return pl.ds(pl.multiple_of(on_chip * chip_rows + (i // n_tiles) * part_rows, part_rows), part_rows)

    def y_tile(i):
        p_copy(i).wait_recv()
        res = hid[pl.ds(pl.multiple_of((i // n_tiles) * part_rows, part_rows), part_rows),
                  pl.ds(pl.multiple_of((i % n_tiles) * TN, TN), TN)].astype(jnp.float32)
        y = (res + (p_buf[i] + p_recv[i])).astype(jnp.bfloat16)
        y_send[i] = y.astype(jnp.float32)
        y_ref[out_rows(i, chip), out_cols(i, core)] = y
        yx_copy(i).start()
        yc_copy(i).start()

    def y_from_chip(i):
        yx_copy(i).wait_recv()
        yf_copy(i).start()
        y_ref[out_rows(i, 1 - chip), out_cols(i, core)] = y_chip[i].astype(jnp.bfloat16)
        yc_copy(i).wait_recv()
        y_ref[out_rows(i, chip), out_cols(i, 1 - core)] = y_core[i].astype(jnp.bfloat16)

    def y_from_fwd(i):
        yf_copy(i).wait_recv()
        y_ref[out_rows(i, 1 - chip), out_cols(i, 1 - core)] = y_fwd[i].astype(jnp.bfloat16)

    total = NH * n_tiles
    last = (n_blk + 2) // 2
    lax.fori_loop(0, G_FINISH, two_blocks, 0)
    finish_part(0)
    lax.fori_loop(G_FINISH, G_PROJECT, two_blocks, 0)
    project_part(0)

    def two_blocks_and_tile(g, _):
        two_blocks(g, 0)

        @pl.when(g == last - 3)
        def _():
            hid_copy.wait()

        @pl.when(jnp.logical_or(g == last - 3, g == last - 1))
        def _():
            y_tile((g - (last - 3)) // 2)
        return 0
    lax.fori_loop(G_PROJECT, last, two_blocks_and_tile, 0)
    finish_part(1)
    y_tile(2)
    project_part(1)
    early = 3

    def step(s, _):
        @pl.when(s + early < total)
        def _():
            y_tile(s + early)

        @pl.when(s < total)
        def _():
            y_from_chip(s)

        @pl.when(s >= 1)
        def _():
            y_from_fwd(s - 1)
        return 0
    lax.fori_loop(0, total + 1, step, 0)

    for t in range(n_q):
        q_copy(t).wait_send()
    for k in range(2 * NC):
        d2d(k).wait_send()
    for n in range(NC):
        xsend(n).wait_send()
        at_copy(n).wait_send()

    def drain(i, _):
        p_copy(i).wait_send()
        yc_copy(i).wait_send()
        yx_copy(i).wait_send()
        yf_copy(i).wait_send()
        return 0
    lax.fori_loop(0, total, drain, 0)


def attention(seq_lens, cos_t, sin_t, norm_w, b_q, b_k, b_v, hidden, w_q, w_k, w_v, k_cache, v_cache, w_o):
    n_rows, d_model = hidden.shape
    s_dev, head_dim = k_cache.shape[1], k_cache.shape[2]
    heads = w_q.shape[1] // head_dim
    half = d_model // 2
    n_tiles = half // TN
    n_q = w_q.shape[1] // (2 * TN)
    quarter = n_rows // (4 * NC)
    msg = quarter * heads + 2 * heads
    total = NH * n_tiles
    vmem = pl.BlockSpec(memory_space=pltpu.VMEM)
    hbm = pl.BlockSpec(memory_space=pl.ANY)
    f32, bf16 = jnp.float32, jnp.bfloat16
    dma = pltpu.SemaphoreType.DMA
    tile_f32 = pltpu.VMEM((total, n_rows // (2 * NH), TN), f32)
    return pl.pallas_call(
        attn_kernel,
        out_shape=[jax.ShapeDtypeStruct((n_rows, d_model), bf16)] + [jax.ShapeDtypeStruct((n_rows, head_dim), bf16)] * 2,
        in_specs=[pl.BlockSpec(memory_space=pltpu.SMEM)] + [vmem] * 6 + [hbm] * 7,
        out_specs=[vmem] * 3,
        scratch_shapes=[
            pltpu.VMEM((n_rows * heads, head_dim), f32),
            pltpu.VMEM((n_q, n_rows * TN // head_dim, head_dim), f32),
            pltpu.VMEM((n_q, n_rows * TN // head_dim, head_dim), f32),
            pltpu.VMEM((d_model, 2 * head_dim), bf16),
            pltpu.VMEM((heads, head_dim), f32),
            pltpu.VMEM((n_rows, head_dim), f32), pltpu.VMEM((n_rows, head_dim), f32),
            dma((n_rows // NORM_ROWS,)), dma((2,)), dma((n_q,)), dma((n_q,)),
            pltpu.VMEM((NC * 4, msg, head_dim), f32),
            pltpu.VMEM((NC * 2, msg, head_dim), f32),
            pltpu.VMEM((NC, msg, head_dim), f32),
            pltpu.VMEM((NC * 2, quarter * heads, head_dim), f32),
            pltpu.VMEM((n_rows // (2 * NH), heads * head_dim), bf16),
            pltpu.VMEM((2, BR // 2, 2 * heads, s_dev), f32),
            pltpu.VMEM((2, BR // 2, 2 * heads, s_dev), bf16),
            pltpu.VMEM((NC, heads, head_dim), f32),
            tile_f32, tile_f32, tile_f32, tile_f32, tile_f32, tile_f32,
            pltpu.VMEM((n_tiles, heads * head_dim, TN), bf16),
            pltpu.VMEM((n_rows // 2, half), bf16),
            pltpu.VMEM((NBK, BR, s_dev, head_dim), bf16),
            pltpu.VMEM((NBV, BR, s_dev, head_dim), bf16),
            dma((NBK,)), dma((NBV,)), dma((n_tiles,)), dma,
            dma((NC * 2,)), dma((NC * 2,)), dma((NC,)), dma((NC,)), dma((NC,)), dma((NC,)),
            dma((total,)), dma((total,)), dma((total,)), dma((total,)), dma((total,)), dma((total,)),
            dma((total,)), dma((total,)),
        ],
        compiler_params=pltpu.CompilerParams(
            collective_id=0, has_side_effects=True, vmem_limit_bytes=VMEM_LIMIT),
        name="attend",
    )(seq_lens, cos_t, sin_t, norm_w.reshape(-1, 128), b_q.reshape(heads, head_dim), b_k[None], b_v[None], hidden,
      w_q, w_k, w_v, k_cache, v_cache, w_o)


def copy_kernel(parts, y_in, k_in, v_in, y_out, k_out, v_out, buf, kv_buf, in_sem, out_sem):
    rows = y_in.shape[0] // parts
    pairs = [(y_in.at[pl.ds(p * rows, rows)], buf.at[p], y_out.at[pl.ds(p * rows, rows)]) for p in range(parts)]
    pairs += [(k_in, kv_buf.at[0], k_out), (v_in, kv_buf.at[1], v_out)]
    loads = [pltpu.make_async_copy(a, m, in_sem.at[i]) for i, (a, m, _) in enumerate(pairs)]
    stores = [pltpu.make_async_copy(m, z, out_sem.at[i]) for i, (_, m, z) in enumerate(pairs)]
    for c in loads:
        c.start()
    for c, d in zip(loads, stores):
        c.wait()
        d.start()
    for d in stores:
        d.wait()


def copy_out(y, k, v):
    parts = 8
    hbm = pl.BlockSpec(memory_space=pl.ANY)
    dma = pltpu.SemaphoreType.DMA
    return pl.pallas_call(
        functools.partial(copy_kernel, parts),
        out_shape=[jax.ShapeDtypeStruct(a.shape, a.dtype) for a in (y, k, v)],
        in_specs=[hbm] * 3, out_specs=[hbm] * 3,
        scratch_shapes=[pltpu.VMEM((parts, y.shape[0] // parts, y.shape[1]), y.dtype),
                        pltpu.VMEM((2,) + k.shape, k.dtype), dma((parts + 2,)), dma((parts + 2,))],
        name="copy_out",
    )(y, k, v)


def solution(mesh):
    def device_step(hidden, norm_w, w_q, b_q, w_k, b_k, w_v, b_v, w_o, k_cache, v_cache, positions, seq_lens):
        n_rows = hidden.shape[0]
        s_dev, head_dim = k_cache.shape[1], k_cache.shape[3]
        cos_t, sin_t = rope_tables(positions, head_dim)
        outs = attention(seq_lens, cos_t, sin_t, norm_w, b_q, b_k, b_v, hidden, w_q, w_k, w_v,
                         k_cache.reshape(n_rows, s_dev, head_dim), v_cache.reshape(n_rows, s_dev, head_dim), w_o)
        y_out, kb, vb = copy_out(*outs)
        return y_out, kb.reshape(n_rows, 1, head_dim), vb.reshape(n_rows, 1, head_dim)

    col_spec = P(None, 'tp')
    vec_spec = P('tp')
    cache_spec = P('dp', 'sp', 'tp', None)
    group_spec = P('dp', 'tp', None)
    in_specs = (P('dp', None), P(None), col_spec, vec_spec, col_spec, vec_spec, col_spec, vec_spec,
                P('tp', None), cache_spec, cache_spec, P('dp'), P('dp'))
    out_specs = (P('dp', None), group_spec, group_spec)
    return jax.shard_map(device_step, mesh=mesh, in_specs=in_specs, out_specs=out_specs, check_vma=False)
```

```python
import functools

import jax
import jax.numpy as jnp
from jax import lax
from jax.experimental import pallas as pl
from jax.experimental.pallas import tpu as pltpu
from jax.sharding import PartitionSpec as P

RMS_EPS = 1.5625e-7
ROPE_BASE = 10000.0
LOG2E = 1.4426950408889634
NEG = -3e38
NEG_FLOOR = -1e38
MESH = pl.DeviceIdType.MESH
VMEM_LIMIT = 67_043_328


NORM_ROWS = 32
NC = 4
NH = 2
BR = 8
NBK, NBV = 4, 6
TN = 512
G_FINISH, G_PROJECT = 10, 11
G_TILE = 12
WO_FROM = 8


def rope_tables(positions, head_dim):
    rot_dim = head_dim // 2
    lane = jnp.arange(head_dim, dtype=jnp.int32)
    freq = ROPE_BASE ** (-2.0 * (lane // 2).astype(jnp.float32) / rot_dim)
    freq = jnp.where(lane < rot_dim, freq, 0.0)
    angles = positions.astype(jnp.float32)[:, None] * freq
    sign = jnp.where(lane % 2 == 0, -1.0, 1.0)
    return jnp.cos(angles), jnp.sin(angles) * sign


def rope(x, cos_t, sin_t, even):
    width = x.shape[-1]
    swapped = jnp.where(even, pltpu.roll(x, width - 1, 1), pltpu.roll(x, 1, 1))
    return (x * cos_t + swapped * sin_t).astype(jnp.bfloat16).astype(jnp.float32)


def attn_kernel(seq_ref, cos_ref, sin_ref, nw_ref, bq_ref, bk_ref, bv_ref, hid_hbm, wq_hbm, wk_hbm, wv_hbm,
                k_hbm, v_hbm, wo_hbm, y_ref, kb_ref, vb_ref,
                q_ref, q_send, q_recv, wkv, bqf, kf_ref, vf_ref, in_sem, wkv_sem, q_s, q_r, o_buf, rd, rx, att, lhs, s_sc, p_sc, new_sc, p_buf, p_recv, y_send, y_core, y_chip, y_fwd, wo, hid,
                kbuf, vbuf, k_sem, v_sem, wo_sem, hid_sem, rd_s, rd_r, rx_s, rx_r, at_s, at_r, p_s, p_r,
                yc_s, yc_r, yx_s, yx_r, yf_s, yf_r):
    n_rows, d_model = y_ref.shape
    s_dev, head_dim = kbuf.shape[2], kbuf.shape[3]
    heads = q_ref.shape[0] // n_rows
    n_tiles = wo.shape[0]
    half = n_tiles * TN
    quarter = n_rows // (4 * NC)
    o_rows = quarter * heads
    chip_rows = n_rows // 2
    bq = quarter // BR
    n_blk = n_rows // BR
    coef = head_dim ** -0.5 * LOG2E

    dp, tp, sp = lax.axis_index("dp"), lax.axis_index("tp"), lax.axis_index("sp")
    chip, core = sp // 2, sp % 2
    to_core = (dp, tp, 2 * chip + (1 - core))
    to_chip = (dp, tp, 2 * (1 - chip) + core)
    to_tp = (dp, 1 - tp, sp)

    def remote(src, dst, s_sem, r_sem, dev):
        return pltpu.make_async_remote_copy(src_ref=src, dst_ref=dst, send_sem=s_sem, recv_sem=r_sem,
                                            device_id=dev, device_id_type=MESH)

    per_part = NC // NH
    part_rows = chip_rows // NH

    def group_piece(u):
        return (u // (4 * per_part)) * per_part + (u % (2 * per_part)) // 2

    def group_far(u):
        return u % (4 * per_part) < 2 * per_part

    def group_row(u):
        near = (u % (4 * per_part)) // (2 * per_part)
        own = u % 2
        on_chip = near * chip + (1 - near) * (1 - chip)
        on_core = own * core + (1 - own) * (1 - core)
        return on_chip * chip_rows + group_piece(u) * 2 * quarter + on_core * quarter

    def kept_group(n, near):
        return (n // per_part) * 4 * per_part + near * 2 * per_part + 2 * (n % per_part) + 1

    def block_row(b):
        return pl.multiple_of(group_row(b // bq) + (b % bq) * BR, BR)

    def k_copy(b):
        return pltpu.make_async_copy(k_hbm.at[pl.ds(block_row(b), BR)], kbuf.at[b % NBK], k_sem.at[b % NBK])

    def v_copy(b):
        return pltpu.make_async_copy(v_hbm.at[pl.ds(block_row(b), BR)], vbuf.at[b % NBV], v_sem.at[b % NBV])

    def wo_copy(t):
        cols = pl.ds(pl.multiple_of(core * half + t * TN, 128), TN)
        return pltpu.make_async_copy(wo_hbm.at[:, cols], wo.at[t], wo_sem.at[t])

    hid_copy = pltpu.make_async_copy(
        hid_hbm.at[pl.ds(pl.multiple_of(chip * chip_rows, 128), chip_rows),
                   pl.ds(pl.multiple_of(core * half, 128), half)], hid, hid_sem)

    n_q = q_send.shape[0]
    tile_heads = TN // head_dim
    k_half = wo.shape[1]

    def in_copy(i):
        rows = pl.ds(pl.multiple_of(i * NORM_ROWS, NORM_ROWS), NORM_ROWS)
        return pltpu.make_async_copy(hid_hbm.at[rows], y_ref.at[rows], in_sem.at[i])

    wk_copy = pltpu.make_async_copy(wk_hbm, wkv.at[:, :head_dim], wkv_sem.at[0])
    wv_copy = pltpu.make_async_copy(wv_hbm, wkv.at[:, head_dim:], wkv_sem.at[1])

    def wq_copy(i):
        cols = pl.ds(pl.multiple_of((core * n_q + i // 2) * TN, TN), TN)
        return pltpu.make_async_copy(wq_hbm.at[pl.ds((i % 2) * k_half, k_half), cols], wo.at[i], wo_sem.at[i])

    n_norm = n_rows // NORM_ROWS
    for i in range(n_norm):
        in_copy(i).start()

    barrier = pltpu.get_barrier_semaphore()
    for dev in (to_core, to_chip, to_tp):
        pl.semaphore_signal(barrier, inc=1, device_id=dev, device_id_type=MESH)

    bqf[...] = bq_ref[...].astype(jnp.float32)

    def norm_rows(i, _):
        rows = pl.ds(pl.multiple_of(i * NORM_ROWS, NORM_ROWS), NORM_ROWS)
        in_copy(i).wait()

        @pl.when(i < 2 * n_q)
        def _():
            wq_copy(i).start()

        @pl.when(i == n_norm - 1)
        def _():
            wk_copy.start()
            wv_copy.start()
        sq = jnp.zeros((NORM_ROWS, 128), jnp.float32)
        for c in range(d_model // 128):
            x = y_ref[rows, c * 128:(c + 1) * 128].astype(jnp.float32)
            sq = sq + x * x
        inv = lax.rsqrt(jnp.sum(sq, axis=-1, keepdims=True) / d_model + RMS_EPS)
        for c in range(d_model // 128):
            x = y_ref[rows, c * 128:(c + 1) * 128].astype(jnp.float32)
            x = x * inv * nw_ref[c:c + 1, :].astype(jnp.float32)
            y_ref[rows, c * 128:(c + 1) * 128] = x.astype(jnp.bfloat16)
        return 0
    lax.fori_loop(0, n_norm, norm_rows, 0)
    pl.semaphore_wait(barrier, 3)

    even = lax.broadcasted_iota(jnp.int32, (n_rows, head_dim), 1) % 2 == 0

    def round_f32(x):
        return x.astype(jnp.bfloat16).astype(jnp.float32)

    def q_copy(t):
        return remote(q_send.at[t], q_recv.at[t], q_s.at[t], q_r.at[t], to_core)

    def q_tile(t, _):
        wq_copy(2 * t).wait()
        wq_copy(2 * t + 1).wait()

        @pl.when(t == n_q - 1)
        def _():
            for b in range(NBV):
                if b < NBK:
                    k_copy(b).start()
                v_copy(b).start()
        acc = jnp.dot(y_ref[:, :k_half], wo[2 * t], preferred_element_type=jnp.float32)
        acc = acc + jnp.dot(y_ref[:, k_half:], wo[2 * t + 1], preferred_element_type=jnp.float32)
        for h in range(tile_heads):
            head = core * (heads // 2) + t * tile_heads + h
            val = round_f32(acc[:, h * head_dim:(h + 1) * head_dim] + bqf[pl.ds(head, 1), :])
            val = rope(val, cos_ref[...], sin_ref[...], even)
            q_ref[pl.ds(head, n_rows, stride=heads), :] = val
            q_send[t, pl.ds(h, n_rows, stride=tile_heads), :] = val
        q_copy(t).start()
        return 0
    lax.fori_loop(0, n_q, q_tile, 0)

    wk_copy.wait()
    wv_copy.wait()
    kv = jnp.dot(y_ref[...], wkv[...], preferred_element_type=jnp.float32)
    k_rot = rope(round_f32(kv[:, :head_dim] + bk_ref[...].astype(jnp.float32)), cos_ref[...], sin_ref[...], even)
    kf_ref[...] = k_rot
    kb_ref[...] = k_rot.astype(jnp.bfloat16)
    v_val = round_f32(kv[:, head_dim:] + bv_ref[...].astype(jnp.float32))
    vf_ref[...] = v_val
    vb_ref[...] = v_val.astype(jnp.bfloat16)

    def q_take(t, _):
        q_copy(t).wait_recv()
        for h in range(tile_heads):
            head = (1 - core) * (heads // 2) + t * tile_heads + h
            q_ref[pl.ds(head, n_rows, stride=heads), :] = q_recv[t, pl.ds(h, n_rows, stride=tile_heads), :]
        return 0
    lax.fori_loop(0, n_q, q_take, 0)

    lane = lax.broadcasted_iota(jnp.int32, (heads, head_dim), 1)
    pos = lax.broadcasted_iota(jnp.int32, (heads, s_dev), 1) + sp * s_dev
    zeros_q = jnp.zeros((heads, head_dim), jnp.float32)

    def q_rows(row):
        return q_ref[pl.ds(pl.multiple_of(row * heads, 8), heads), :]

    def new_scores(n):
        row0 = chip * chip_rows + n * 2 * quarter + core * quarter

        def rows8(g, acc):
            base = pl.multiple_of(row0 + g * 8, 8)
            k_new = kf_ref[pl.ds(base, 8), :]
            for r in range(8):
                s_new = jnp.sum(q_rows(base + r) * k_new[r:r + 1], axis=-1, keepdims=True)
                acc = jnp.where(lane == g * 8 + r, s_new, acc)
            return acc
        new_sc[n] = lax.fori_loop(0, quarter // 8, rows8, zeros_q)

    for n in range(NC):
        new_scores(n)

    def column(vals, j):
        return jnp.broadcast_to(vals[:, j:j + 1], (heads, head_dim))

    def d2d(k):
        return remote(o_buf.at[2 * k], rd.at[k], rd_s.at[k], rd_r.at[k], to_core)

    def xsend(n):
        return remote(o_buf.at[kept_group(n, 0)], rx.at[n], rx_s.at[n], rx_r.at[n], to_chip)

    def at_copy(n):
        return remote(att.at[n * 2 + core], att.at[n * 2 + core], at_s.at[n], at_r.at[n], to_core)

    def merge_core(u):
        k = u // 2
        m1 = o_buf[u, o_rows:o_rows + heads, :]
        l1 = o_buf[u, o_rows + heads:o_rows + 2 * heads, :]
        m2 = rd[k, o_rows:o_rows + heads, :]
        l2 = rd[k, o_rows + heads:o_rows + 2 * heads, :]
        m = jnp.maximum(m1, m2)
        f1 = jnp.exp2((m1 - m) * coef)
        f2 = jnp.exp2((m2 - m) * coef)
        o_buf[u, o_rows:o_rows + heads, :] = m
        o_buf[u, o_rows + heads:o_rows + 2 * heads, :] = l1 * f1 + l2 * f2

        for j in range(quarter):
            rows = pl.ds(j * heads, heads)
            o_buf[u, rows, :] = o_buf[u, rows, :] * column(f1, j) + rd[k, rows, :] * column(f2, j)

    def finish(n):
        u = kept_group(n, 1)
        row0 = chip * chip_rows + n * 2 * quarter + core * quarter
        m1 = o_buf[u, o_rows:o_rows + heads, :]
        l1 = o_buf[u, o_rows + heads:o_rows + 2 * heads, :]
        m2 = rx[n, o_rows:o_rows + heads, :]
        l2 = rx[n, o_rows + heads:o_rows + 2 * heads, :]
        m3 = new_sc[n]
        m = jnp.maximum(jnp.maximum(m1, m2), m3)
        f1 = jnp.exp2((m1 - m) * coef)
        f2 = jnp.exp2((m2 - m) * coef)
        f3 = jnp.exp2((m3 - m) * coef)
        l = l1 * f1 + l2 * f2 + f3
        f1, f2, f3 = f1 / l, f2 / l, f3 / l

        for j in range(quarter):
            if j % 8 == 0:
                v_new = vf_ref[pl.ds(pl.multiple_of(row0 + j, 8), 8), :]
            rows = pl.ds(j * heads, heads)
            o = o_buf[u, rows, :] * column(f1, j) + rx[n, rows, :] * column(f2, j)
            o = o + column(f3, j) * v_new[j % 8:j % 8 + 1]
            att[n * 2 + core, rows, :] = round_f32(o)

    def block(b, new, old):
        @pl.when(b < n_blk)
        def _():
            k_copy(b).wait()

        b1 = jnp.minimum(b, n_blk - 1)
        b2 = jnp.clip(b - 1, 0, n_blk - 1)
        b3 = jnp.clip(b - 2, 0, n_blk - 1)

        @pl.when(jnp.logical_or(b == 0, b >= 3))
        def _():
            v_copy(b3).wait()

        u2, row2 = b2 // bq, block_row(b2)
        m_all = o_buf[u2, o_rows:o_rows + heads, :]
        l_all = o_buf[u2, o_rows + heads:o_rows + 2 * heads, :]
        for pair in range(BR // 2):
            p_list = []
            for i in range(2):
                r = 2 * pair + i
                s = s_sc[old, pair, i * heads:(i + 1) * heads, :]
                s = jnp.where(pos < seq_ref[row2 + r], s, NEG)
                m = jnp.maximum(jnp.max(s, axis=-1, keepdims=True), NEG_FLOOR)
                p = jnp.exp2((s - m) * coef)
                l = jnp.sum(p, axis=-1, keepdims=True)
                here = lane == (b2 % bq) * BR + r
                m_all = jnp.where(here, m, m_all)
                l_all = jnp.where(here, l, l_all)
                p_list.append(p)
            p_sc[new, pair] = jnp.concatenate(p_list, axis=0).astype(jnp.bfloat16)
        o_buf[u2, o_rows:o_rows + heads, :] = m_all
        o_buf[u2, o_rows + heads:o_rows + 2 * heads, :] = l_all
        row1, kslot = block_row(b1), b1 % NBK
        for pair in range(BR // 2):
            r = 2 * pair
            left = jnp.concatenate([q_rows(row1 + r), zeros_q], axis=0)
            right = jnp.concatenate([zeros_q, q_rows(row1 + r + 1)], axis=0)
            q_pair = jnp.concatenate([left, right], axis=1).astype(jnp.bfloat16)
            k_pair = jnp.concatenate([kbuf[kslot, r], kbuf[kslot, r + 1]], axis=1)
            s_sc[new, pair] = lax.dot_general(q_pair, k_pair, (((1,), (1,)), ((), ())),
                                         preferred_element_type=jnp.float32)
        u3, vslot = b3 // bq, b3 % NBV
        for pair in range(BR // 2):
            r = 2 * pair
            v_pair = jnp.concatenate([vbuf[vslot, r], vbuf[vslot, r + 1]], axis=1)
            o_pair = jnp.dot(p_sc[old, pair], v_pair, preferred_element_type=jnp.float32)
            for i in range(2):
                o = o_pair[i * heads:(i + 1) * heads, i * head_dim:(i + 1) * head_dim]
                o_buf[u3, pl.ds(pl.multiple_of(((b3 % bq) * BR + r + i) * heads, 8), heads), :] = o

        @pl.when(b + NBK < n_blk)
        def _():
            k_copy(b + NBK).start()

        @pl.when(jnp.logical_and(b >= 2, b - 2 + NBV < n_blk))
        def _():
            v_copy(b - 2 + NBV).start()

        w = b - WO_FROM

        @pl.when(jnp.logical_and(w >= 0, jnp.logical_and(w % 2 == 0, w < 2 * n_tiles)))
        def _():
            wo_copy(w // 2).start()

        @pl.when(w == 2 * n_tiles)
        def _():
            hid_copy.start()

        done = jnp.logical_and(b >= 2, (b - 2) % bq == bq - 1)
        u = b3 // bq

        @pl.when(jnp.logical_and(done, u % 2 == 0))
        def _():
            d2d(u // 2).start()

        @pl.when(jnp.logical_and(done, u % 2 == 1))
        def _():
            d2d(u // 2).wait_recv()
            merge_core(u)

            @pl.when(group_far(u))
            def _():
                xsend(group_piece(u)).start()

    def two_blocks(g, _):
        block(2 * g, 0, 1)
        block(2 * g + 1, 1, 0)
        return 0

    def p_copy(i):
        return remote(p_buf.at[i], p_recv.at[i], p_s.at[i], p_r.at[i], to_tp)

    def yc_copy(i):
        return remote(y_send.at[i], y_core.at[i], yc_s.at[i], yc_r.at[i], to_core)

    def yx_copy(i):
        return remote(y_send.at[i], y_chip.at[i], yx_s.at[i], yx_r.at[i], to_chip)

    def yf_copy(i):
        return remote(y_chip.at[i], y_fwd.at[i], yf_s.at[i], yf_r.at[i], to_core)

    def finish_part(h):
        for k in range(per_part):
            n = h * per_part + k
            xsend(n).wait_recv()
            finish(n)
            at_copy(n).start()

    def project_part(h):
        for k in range(per_part):
            n = h * per_part + k
            at_copy(n).wait_recv()
            for hd in range(heads):
                cols = [att[n * 2 + c, pl.ds(hd, quarter, stride=heads), :] for c in range(2)]
                lhs[k * 2 * quarter:(k + 1) * 2 * quarter, hd * head_dim:(hd + 1) * head_dim] = (
                    jnp.concatenate(cols, axis=0).astype(jnp.bfloat16))

        def tile(t, _):
            if h == 0:
                wo_copy(t).wait()
            i = h * n_tiles + t
            p_buf[i] = jnp.dot(lhs[...], wo[t], preferred_element_type=jnp.float32)
            p_copy(i).start()
            return 0
        lax.fori_loop(0, n_tiles, tile, 0)

    def out_cols(i, on_core):
        return pl.ds(pl.multiple_of(on_core * half + (i % n_tiles) * TN, TN), TN)

    def out_rows(i, on_chip):
        return pl.ds(pl.multiple_of(on_chip * chip_rows + (i // n_tiles) * part_rows, part_rows), part_rows)

    def y_tile(i):
        p_copy(i).wait_recv()
        res = hid[pl.ds(pl.multiple_of((i // n_tiles) * part_rows, part_rows), part_rows),
                  pl.ds(pl.multiple_of((i % n_tiles) * TN, TN), TN)].astype(jnp.float32)
        y = (res + (p_buf[i] + p_recv[i])).astype(jnp.bfloat16)
        y_send[i] = y.astype(jnp.float32)
        y_ref[out_rows(i, chip), out_cols(i, core)] = y
        yx_copy(i).start()
        yc_copy(i).start()

    def y_from_chip(i):
        yx_copy(i).wait_recv()
        yf_copy(i).start()
        y_ref[out_rows(i, 1 - chip), out_cols(i, core)] = y_chip[i].astype(jnp.bfloat16)
        yc_copy(i).wait_recv()
        y_ref[out_rows(i, chip), out_cols(i, 1 - core)] = y_core[i].astype(jnp.bfloat16)

    def y_from_fwd(i):
        yf_copy(i).wait_recv()
        y_ref[out_rows(i, 1 - chip), out_cols(i, 1 - core)] = y_fwd[i].astype(jnp.bfloat16)

    total = NH * n_tiles
    last = (n_blk + 2) // 2
    lax.fori_loop(0, G_FINISH, two_blocks, 0)
    finish_part(0)
    lax.fori_loop(G_FINISH, G_PROJECT, two_blocks, 0)
    project_part(0)

    def two_blocks_and_tile(g, _):
        two_blocks(g, 0)

        @pl.when(g == G_TILE)
        def _():
            hid_copy.wait()

        @pl.when(jnp.logical_and(g >= G_TILE, (g - G_TILE) % 2 == 0))
        def _():
            y_tile((g - G_TILE) // 2)
        return 0
    lax.fori_loop(G_PROJECT, last, two_blocks_and_tile, 0)
    finish_part(1)
    early = (last - G_TILE + 1) // 2
    y_tile(early)
    project_part(1)
    early = early + 1

    def step(s, _):
        @pl.when(s + early < total)
        def _():
            y_tile(s + early)

        @pl.when(s < total)
        def _():
            y_from_chip(s)

        @pl.when(s >= 1)
        def _():
            y_from_fwd(s - 1)
        return 0
    lax.fori_loop(0, total + 1, step, 0)

    for t in range(n_q):
        q_copy(t).wait_send()
    for k in range(2 * NC):
        d2d(k).wait_send()
    for n in range(NC):
        xsend(n).wait_send()
        at_copy(n).wait_send()

    def drain(i, _):
        p_copy(i).wait_send()
        yc_copy(i).wait_send()
        yx_copy(i).wait_send()
        yf_copy(i).wait_send()
        return 0
    lax.fori_loop(0, total, drain, 0)


def attention(seq_lens, cos_t, sin_t, norm_w, b_q, b_k, b_v, hidden, w_q, w_k, w_v, k_cache, v_cache, w_o):
    n_rows, d_model = hidden.shape
    s_dev, head_dim = k_cache.shape[1], k_cache.shape[2]
    heads = w_q.shape[1] // head_dim
    half = d_model // 2
    n_tiles = half // TN
    n_q = w_q.shape[1] // (2 * TN)
    quarter = n_rows // (4 * NC)
    msg = quarter * heads + 2 * heads
    total = NH * n_tiles
    vmem = pl.BlockSpec(memory_space=pltpu.VMEM)
    hbm = pl.BlockSpec(memory_space=pl.ANY)
    f32, bf16 = jnp.float32, jnp.bfloat16
    dma = pltpu.SemaphoreType.DMA
    tile_f32 = pltpu.VMEM((total, n_rows // (2 * NH), TN), f32)
    return pl.pallas_call(
        attn_kernel,
        out_shape=[jax.ShapeDtypeStruct((n_rows, d_model), bf16)] + [jax.ShapeDtypeStruct((n_rows, head_dim), bf16)] * 2,
        in_specs=[pl.BlockSpec(memory_space=pltpu.SMEM)] + [vmem] * 6 + [hbm] * 7,
        out_specs=[vmem] * 3,
        scratch_shapes=[
            pltpu.VMEM((n_rows * heads, head_dim), f32),
            pltpu.VMEM((n_q, n_rows * TN // head_dim, head_dim), f32),
            pltpu.VMEM((n_q, n_rows * TN // head_dim, head_dim), f32),
            pltpu.VMEM((d_model, 2 * head_dim), bf16),
            pltpu.VMEM((heads, head_dim), f32),
            pltpu.VMEM((n_rows, head_dim), f32), pltpu.VMEM((n_rows, head_dim), f32),
            dma((n_rows // NORM_ROWS,)), dma((2,)), dma((n_q,)), dma((n_q,)),
            pltpu.VMEM((NC * 4, msg, head_dim), f32),
            pltpu.VMEM((NC * 2, msg, head_dim), f32),
            pltpu.VMEM((NC, msg, head_dim), f32),
            pltpu.VMEM((NC * 2, quarter * heads, head_dim), f32),
            pltpu.VMEM((n_rows // (2 * NH), heads * head_dim), bf16),
            pltpu.VMEM((2, BR // 2, 2 * heads, s_dev), f32),
            pltpu.VMEM((2, BR // 2, 2 * heads, s_dev), bf16),
            pltpu.VMEM((NC, heads, head_dim), f32),
            tile_f32, tile_f32, tile_f32, tile_f32, tile_f32, tile_f32,
            pltpu.VMEM((n_tiles, heads * head_dim, TN), bf16),
            pltpu.VMEM((n_rows // 2, half), bf16),
            pltpu.VMEM((NBK, BR, s_dev, head_dim), bf16),
            pltpu.VMEM((NBV, BR, s_dev, head_dim), bf16),
            dma((NBK,)), dma((NBV,)), dma((n_tiles,)), dma,
            dma((NC * 2,)), dma((NC * 2,)), dma((NC,)), dma((NC,)), dma((NC,)), dma((NC,)),
            dma((total,)), dma((total,)), dma((total,)), dma((total,)), dma((total,)), dma((total,)),
            dma((total,)), dma((total,)),
        ],
        compiler_params=pltpu.CompilerParams(
            collective_id=0, has_side_effects=True, vmem_limit_bytes=VMEM_LIMIT),
        name="attend",
    )(seq_lens, cos_t, sin_t, norm_w.reshape(-1, 128), b_q.reshape(heads, head_dim), b_k[None], b_v[None], hidden,
      w_q, w_k, w_v, k_cache, v_cache, w_o)


def copy_kernel(parts, y_in, k_in, v_in, y_out, k_out, v_out, buf, kv_buf, in_sem, out_sem):
    rows = y_in.shape[0] // parts
    pairs = [(y_in.at[pl.ds(p * rows, rows)], buf.at[p], y_out.at[pl.ds(p * rows, rows)]) for p in range(parts)]
    pairs += [(k_in, kv_buf.at[0], k_out), (v_in, kv_buf.at[1], v_out)]
    loads = [pltpu.make_async_copy(a, m, in_sem.at[i]) for i, (a, m, _) in enumerate(pairs)]
    stores = [pltpu.make_async_copy(m, z, out_sem.at[i]) for i, (_, m, z) in enumerate(pairs)]
    for c in loads:
        c.start()
    for c, d in zip(loads, stores):
        c.wait()
        d.start()
    for d in stores:
        d.wait()


def copy_out(y, k, v):
    parts = 8
    hbm = pl.BlockSpec(memory_space=pl.ANY)
    dma = pltpu.SemaphoreType.DMA
    return pl.pallas_call(
        functools.partial(copy_kernel, parts),
        out_shape=[jax.ShapeDtypeStruct(a.shape, a.dtype) for a in (y, k, v)],
        in_specs=[hbm] * 3, out_specs=[hbm] * 3,
        scratch_shapes=[pltpu.VMEM((parts, y.shape[0] // parts, y.shape[1]), y.dtype),
                        pltpu.VMEM((2,) + k.shape, k.dtype), dma((parts + 2,)), dma((parts + 2,))],
        name="copy_out",
    )(y, k, v)


def solution(mesh):
    def device_step(hidden, norm_w, w_q, b_q, w_k, b_k, w_v, b_v, w_o, k_cache, v_cache, positions, seq_lens):
        n_rows = hidden.shape[0]
        s_dev, head_dim = k_cache.shape[1], k_cache.shape[3]
        cos_t, sin_t = rope_tables(positions, head_dim)
        outs = attention(seq_lens, cos_t, sin_t, norm_w, b_q, b_k, b_v, hidden, w_q, w_k, w_v,
                         k_cache.reshape(n_rows, s_dev, head_dim), v_cache.reshape(n_rows, s_dev, head_dim), w_o)
        y_out, kb, vb = copy_out(*outs)
        return y_out, kb.reshape(n_rows, 1, head_dim), vb.reshape(n_rows, 1, head_dim)

    col_spec = P(None, 'tp')
    vec_spec = P('tp')
    cache_spec = P('dp', 'sp', 'tp', None)
    group_spec = P('dp', 'tp', None)
    in_specs = (P('dp', None), P(None), col_spec, vec_spec, col_spec, vec_spec, col_spec, vec_spec,
                P('tp', None), cache_spec, cache_spec, P('dp'), P('dp'))
    out_specs = (P('dp', None), group_spec, group_spec)
    return jax.shard_map(device_step, mesh=mesh, in_specs=in_specs, out_specs=out_specs, check_vma=False)
```

```python
import functools

import jax
import jax.numpy as jnp
from jax import lax
from jax.experimental import pallas as pl
from jax.experimental.pallas import tpu as pltpu
from jax.sharding import PartitionSpec as P

RMS_EPS = 1.5625e-7
ROPE_BASE = 10000.0
LOG2E = 1.4426950408889634
NEG = -3e38
NEG_FLOOR = -1e38
MESH = pl.DeviceIdType.MESH
VMEM_LIMIT = 67_043_328


NORM_ROWS = 32
NC = 4
NH = 2
BR = 8
NBK, NBV = 4, 6
TN = 512
G_FINISH, G_PROJECT = 12, 13


def rope_tables(positions, head_dim):
    rot_dim = head_dim // 2
    lane = jnp.arange(head_dim, dtype=jnp.int32)
    freq = ROPE_BASE ** (-2.0 * (lane // 2).astype(jnp.float32) / rot_dim)
    freq = jnp.where(lane < rot_dim, freq, 0.0)
    angles = positions.astype(jnp.float32)[:, None] * freq
    sign = jnp.where(lane % 2 == 0, -1.0, 1.0)
    return jnp.cos(angles), jnp.sin(angles) * sign


def rope(x, cos_t, sin_t, even):
    width = x.shape[-1]
    swapped = jnp.where(even, pltpu.roll(x, width - 1, 1), pltpu.roll(x, 1, 1))
    return (x * cos_t + swapped * sin_t).astype(jnp.bfloat16).astype(jnp.float32)


def attn_kernel(seq_ref, cos_ref, sin_ref, nw_ref, bq_ref, bk_ref, bv_ref, hid_hbm, wq_hbm, wk_hbm, wv_hbm,
                k_hbm, v_hbm, wo_hbm, y_ref, kb_ref, vb_ref,
                q_ref, q_send, q_recv, wkv, bqf, kf_ref, vf_ref, in_sem, wkv_sem, q_s, q_r, o_buf, rd, rx, att, lhs, s_sc, p_sc, new_sc, p_buf, p_recv, y_send, y_core, y_chip, y_fwd, wo, hid,
                kbuf, vbuf, k_sem, v_sem, wo_sem, hid_sem, rd_s, rd_r, rx_s, rx_r, at_s, at_r, p_s, p_r,
                yc_s, yc_r, yx_s, yx_r, yf_s, yf_r):
    n_rows, d_model = y_ref.shape
    s_dev, head_dim = kbuf.shape[2], kbuf.shape[3]
    heads = q_ref.shape[0] // n_rows
    n_tiles = wo.shape[0]
    half = n_tiles * TN
    quarter = n_rows // (4 * NC)
    o_rows = quarter * heads
    chip_rows = n_rows // 2
    bq = quarter // BR
    n_blk = n_rows // BR
    coef = head_dim ** -0.5 * LOG2E

    dp, tp, sp = lax.axis_index("dp"), lax.axis_index("tp"), lax.axis_index("sp")
    chip, core = sp // 2, sp % 2
    to_core = (dp, tp, 2 * chip + (1 - core))
    to_chip = (dp, tp, 2 * (1 - chip) + core)
    to_tp = (dp, 1 - tp, sp)

    def remote(src, dst, s_sem, r_sem, dev):
        return pltpu.make_async_remote_copy(src_ref=src, dst_ref=dst, send_sem=s_sem, recv_sem=r_sem,
                                            device_id=dev, device_id_type=MESH)

    per_part = NC // NH
    part_rows = chip_rows // NH

    def group_piece(u):
        return (u // (4 * per_part)) * per_part + (u % (2 * per_part)) // 2

    def group_far(u):
        return u % (4 * per_part) < 2 * per_part

    def group_row(u):
        near = (u % (4 * per_part)) // (2 * per_part)
        own = u % 2
        on_chip = near * chip + (1 - near) * (1 - chip)
        on_core = own * core + (1 - own) * (1 - core)
        return on_chip * chip_rows + group_piece(u) * 2 * quarter + on_core * quarter

    def kept_group(n, near):
        return (n // per_part) * 4 * per_part + near * 2 * per_part + 2 * (n % per_part) + 1

    def block_row(b):
        return pl.multiple_of(group_row(b // bq) + (b % bq) * BR, BR)

    def k_copy(b):
        return pltpu.make_async_copy(k_hbm.at[pl.ds(block_row(b), BR)], kbuf.at[b % NBK], k_sem.at[b % NBK])

    def v_copy(b):
        return pltpu.make_async_copy(v_hbm.at[pl.ds(block_row(b), BR)], vbuf.at[b % NBV], v_sem.at[b % NBV])

    def wo_copy(t):
        cols = pl.ds(pl.multiple_of(core * half + t * TN, 128), TN)
        return pltpu.make_async_copy(wo_hbm.at[:, cols], wo.at[t], wo_sem.at[t])

    hid_copy = pltpu.make_async_copy(
        hid_hbm.at[pl.ds(pl.multiple_of(chip * chip_rows, 128), chip_rows),
                   pl.ds(pl.multiple_of(core * half, 128), half)], hid, hid_sem)

    n_q = q_send.shape[0]
    tile_heads = TN // head_dim
    k_half = wo.shape[1]

    def in_copy(i):
        rows = pl.ds(pl.multiple_of(i * NORM_ROWS, NORM_ROWS), NORM_ROWS)
        return pltpu.make_async_copy(hid_hbm.at[rows], y_ref.at[rows], in_sem.at[i])

    wk_copy = pltpu.make_async_copy(wk_hbm, wkv.at[:, :head_dim], wkv_sem.at[0])
    wv_copy = pltpu.make_async_copy(wv_hbm, wkv.at[:, head_dim:], wkv_sem.at[1])

    def wq_copy(i):
        cols = pl.ds(pl.multiple_of((core * n_q + i // 2) * TN, TN), TN)
        return pltpu.make_async_copy(wq_hbm.at[pl.ds((i % 2) * k_half, k_half), cols], wo.at[i], wo_sem.at[i])

    n_norm = n_rows // NORM_ROWS
    for i in range(n_norm):
        in_copy(i).start()

    barrier = pltpu.get_barrier_semaphore()
    for dev in (to_core, to_chip, to_tp):
        pl.semaphore_signal(barrier, inc=1, device_id=dev, device_id_type=MESH)

    bqf[...] = bq_ref[...].astype(jnp.float32)

    def norm_rows(i, _):
        rows = pl.ds(pl.multiple_of(i * NORM_ROWS, NORM_ROWS), NORM_ROWS)
        in_copy(i).wait()

        @pl.when(i < 2 * n_q)
        def _():
            wq_copy(i).start()

        @pl.when(i == n_norm - 1)
        def _():
            wk_copy.start()
            wv_copy.start()
        sq = jnp.zeros((NORM_ROWS, 128), jnp.float32)
        for c in range(d_model // 128):
            x = y_ref[rows, c * 128:(c + 1) * 128].astype(jnp.float32)
            sq = sq + x * x
        inv = lax.rsqrt(jnp.sum(sq, axis=-1, keepdims=True) / d_model + RMS_EPS)
        for c in range(d_model // 128):
            x = y_ref[rows, c * 128:(c + 1) * 128].astype(jnp.float32)
            x = x * inv * nw_ref[c:c + 1, :].astype(jnp.float32)
            y_ref[rows, c * 128:(c + 1) * 128] = x.astype(jnp.bfloat16)
        return 0
    lax.fori_loop(0, n_norm, norm_rows, 0)
    pl.semaphore_wait(barrier, 3)

    even = lax.broadcasted_iota(jnp.int32, (n_rows, head_dim), 1) % 2 == 0

    def round_f32(x):
        return x.astype(jnp.bfloat16).astype(jnp.float32)

    def q_copy(t):
        return remote(q_send.at[t], q_recv.at[t], q_s.at[t], q_r.at[t], to_core)

    def q_tile(t, _):
        wq_copy(2 * t).wait()
        wq_copy(2 * t + 1).wait()

        @pl.when(t == n_q - 1)
        def _():
            for b in range(NBV):
                if b < NBK:
                    k_copy(b).start()
                v_copy(b).start()
        acc = jnp.dot(y_ref[:, :k_half], wo[2 * t], preferred_element_type=jnp.float32)
        acc = acc + jnp.dot(y_ref[:, k_half:], wo[2 * t + 1], preferred_element_type=jnp.float32)
        for h in range(tile_heads):
            head = core * (heads // 2) + t * tile_heads + h
            val = round_f32(acc[:, h * head_dim:(h + 1) * head_dim] + bqf[pl.ds(head, 1), :])
            val = rope(val, cos_ref[...], sin_ref[...], even)
            q_ref[pl.ds(head, n_rows, stride=heads), :] = val
            q_send[t, pl.ds(h, n_rows, stride=tile_heads), :] = val
        q_copy(t).start()
        wo_copy(2 * t).start()
        wo_copy(2 * t + 1).start()
        return 0
    lax.fori_loop(0, n_q, q_tile, 0)
    hid_copy.start()

    wk_copy.wait()
    wv_copy.wait()
    kv = jnp.dot(y_ref[...], wkv[...], preferred_element_type=jnp.float32)
    k_rot = rope(round_f32(kv[:, :head_dim] + bk_ref[...].astype(jnp.float32)), cos_ref[...], sin_ref[...], even)
    kf_ref[...] = k_rot
    kb_ref[...] = k_rot.astype(jnp.bfloat16)
    v_val = round_f32(kv[:, head_dim:] + bv_ref[...].astype(jnp.float32))
    vf_ref[...] = v_val
    vb_ref[...] = v_val.astype(jnp.bfloat16)

    def q_take(t, _):
        q_copy(t).wait_recv()
        for h in range(tile_heads):
            head = (1 - core) * (heads // 2) + t * tile_heads + h
            q_ref[pl.ds(head, n_rows, stride=heads), :] = q_recv[t, pl.ds(h, n_rows, stride=tile_heads), :]
        return 0
    lax.fori_loop(0, n_q, q_take, 0)

    lane = lax.broadcasted_iota(jnp.int32, (heads, head_dim), 1)
    pos = lax.broadcasted_iota(jnp.int32, (heads, s_dev), 1) + sp * s_dev
    zeros_q = jnp.zeros((heads, head_dim), jnp.float32)

    def q_rows(row):
        return q_ref[pl.ds(pl.multiple_of(row * heads, 8), heads), :]

    def new_scores(n):
        row0 = chip * chip_rows + n * 2 * quarter + core * quarter

        def rows8(g, acc):
            base = pl.multiple_of(row0 + g * 8, 8)
            k_new = kf_ref[pl.ds(base, 8), :]
            for r in range(8):
                s_new = jnp.sum(q_rows(base + r) * k_new[r:r + 1], axis=-1, keepdims=True)
                acc = jnp.where(lane == g * 8 + r, s_new, acc)
            return acc
        new_sc[n] = lax.fori_loop(0, quarter // 8, rows8, zeros_q)

    for n in range(NC):
        new_scores(n)

    def column(vals, j):
        return jnp.broadcast_to(vals[:, j:j + 1], (heads, head_dim))

    def d2d(k):
        return remote(o_buf.at[2 * k], rd.at[k], rd_s.at[k], rd_r.at[k], to_core)

    def xsend(n):
        return remote(o_buf.at[kept_group(n, 0)], rx.at[n], rx_s.at[n], rx_r.at[n], to_chip)

    def at_copy(n):
        return remote(att.at[n * 2 + core], att.at[n * 2 + core], at_s.at[n], at_r.at[n], to_core)

    def merge_core(u):
        k = u // 2
        m1 = o_buf[u, o_rows:o_rows + heads, :]
        l1 = o_buf[u, o_rows + heads:o_rows + 2 * heads, :]
        m2 = rd[k, o_rows:o_rows + heads, :]
        l2 = rd[k, o_rows + heads:o_rows + 2 * heads, :]
        m = jnp.maximum(m1, m2)
        f1 = jnp.exp2((m1 - m) * coef)
        f2 = jnp.exp2((m2 - m) * coef)
        o_buf[u, o_rows:o_rows + heads, :] = m
        o_buf[u, o_rows + heads:o_rows + 2 * heads, :] = l1 * f1 + l2 * f2

        for j in range(quarter):
            rows = pl.ds(j * heads, heads)
            o_buf[u, rows, :] = o_buf[u, rows, :] * column(f1, j) + rd[k, rows, :] * column(f2, j)

    def finish(n):
        u = kept_group(n, 1)
        row0 = chip * chip_rows + n * 2 * quarter + core * quarter
        m1 = o_buf[u, o_rows:o_rows + heads, :]
        l1 = o_buf[u, o_rows + heads:o_rows + 2 * heads, :]
        m2 = rx[n, o_rows:o_rows + heads, :]
        l2 = rx[n, o_rows + heads:o_rows + 2 * heads, :]
        m3 = new_sc[n]
        m = jnp.maximum(jnp.maximum(m1, m2), m3)
        f1 = jnp.exp2((m1 - m) * coef)
        f2 = jnp.exp2((m2 - m) * coef)
        f3 = jnp.exp2((m3 - m) * coef)
        l = l1 * f1 + l2 * f2 + f3
        f1, f2, f3 = f1 / l, f2 / l, f3 / l

        for j in range(quarter):
            if j % 8 == 0:
                v_new = vf_ref[pl.ds(pl.multiple_of(row0 + j, 8), 8), :]
            rows = pl.ds(j * heads, heads)
            o = o_buf[u, rows, :] * column(f1, j) + rx[n, rows, :] * column(f2, j)
            o = o + column(f3, j) * v_new[j % 8:j % 8 + 1]
            att[n * 2 + core, rows, :] = round_f32(o)

    def block(b, new, old):
        @pl.when(b < n_blk)
        def _():
            k_copy(b).wait()

        b1 = jnp.minimum(b, n_blk - 1)
        b2 = jnp.clip(b - 1, 0, n_blk - 1)
        b3 = jnp.clip(b - 2, 0, n_blk - 1)

        @pl.when(jnp.logical_or(b == 0, b >= 3))
        def _():
            v_copy(b3).wait()

        u2, row2 = b2 // bq, block_row(b2)
        m_all = o_buf[u2, o_rows:o_rows + heads, :]
        l_all = o_buf[u2, o_rows + heads:o_rows + 2 * heads, :]
        for pair in range(BR // 2):
            p_list = []
            for i in range(2):
                r = 2 * pair + i
                s = s_sc[old, pair, i * heads:(i + 1) * heads, :]
                s = jnp.where(pos < seq_ref[row2 + r], s, NEG)
                m = jnp.maximum(jnp.max(s, axis=-1, keepdims=True), NEG_FLOOR)
                p = jnp.exp2((s - m) * coef)
                l = jnp.sum(p, axis=-1, keepdims=True)
                here = lane == (b2 % bq) * BR + r
                m_all = jnp.where(here, m, m_all)
                l_all = jnp.where(here, l, l_all)
                p_list.append(p)
            p_sc[new, pair] = jnp.concatenate(p_list, axis=0).astype(jnp.bfloat16)
        o_buf[u2, o_rows:o_rows + heads, :] = m_all
        o_buf[u2, o_rows + heads:o_rows + 2 * heads, :] = l_all
        row1, kslot = block_row(b1), b1 % NBK
        for pair in range(BR // 2):
            r = 2 * pair
            left = jnp.concatenate([q_rows(row1 + r), zeros_q], axis=0)
            right = jnp.concatenate([zeros_q, q_rows(row1 + r + 1)], axis=0)
            q_pair = jnp.concatenate([left, right], axis=1).astype(jnp.bfloat16)
            k_pair = jnp.concatenate([kbuf[kslot, r], kbuf[kslot, r + 1]], axis=1)
            s_sc[new, pair] = lax.dot_general(q_pair, k_pair, (((1,), (1,)), ((), ())),
                                         preferred_element_type=jnp.float32)
        u3, vslot = b3 // bq, b3 % NBV
        for pair in range(BR // 2):
            r = 2 * pair
            v_pair = jnp.concatenate([vbuf[vslot, r], vbuf[vslot, r + 1]], axis=1)
            o_pair = jnp.dot(p_sc[old, pair], v_pair, preferred_element_type=jnp.float32)
            for i in range(2):
                o = o_pair[i * heads:(i + 1) * heads, i * head_dim:(i + 1) * head_dim]
                o_buf[u3, pl.ds(pl.multiple_of(((b3 % bq) * BR + r + i) * heads, 8), heads), :] = o

        @pl.when(b + NBK < n_blk)
        def _():
            k_copy(b + NBK).start()

        @pl.when(jnp.logical_and(b >= 2, b - 2 + NBV < n_blk))
        def _():
            v_copy(b - 2 + NBV).start()

        done = jnp.logical_and(b >= 2, (b - 2) % bq == bq - 1)
        u = b3 // bq

        @pl.when(jnp.logical_and(done, u % 2 == 0))
        def _():
            d2d(u // 2).start()

        @pl.when(jnp.logical_and(done, u % 2 == 1))
        def _():
            d2d(u // 2).wait_recv()
            merge_core(u)

            @pl.when(group_far(u))
            def _():
                xsend(group_piece(u)).start()

    def two_blocks(g, _):
        block(2 * g, 0, 1)
        block(2 * g + 1, 1, 0)
        return 0

    def p_copy(i):
        return remote(p_buf.at[i], p_recv.at[i], p_s.at[i], p_r.at[i], to_tp)

    def yc_copy(i):
        return remote(y_send.at[i], y_core.at[i], yc_s.at[i], yc_r.at[i], to_core)

    def yx_copy(i):
        return remote(y_send.at[i], y_chip.at[i], yx_s.at[i], yx_r.at[i], to_chip)

    def yf_copy(i):
        return remote(y_chip.at[i], y_fwd.at[i], yf_s.at[i], yf_r.at[i], to_core)

    def finish_part(h):
        for k in range(per_part):
            n = h * per_part + k
            xsend(n).wait_recv()
            finish(n)
            at_copy(n).start()

    def project_part(h):
        for k in range(per_part):
            n = h * per_part + k
            at_copy(n).wait_recv()
            for hd in range(heads):
                cols = [att[n * 2 + c, pl.ds(hd, quarter, stride=heads), :] for c in range(2)]
                lhs[k * 2 * quarter:(k + 1) * 2 * quarter, hd * head_dim:(hd + 1) * head_dim] = (
                    jnp.concatenate(cols, axis=0).astype(jnp.bfloat16))

        def tile(t, _):
            if h == 0:
                wo_copy(t).wait()
            i = h * n_tiles + t
            p_buf[i] = jnp.dot(lhs[...], wo[t], preferred_element_type=jnp.float32)
            p_copy(i).start()
            return 0
        lax.fori_loop(0, n_tiles, tile, 0)

    def out_cols(i, on_core):
        return pl.ds(pl.multiple_of(on_core * half + (i % n_tiles) * TN, TN), TN)

    def out_rows(i, on_chip):
        return pl.ds(pl.multiple_of(on_chip * chip_rows + (i // n_tiles) * part_rows, part_rows), part_rows)

    def y_tile(i):
        p_copy(i).wait_recv()
        res = hid[pl.ds(pl.multiple_of((i // n_tiles) * part_rows, part_rows), part_rows),
                  pl.ds(pl.multiple_of((i % n_tiles) * TN, TN), TN)].astype(jnp.float32)
        y = (res + (p_buf[i] + p_recv[i])).astype(jnp.bfloat16)
        y_send[i] = y.astype(jnp.float32)
        y_ref[out_rows(i, chip), out_cols(i, core)] = y
        yx_copy(i).start()
        yc_copy(i).start()

    def y_from_chip(i):
        yx_copy(i).wait_recv()
        yf_copy(i).start()
        y_ref[out_rows(i, 1 - chip), out_cols(i, core)] = y_chip[i].astype(jnp.bfloat16)
        yc_copy(i).wait_recv()
        y_ref[out_rows(i, chip), out_cols(i, 1 - core)] = y_core[i].astype(jnp.bfloat16)

    def y_from_fwd(i):
        yf_copy(i).wait_recv()
        y_ref[out_rows(i, 1 - chip), out_cols(i, 1 - core)] = y_fwd[i].astype(jnp.bfloat16)

    total = NH * n_tiles
    last = (n_blk + 2) // 2
    lax.fori_loop(0, G_FINISH, two_blocks, 0)
    finish_part(0)
    lax.fori_loop(G_FINISH, G_PROJECT, two_blocks, 0)
    project_part(0)

    def two_blocks_and_tile(g, _):
        two_blocks(g, 0)

        @pl.when(g == last - 3)
        def _():
            hid_copy.wait()

        @pl.when(jnp.logical_or(g == last - 3, g == last - 1))
        def _():
            y_tile((g - (last - 3)) // 2)
        return 0
    lax.fori_loop(G_PROJECT, last, two_blocks_and_tile, 0)
    finish_part(1)
    y_tile(2)
    project_part(1)
    early = 3

    def step(s, _):
        @pl.when(s + early < total)
        def _():
            y_tile(s + early)

        @pl.when(s < total)
        def _():
            y_from_chip(s)

        @pl.when(s >= 1)
        def _():
            y_from_fwd(s - 1)
        return 0
    lax.fori_loop(0, total + 1, step, 0)

    for t in range(n_q):
        q_copy(t).wait_send()
    for k in range(2 * NC):
        d2d(k).wait_send()
    for n in range(NC):
        xsend(n).wait_send()
        at_copy(n).wait_send()

    def drain(i, _):
        p_copy(i).wait_send()
        yc_copy(i).wait_send()
        yx_copy(i).wait_send()
        yf_copy(i).wait_send()
        return 0
    lax.fori_loop(0, total, drain, 0)


def attention(seq_lens, cos_t, sin_t, norm_w, b_q, b_k, b_v, hidden, w_q, w_k, w_v, k_cache, v_cache, w_o):
    n_rows, d_model = hidden.shape
    s_dev, head_dim = k_cache.shape[1], k_cache.shape[2]
    heads = w_q.shape[1] // head_dim
    half = d_model // 2
    n_tiles = half // TN
    n_q = w_q.shape[1] // (2 * TN)
    quarter = n_rows // (4 * NC)
    msg = quarter * heads + 2 * heads
    total = NH * n_tiles
    vmem = pl.BlockSpec(memory_space=pltpu.VMEM)
    hbm = pl.BlockSpec(memory_space=pl.ANY)
    f32, bf16 = jnp.float32, jnp.bfloat16
    dma = pltpu.SemaphoreType.DMA
    tile_f32 = pltpu.VMEM((total, n_rows // (2 * NH), TN), f32)
    return pl.pallas_call(
        attn_kernel,
        out_shape=[jax.ShapeDtypeStruct((n_rows, d_model), bf16)] + [jax.ShapeDtypeStruct((n_rows, head_dim), bf16)] * 2,
        in_specs=[pl.BlockSpec(memory_space=pltpu.SMEM)] + [vmem] * 6 + [hbm] * 7,
        out_specs=[vmem] * 3,
        scratch_shapes=[
            pltpu.VMEM((n_rows * heads, head_dim), f32),
            pltpu.VMEM((n_q, n_rows * TN // head_dim, head_dim), f32),
            pltpu.VMEM((n_q, n_rows * TN // head_dim, head_dim), f32),
            pltpu.VMEM((d_model, 2 * head_dim), bf16),
            pltpu.VMEM((heads, head_dim), f32),
            pltpu.VMEM((n_rows, head_dim), f32), pltpu.VMEM((n_rows, head_dim), f32),
            dma((n_rows // NORM_ROWS,)), dma((2,)), dma((n_q,)), dma((n_q,)),
            pltpu.VMEM((NC * 4, msg, head_dim), f32),
            pltpu.VMEM((NC * 2, msg, head_dim), f32),
            pltpu.VMEM((NC, msg, head_dim), f32),
            pltpu.VMEM((NC * 2, quarter * heads, head_dim), f32),
            pltpu.VMEM((n_rows // (2 * NH), heads * head_dim), bf16),
            pltpu.VMEM((2, BR // 2, 2 * heads, s_dev), f32),
            pltpu.VMEM((2, BR // 2, 2 * heads, s_dev), bf16),
            pltpu.VMEM((NC, heads, head_dim), f32),
            tile_f32, tile_f32, tile_f32, tile_f32, tile_f32, tile_f32,
            pltpu.VMEM((n_tiles, heads * head_dim, TN), bf16),
            pltpu.VMEM((n_rows // 2, half), bf16),
            pltpu.VMEM((NBK, BR, s_dev, head_dim), bf16),
            pltpu.VMEM((NBV, BR, s_dev, head_dim), bf16),
            dma((NBK,)), dma((NBV,)), dma((n_tiles,)), dma,
            dma((NC * 2,)), dma((NC * 2,)), dma((NC,)), dma((NC,)), dma((NC,)), dma((NC,)),
            dma((total,)), dma((total,)), dma((total,)), dma((total,)), dma((total,)), dma((total,)),
            dma((total,)), dma((total,)),
        ],
        compiler_params=pltpu.CompilerParams(
            collective_id=0, has_side_effects=True, vmem_limit_bytes=VMEM_LIMIT),
        name="attend",
    )(seq_lens, cos_t, sin_t, norm_w.reshape(-1, 128), b_q.reshape(heads, head_dim), b_k[None], b_v[None], hidden,
      w_q, w_k, w_v, k_cache, v_cache, w_o)


def copy_kernel(parts, y_in, k_in, v_in, y_out, k_out, v_out, buf, kv_buf, in_sem, out_sem):
    rows = y_in.shape[0] // parts
    pairs = [(y_in.at[pl.ds(p * rows, rows)], buf.at[p], y_out.at[pl.ds(p * rows, rows)]) for p in range(parts)]
    pairs += [(k_in, kv_buf.at[0], k_out), (v_in, kv_buf.at[1], v_out)]
    loads = [pltpu.make_async_copy(a, m, in_sem.at[i]) for i, (a, m, _) in enumerate(pairs)]
    stores = [pltpu.make_async_copy(m, z, out_sem.at[i]) for i, (_, m, z) in enumerate(pairs)]
    for c in loads:
        c.start()
    for c, d in zip(loads, stores):
        c.wait()
        d.start()
    for d in stores:
        d.wait()


def copy_out(y, k, v):
    parts = 8
    hbm = pl.BlockSpec(memory_space=pl.ANY)
    dma = pltpu.SemaphoreType.DMA
    return pl.pallas_call(
        functools.partial(copy_kernel, parts),
        out_shape=[jax.ShapeDtypeStruct(a.shape, a.dtype) for a in (y, k, v)],
        in_specs=[hbm] * 3, out_specs=[hbm] * 3,
        scratch_shapes=[pltpu.VMEM((parts, y.shape[0] // parts, y.shape[1]), y.dtype),
                        pltpu.VMEM((2,) + k.shape, k.dtype), dma((parts + 2,)), dma((parts + 2,))],
        name="copy_out",
    )(y, k, v)


def solution(mesh):
    def device_step(hidden, norm_w, w_q, b_q, w_k, b_k, w_v, b_v, w_o, k_cache, v_cache, positions, seq_lens):
        n_rows = hidden.shape[0]
        s_dev, head_dim = k_cache.shape[1], k_cache.shape[3]
        cos_t, sin_t = rope_tables(positions, head_dim)
        outs = attention(seq_lens, cos_t, sin_t, norm_w, b_q, b_k, b_v, hidden, w_q, w_k, w_v,
                         k_cache.reshape(n_rows, s_dev, head_dim), v_cache.reshape(n_rows, s_dev, head_dim), w_o)
        y_out, kb, vb = copy_out(*outs)
        return y_out, kb.reshape(n_rows, 1, head_dim), vb.reshape(n_rows, 1, head_dim)

    col_spec = P(None, 'tp')
    vec_spec = P('tp')
    cache_spec = P('dp', 'sp', 'tp', None)
    group_spec = P('dp', 'tp', None)
    in_specs = (P('dp', None), P(None), col_spec, vec_spec, col_spec, vec_spec, col_spec, vec_spec,
                P('tp', None), cache_spec, cache_spec, P('dp'), P('dp'))
    out_specs = (P('dp', None), group_spec, group_spec)
    return jax.shard_map(device_step, mesh=mesh, in_specs=in_specs, out_specs=out_specs, check_vma=False)
```

```python
import functools

import jax
import jax.numpy as jnp
from jax import lax
from jax.experimental import pallas as pl
from jax.experimental.pallas import tpu as pltpu
from jax.sharding import PartitionSpec as P

RMS_EPS = 1.5625e-7
ROPE_BASE = 10000.0
LOG2E = 1.4426950408889634
NEG = -3e38
NEG_FLOOR = -1e38
MESH = pl.DeviceIdType.MESH
VMEM_LIMIT = 67_043_328


NORM_ROWS = 32
NC = 4
NH = 2
BR = 8
NBK, NBV = 4, 6
TN = 512
TS = 256
G_FINISH, G_PROJECT = 12, 13


def rope_tables(positions, head_dim):
    rot_dim = head_dim // 2
    lane = jnp.arange(head_dim, dtype=jnp.int32)
    freq = ROPE_BASE ** (-2.0 * (lane // 2).astype(jnp.float32) / rot_dim)
    freq = jnp.where(lane < rot_dim, freq, 0.0)
    angles = positions.astype(jnp.float32)[:, None] * freq
    sign = jnp.where(lane % 2 == 0, -1.0, 1.0)
    return jnp.cos(angles), jnp.sin(angles) * sign


def rope(x, cos_t, sin_t, even):
    width = x.shape[-1]
    swapped = jnp.where(even, pltpu.roll(x, width - 1, 1), pltpu.roll(x, 1, 1))
    return (x * cos_t + swapped * sin_t).astype(jnp.bfloat16).astype(jnp.float32)


def attn_kernel(seq_ref, cos_ref, sin_ref, nw_ref, bq_ref, bk_ref, bv_ref, hid_hbm, wq_hbm, wk_hbm, wv_hbm,
                k_hbm, v_hbm, wo_hbm, y_ref, kb_ref, vb_ref,
                q_ref, q_send, q_recv, wkv, bqf, kf_ref, vf_ref, in_sem, wkv_sem, q_s, q_r, o_buf, rd, rx, att, lhs, s_sc, p_sc, new_sc, p_buf, p_recv, y_send, y_core, y_chip, y_fwd, wo, hid,
                kbuf, vbuf, k_sem, v_sem, wo_sem, hid_sem, rd_s, rd_r, rx_s, rx_r, at_s, at_r, p_s, p_r,
                yc_s, yc_r, yx_s, yx_r, yf_s, yf_r):
    n_rows, d_model = y_ref.shape
    s_dev, head_dim = kbuf.shape[2], kbuf.shape[3]
    heads = q_ref.shape[0] // n_rows
    n_tiles = wo.shape[0]
    half = n_tiles * TN
    quarter = n_rows // (4 * NC)
    o_rows = quarter * heads
    chip_rows = n_rows // 2
    bq = quarter // BR
    n_blk = n_rows // BR
    coef = head_dim ** -0.5 * LOG2E

    dp, tp, sp = lax.axis_index("dp"), lax.axis_index("tp"), lax.axis_index("sp")
    chip, core = sp // 2, sp % 2
    to_core = (dp, tp, 2 * chip + (1 - core))
    to_chip = (dp, tp, 2 * (1 - chip) + core)
    to_tp = (dp, 1 - tp, sp)

    def remote(src, dst, s_sem, r_sem, dev):
        return pltpu.make_async_remote_copy(src_ref=src, dst_ref=dst, send_sem=s_sem, recv_sem=r_sem,
                                            device_id=dev, device_id_type=MESH)

    per_part = NC // NH
    part_rows = chip_rows // NH

    def group_piece(u):
        return (u // (4 * per_part)) * per_part + (u % (2 * per_part)) // 2

    def group_far(u):
        return u % (4 * per_part) < 2 * per_part

    def group_row(u):
        near = (u % (4 * per_part)) // (2 * per_part)
        own = u % 2
        on_chip = near * chip + (1 - near) * (1 - chip)
        on_core = own * core + (1 - own) * (1 - core)
        return on_chip * chip_rows + group_piece(u) * 2 * quarter + on_core * quarter

    def kept_group(n, near):
        return (n // per_part) * 4 * per_part + near * 2 * per_part + 2 * (n % per_part) + 1

    def block_row(b):
        return pl.multiple_of(group_row(b // bq) + (b % bq) * BR, BR)

    def k_copy(b):
        return pltpu.make_async_copy(k_hbm.at[pl.ds(block_row(b), BR)], kbuf.at[b % NBK], k_sem.at[b % NBK])

    def v_copy(b):
        return pltpu.make_async_copy(v_hbm.at[pl.ds(block_row(b), BR)], vbuf.at[b % NBV], v_sem.at[b % NBV])

    def wo_copy(t):
        cols = pl.ds(pl.multiple_of(core * half + t * TN, 128), TN)
        return pltpu.make_async_copy(wo_hbm.at[:, cols], wo.at[t], wo_sem.at[t])

    hid_copy = pltpu.make_async_copy(
        hid_hbm.at[pl.ds(pl.multiple_of(chip * chip_rows, 128), chip_rows),
                   pl.ds(pl.multiple_of(core * half, 128), half)], hid, hid_sem)

    n_q = q_send.shape[0]
    tile_heads = TN // head_dim
    k_half = wo.shape[1]

    def in_copy(i):
        rows = pl.ds(pl.multiple_of(i * NORM_ROWS, NORM_ROWS), NORM_ROWS)
        return pltpu.make_async_copy(hid_hbm.at[rows], y_ref.at[rows], in_sem.at[i])

    wk_copy = pltpu.make_async_copy(wk_hbm, wkv.at[:, :head_dim], wkv_sem.at[0])
    wv_copy = pltpu.make_async_copy(wv_hbm, wkv.at[:, head_dim:], wkv_sem.at[1])

    def wq_copy(i):
        cols = pl.ds(pl.multiple_of((core * n_q + i // 2) * TN, TN), TN)
        return pltpu.make_async_copy(wq_hbm.at[pl.ds((i % 2) * k_half, k_half), cols], wo.at[i], wo_sem.at[i])

    n_norm = n_rows // NORM_ROWS
    for i in range(n_norm):
        in_copy(i).start()

    barrier = pltpu.get_barrier_semaphore()
    for dev in (to_core, to_chip, to_tp):
        pl.semaphore_signal(barrier, inc=1, device_id=dev, device_id_type=MESH)

    bqf[...] = bq_ref[...].astype(jnp.float32)

    def norm_rows(i, _):
        rows = pl.ds(pl.multiple_of(i * NORM_ROWS, NORM_ROWS), NORM_ROWS)
        in_copy(i).wait()

        @pl.when(i < 2 * n_q)
        def _():
            wq_copy(i).start()

        @pl.when(i == n_norm - 1)
        def _():
            wk_copy.start()
            wv_copy.start()
        sq = jnp.zeros((NORM_ROWS, 128), jnp.float32)
        for c in range(d_model // 128):
            x = y_ref[rows, c * 128:(c + 1) * 128].astype(jnp.float32)
            sq = sq + x * x
        inv = lax.rsqrt(jnp.sum(sq, axis=-1, keepdims=True) / d_model + RMS_EPS)
        for c in range(d_model // 128):
            x = y_ref[rows, c * 128:(c + 1) * 128].astype(jnp.float32)
            x = x * inv * nw_ref[c:c + 1, :].astype(jnp.float32)
            y_ref[rows, c * 128:(c + 1) * 128] = x.astype(jnp.bfloat16)
        return 0
    lax.fori_loop(0, n_norm, norm_rows, 0)
    pl.semaphore_wait(barrier, 3)

    even = lax.broadcasted_iota(jnp.int32, (n_rows, head_dim), 1) % 2 == 0

    def round_f32(x):
        return x.astype(jnp.bfloat16).astype(jnp.float32)

    def q_copy(t):
        return remote(q_send.at[t], q_recv.at[t], q_s.at[t], q_r.at[t], to_core)

    def q_tile(t, _):
        wq_copy(2 * t).wait()
        wq_copy(2 * t + 1).wait()

        @pl.when(t == n_q - 1)
        def _():
            for b in range(NBV):
                if b < NBK:
                    k_copy(b).start()
                v_copy(b).start()
        acc = jnp.dot(y_ref[:, :k_half], wo[2 * t], preferred_element_type=jnp.float32)
        acc = acc + jnp.dot(y_ref[:, k_half:], wo[2 * t + 1], preferred_element_type=jnp.float32)
        for h in range(tile_heads):
            head = core * (heads // 2) + t * tile_heads + h
            val = round_f32(acc[:, h * head_dim:(h + 1) * head_dim] + bqf[pl.ds(head, 1), :])
            val = rope(val, cos_ref[...], sin_ref[...], even)
            q_ref[pl.ds(head, n_rows, stride=heads), :] = val
            q_send[t, pl.ds(h, n_rows, stride=tile_heads), :] = val
        q_copy(t).start()
        wo_copy(2 * t).start()
        wo_copy(2 * t + 1).start()
        return 0
    lax.fori_loop(0, n_q, q_tile, 0)
    hid_copy.start()

    wk_copy.wait()
    wv_copy.wait()
    kv = jnp.dot(y_ref[...], wkv[...], preferred_element_type=jnp.float32)
    k_rot = rope(round_f32(kv[:, :head_dim] + bk_ref[...].astype(jnp.float32)), cos_ref[...], sin_ref[...], even)
    kf_ref[...] = k_rot
    kb_ref[...] = k_rot.astype(jnp.bfloat16)
    v_val = round_f32(kv[:, head_dim:] + bv_ref[...].astype(jnp.float32))
    vf_ref[...] = v_val
    vb_ref[...] = v_val.astype(jnp.bfloat16)

    def q_take(t, _):
        q_copy(t).wait_recv()
        for h in range(tile_heads):
            head = (1 - core) * (heads // 2) + t * tile_heads + h
            q_ref[pl.ds(head, n_rows, stride=heads), :] = q_recv[t, pl.ds(h, n_rows, stride=tile_heads), :]
        return 0
    lax.fori_loop(0, n_q, q_take, 0)

    lane = lax.broadcasted_iota(jnp.int32, (heads, head_dim), 1)
    pos = lax.broadcasted_iota(jnp.int32, (heads, s_dev), 1) + sp * s_dev
    zeros_q = jnp.zeros((heads, head_dim), jnp.float32)

    def q_rows(row):
        return q_ref[pl.ds(pl.multiple_of(row * heads, 8), heads), :]

    def new_scores(n):
        row0 = chip * chip_rows + n * 2 * quarter + core * quarter

        def rows8(g, acc):
            base = pl.multiple_of(row0 + g * 8, 8)
            k_new = kf_ref[pl.ds(base, 8), :]
            for r in range(8):
                s_new = jnp.sum(q_rows(base + r) * k_new[r:r + 1], axis=-1, keepdims=True)
                acc = jnp.where(lane == g * 8 + r, s_new, acc)
            return acc
        new_sc[n] = lax.fori_loop(0, quarter // 8, rows8, zeros_q)

    def column(vals, j):
        return jnp.broadcast_to(vals[:, j:j + 1], (heads, head_dim))

    def d2d(k):
        return remote(o_buf.at[2 * k], rd.at[k], rd_s.at[k], rd_r.at[k], to_core)

    def xsend(n):
        return remote(o_buf.at[kept_group(n, 0)], rx.at[n], rx_s.at[n], rx_r.at[n], to_chip)

    def at_copy(n):
        return remote(att.at[n * 2 + core], att.at[n * 2 + core], at_s.at[n], at_r.at[n], to_core)

    def merge_core(u):
        k = u // 2
        st1 = o_buf[u, o_rows:o_rows + heads, :]
        st2 = rd[k, o_rows:o_rows + heads, :]
        m = jnp.maximum(st1, st2)
        f1 = jnp.exp2((st1 - m) * coef)
        f2 = jnp.exp2((st2 - m) * coef)
        l = st1 * pltpu.roll(f1, quarter, 1) + st2 * pltpu.roll(f2, quarter, 1)
        o_buf[u, o_rows:o_rows + heads, :] = jnp.where(lane < quarter, m, l)

        for j in range(quarter):
            rows = pl.ds(j * heads, heads)
            o_buf[u, rows, :] = o_buf[u, rows, :] * column(f1, j) + rd[k, rows, :] * column(f2, j)

    def finish(n):
        u = kept_group(n, 1)
        row0 = chip * chip_rows + n * 2 * quarter + core * quarter
        st1 = o_buf[u, o_rows:o_rows + heads, :]
        st2 = rx[n, o_rows:o_rows + heads, :]
        m3 = new_sc[n]
        m = jnp.maximum(jnp.maximum(st1, st2), m3)
        f1 = jnp.exp2((st1 - m) * coef)
        f2 = jnp.exp2((st2 - m) * coef)
        f3 = jnp.exp2((m3 - m) * coef)
        l = st1 * pltpu.roll(f1, quarter, 1) + st2 * pltpu.roll(f2, quarter, 1) + pltpu.roll(f3, quarter, 1)
        l = pltpu.roll(l, head_dim - quarter, 1)
        f1, f2, f3 = f1 / l, f2 / l, f3 / l

        for j in range(quarter):
            if j % 8 == 0:
                v_new = vf_ref[pl.ds(pl.multiple_of(row0 + j, 8), 8), :]
            rows = pl.ds(j * heads, heads)
            o = o_buf[u, rows, :] * column(f1, j) + rx[n, rows, :] * column(f2, j)
            o = o + column(f3, j) * v_new[j % 8:j % 8 + 1]
            att[n * 2 + core, rows, :] = round_f32(o)

    def block(b, new, old):
        @pl.when(b < n_blk)
        def _():
            k_copy(b).wait()

        b1 = jnp.minimum(b, n_blk - 1)
        b2 = jnp.clip(b - 1, 0, n_blk - 1)
        b3 = jnp.clip(b - 2, 0, n_blk - 1)

        @pl.when(jnp.logical_or(b == 0, b >= 3))
        def _():
            v_copy(b3).wait()

        u2, row2 = b2 // bq, block_row(b2)
        stats = o_buf[u2, o_rows:o_rows + heads, :]
        for pair in range(BR // 2):
            p_list = []
            for i in range(2):
                r = 2 * pair + i
                s = s_sc[old, pair, i * heads:(i + 1) * heads, :]
                s = jnp.where(pos < seq_ref[row2 + r], s, NEG)
                m = jnp.maximum(jnp.max(s, axis=-1, keepdims=True), NEG_FLOOR)
                p = jnp.exp2((s - m) * coef)
                l = jnp.sum(p, axis=-1, keepdims=True)
                j = (b2 % bq) * BR + r
                stats = jnp.where(lane == j, m, jnp.where(lane == quarter + j, l, stats))
                p_list.append(p)
            p_sc[new, pair] = jnp.concatenate(p_list, axis=0).astype(jnp.bfloat16)
        o_buf[u2, o_rows:o_rows + heads, :] = stats
        row1, kslot = block_row(b1), b1 % NBK
        for pair in range(BR // 2):
            r = 2 * pair
            left = jnp.concatenate([q_rows(row1 + r), zeros_q], axis=0)
            right = jnp.concatenate([zeros_q, q_rows(row1 + r + 1)], axis=0)
            q_pair = jnp.concatenate([left, right], axis=1).astype(jnp.bfloat16)
            k_pair = jnp.concatenate([kbuf[kslot, r], kbuf[kslot, r + 1]], axis=1)
            s_sc[new, pair] = lax.dot_general(q_pair, k_pair, (((1,), (1,)), ((), ())),
                                         preferred_element_type=jnp.float32)
        u3, vslot = b3 // bq, b3 % NBV
        for pair in range(BR // 2):
            r = 2 * pair
            v_pair = jnp.concatenate([vbuf[vslot, r], vbuf[vslot, r + 1]], axis=1)
            o_pair = jnp.dot(p_sc[old, pair], v_pair, preferred_element_type=jnp.float32)
            for i in range(2):
                o = o_pair[i * heads:(i + 1) * heads, i * head_dim:(i + 1) * head_dim]
                o_buf[u3, pl.ds(pl.multiple_of(((b3 % bq) * BR + r + i) * heads, 8), heads), :] = o

        @pl.when(b + NBK < n_blk)
        def _():
            k_copy(b + NBK).start()

        @pl.when(jnp.logical_and(b >= 2, b - 2 + NBV < n_blk))
        def _():
            v_copy(b - 2 + NBV).start()

        done = jnp.logical_and(b >= 2, (b - 2) % bq == bq - 1)
        u = b3 // bq

        @pl.when(jnp.logical_and(done, u % 2 == 0))
        def _():
            d2d(u // 2).start()

        @pl.when(jnp.logical_and(done, u % 2 == 1))
        def _():
            d2d(u // 2).wait_recv()
            merge_core(u)

            @pl.when(group_far(u))
            def _():
                xsend(group_piece(u)).start()

    def two_blocks(g, _):
        block(2 * g, 0, 1)
        block(2 * g + 1, 1, 0)
        return 0

    def p_copy(i):
        return remote(p_buf.at[i], p_recv.at[i], p_s.at[i], p_r.at[i], to_tp)

    def yc_copy(i):
        return remote(y_send.at[i], y_core.at[i], yc_s.at[i], yc_r.at[i], to_core)

    def yx_copy(i):
        return remote(y_send.at[i], y_chip.at[i], yx_s.at[i], yx_r.at[i], to_chip)

    def yf_copy(i):
        return remote(y_chip.at[i], y_fwd.at[i], yf_s.at[i], yf_r.at[i], to_core)

    per = TN // TS
    n_sub = n_tiles * per

    def finish_part(h):
        for k in range(per_part):
            n = h * per_part + k
            xsend(n).wait_recv()
            finish(n)
            at_copy(n).start()

    def project_part(h):
        for k in range(per_part):
            n = h * per_part + k
            at_copy(n).wait_recv()
            for hd in range(heads):
                cols = [att[n * 2 + c, pl.ds(hd, quarter, stride=heads), :] for c in range(2)]
                lhs[k * 2 * quarter:(k + 1) * 2 * quarter, hd * head_dim:(hd + 1) * head_dim] = (
                    jnp.concatenate(cols, axis=0).astype(jnp.bfloat16))

        def tile(t, _):
            if h == 0:
                wo_copy(t).wait()
            res = jnp.dot(lhs[...], wo[t], preferred_element_type=jnp.float32)
            for k in range(per):
                i = h * n_sub + t * per + k
                p_buf[i] = res[:, k * TS:(k + 1) * TS]
                p_copy(i).start()
            if h == 1:
                @pl.when(t % 2 == 1)
                def _():
                    y_tile(early + t // 2)
            return 0
        lax.fori_loop(0, n_tiles, tile, 0)

    def out_cols(i, on_core):
        return pl.ds(pl.multiple_of(on_core * half + (i % n_sub) * TS, TS), TS)

    def out_rows(i, on_chip):
        return pl.ds(pl.multiple_of(on_chip * chip_rows + (i // n_sub) * part_rows, part_rows), part_rows)

    def y_tile(i):
        p_copy(i).wait_recv()
        res = hid[pl.ds(pl.multiple_of((i // n_sub) * part_rows, part_rows), part_rows),
                  pl.ds(pl.multiple_of((i % n_sub) * TS, TS), TS)].astype(jnp.float32)
        y = (res + (p_buf[i] + p_recv[i])).astype(jnp.bfloat16)
        y_send[i] = y.astype(jnp.float32)
        y_ref[out_rows(i, chip), out_cols(i, core)] = y
        yx_copy(i).start()
        yc_copy(i).start()

    def y_from_chip(i):
        yx_copy(i).wait_recv()
        yf_copy(i).start()
        y_ref[out_rows(i, 1 - chip), out_cols(i, core)] = y_chip[i].astype(jnp.bfloat16)
        yc_copy(i).wait_recv()
        y_ref[out_rows(i, chip), out_cols(i, 1 - core)] = y_core[i].astype(jnp.bfloat16)

    def y_from_fwd(i):
        yf_copy(i).wait_recv()
        y_ref[out_rows(i, 1 - chip), out_cols(i, 1 - core)] = y_fwd[i].astype(jnp.bfloat16)

    total = NH * n_sub
    last = (n_blk + 2) // 2
    lax.fori_loop(0, G_FINISH, two_blocks, 0)
    for n in range(NC):
        new_scores(n)
    finish_part(0)
    lax.fori_loop(G_FINISH, G_PROJECT, two_blocks, 0)
    early = last - G_PROJECT + 2
    project_part(0)
    hid_copy.wait()

    def two_blocks_and_tile(g, _):
        two_blocks(g, 0)
        y_tile(g - G_PROJECT)
        return 0
    lax.fori_loop(G_PROJECT, last, two_blocks_and_tile, 0)
    finish_part(1)
    y_tile(early - 2)
    y_tile(early - 1)
    project_part(1)
    early = early + n_tiles // 2

    def step(s, _):
        @pl.when(s + early < total)
        def _():
            y_tile(s + early)

        @pl.when(s < total)
        def _():
            y_from_chip(s)

        @pl.when(s >= 1)
        def _():
            y_from_fwd(s - 1)
        return 0
    lax.fori_loop(0, total + 1, step, 0)

    for t in range(n_q):
        q_copy(t).wait_send()
    for k in range(2 * NC):
        d2d(k).wait_send()
    for n in range(NC):
        xsend(n).wait_send()
        at_copy(n).wait_send()

    def drain(i, _):
        p_copy(i).wait_send()
        yc_copy(i).wait_send()
        yx_copy(i).wait_send()
        yf_copy(i).wait_send()
        return 0
    lax.fori_loop(0, total, drain, 0)


def attention(seq_lens, cos_t, sin_t, norm_w, b_q, b_k, b_v, hidden, w_q, w_k, w_v, k_cache, v_cache, w_o):
    n_rows, d_model = hidden.shape
    s_dev, head_dim = k_cache.shape[1], k_cache.shape[2]
    heads = w_q.shape[1] // head_dim
    half = d_model // 2
    n_tiles = half // TN
    n_q = w_q.shape[1] // (2 * TN)
    quarter = n_rows // (4 * NC)
    msg = quarter * heads + heads
    total = NH * n_tiles * (TN // TS)
    vmem = pl.BlockSpec(memory_space=pltpu.VMEM)
    hbm = pl.BlockSpec(memory_space=pl.ANY)
    f32, bf16 = jnp.float32, jnp.bfloat16
    dma = pltpu.SemaphoreType.DMA
    tile_f32 = pltpu.VMEM((total, n_rows // (2 * NH), TS), f32)
    return pl.pallas_call(
        attn_kernel,
        out_shape=[jax.ShapeDtypeStruct((n_rows, d_model), bf16)] + [jax.ShapeDtypeStruct((n_rows, head_dim), bf16)] * 2,
        in_specs=[pl.BlockSpec(memory_space=pltpu.SMEM)] + [vmem] * 6 + [hbm] * 7,
        out_specs=[vmem] * 3,
        scratch_shapes=[
            pltpu.VMEM((n_rows * heads, head_dim), f32),
            pltpu.VMEM((n_q, n_rows * TN // head_dim, head_dim), f32),
            pltpu.VMEM((n_q, n_rows * TN // head_dim, head_dim), f32),
            pltpu.VMEM((d_model, 2 * head_dim), bf16),
            pltpu.VMEM((heads, head_dim), f32),
            pltpu.VMEM((n_rows, head_dim), f32), pltpu.VMEM((n_rows, head_dim), f32),
            dma((n_rows // NORM_ROWS,)), dma((2,)), dma((n_q,)), dma((n_q,)),
            pltpu.VMEM((NC * 4, msg, head_dim), f32),
            pltpu.VMEM((NC * 2, msg, head_dim), f32),
            pltpu.VMEM((NC, msg, head_dim), f32),
            pltpu.VMEM((NC * 2, quarter * heads, head_dim), f32),
            pltpu.VMEM((n_rows // (2 * NH), heads * head_dim), bf16),
            pltpu.VMEM((2, BR // 2, 2 * heads, s_dev), f32),
            pltpu.VMEM((2, BR // 2, 2 * heads, s_dev), bf16),
            pltpu.VMEM((NC, heads, head_dim), f32),
            tile_f32, tile_f32, tile_f32, tile_f32, tile_f32, tile_f32,
            pltpu.VMEM((n_tiles, heads * head_dim, TN), bf16),
            pltpu.VMEM((n_rows // 2, half), bf16),
            pltpu.VMEM((NBK, BR, s_dev, head_dim), bf16),
            pltpu.VMEM((NBV, BR, s_dev, head_dim), bf16),
            dma((NBK,)), dma((NBV,)), dma((n_tiles,)), dma,
            dma((NC * 2,)), dma((NC * 2,)), dma((NC,)), dma((NC,)), dma((NC,)), dma((NC,)),
            dma((total,)), dma((total,)), dma((total,)), dma((total,)), dma((total,)), dma((total,)),
            dma((total,)), dma((total,)),
        ],
        compiler_params=pltpu.CompilerParams(
            collective_id=0, has_side_effects=True, vmem_limit_bytes=VMEM_LIMIT),
        name="attend",
    )(seq_lens, cos_t, sin_t, norm_w.reshape(-1, 128), b_q.reshape(heads, head_dim), b_k[None], b_v[None], hidden,
      w_q, w_k, w_v, k_cache, v_cache, w_o)


def copy_kernel(parts, y_in, k_in, v_in, y_out, k_out, v_out, buf, kv_buf, in_sem, out_sem):
    rows = y_in.shape[0] // parts
    pairs = [(y_in.at[pl.ds(p * rows, rows)], buf.at[p], y_out.at[pl.ds(p * rows, rows)]) for p in range(parts)]
    pairs += [(k_in, kv_buf.at[0], k_out), (v_in, kv_buf.at[1], v_out)]
    loads = [pltpu.make_async_copy(a, m, in_sem.at[i]) for i, (a, m, _) in enumerate(pairs)]
    stores = [pltpu.make_async_copy(m, z, out_sem.at[i]) for i, (_, m, z) in enumerate(pairs)]
    for c in loads:
        c.start()
    for c, d in zip(loads, stores):
        c.wait()
        d.start()
    for d in stores:
        d.wait()


def copy_out(y, k, v):
    parts = 8
    hbm = pl.BlockSpec(memory_space=pl.ANY)
    dma = pltpu.SemaphoreType.DMA
    return pl.pallas_call(
        functools.partial(copy_kernel, parts),
        out_shape=[jax.ShapeDtypeStruct(a.shape, a.dtype) for a in (y, k, v)],
        in_specs=[hbm] * 3, out_specs=[hbm] * 3,
        scratch_shapes=[pltpu.VMEM((parts, y.shape[0] // parts, y.shape[1]), y.dtype),
                        pltpu.VMEM((2,) + k.shape, k.dtype), dma((parts + 2,)), dma((parts + 2,))],
        name="copy_out",
    )(y, k, v)


def solution(mesh):
    def device_step(hidden, norm_w, w_q, b_q, w_k, b_k, w_v, b_v, w_o, k_cache, v_cache, positions, seq_lens):
        n_rows = hidden.shape[0]
        s_dev, head_dim = k_cache.shape[1], k_cache.shape[3]
        cos_t, sin_t = rope_tables(positions, head_dim)
        outs = attention(seq_lens, cos_t, sin_t, norm_w, b_q, b_k, b_v, hidden, w_q, w_k, w_v,
                         k_cache.reshape(n_rows, s_dev, head_dim), v_cache.reshape(n_rows, s_dev, head_dim), w_o)
        y_out, kb, vb = copy_out(*outs)
        return y_out, kb.reshape(n_rows, 1, head_dim), vb.reshape(n_rows, 1, head_dim)

    col_spec = P(None, 'tp')
    vec_spec = P('tp')
    cache_spec = P('dp', 'sp', 'tp', None)
    group_spec = P('dp', 'tp', None)
    in_specs = (P('dp', None), P(None), col_spec, vec_spec, col_spec, vec_spec, col_spec, vec_spec,
                P('tp', None), cache_spec, cache_spec, P('dp'), P('dp'))
    out_specs = (P('dp', None), group_spec, group_spec)
    return jax.shard_map(device_step, mesh=mesh, in_specs=in_specs, out_specs=out_specs, check_vma=False)
```

```python
import functools

import jax
import jax.numpy as jnp
from jax import lax
from jax.experimental import pallas as pl
from jax.experimental.pallas import tpu as pltpu
from jax.sharding import PartitionSpec as P

RMS_EPS = 1.5625e-7
ROPE_BASE = 10000.0
LOG2E = 1.4426950408889634
NEG = -3e38
NEG_FLOOR = -1e38
MESH = pl.DeviceIdType.MESH
VMEM_LIMIT = 67_043_328


WO_FROM = 12
NORM_ROWS = 32
NC = 4
NH = 2
BR = 8
NBK, NBV = 4, 6
TN = 512
TS = 256
G_FINISH, G_PROJECT = 12, 13


def rope_tables(positions, head_dim):
    rot_dim = head_dim // 2
    lane = jnp.arange(head_dim, dtype=jnp.int32)
    freq = ROPE_BASE ** (-2.0 * (lane // 2).astype(jnp.float32) / rot_dim)
    freq = jnp.where(lane < rot_dim, freq, 0.0)
    angles = positions.astype(jnp.float32)[:, None] * freq
    sign = jnp.where(lane % 2 == 0, -1.0, 1.0)
    return jnp.cos(angles), jnp.sin(angles) * sign


def rope(x, cos_t, sin_t, even):
    width = x.shape[-1]
    swapped = jnp.where(even, pltpu.roll(x, width - 1, 1), pltpu.roll(x, 1, 1))
    return (x * cos_t + swapped * sin_t).astype(jnp.bfloat16).astype(jnp.float32)


def attn_kernel(seq_ref, cos_ref, sin_ref, nw_ref, bq_ref, bk_ref, bv_ref, hid_hbm, wq_hbm, wk_hbm, wv_hbm,
                k_hbm, v_hbm, wo_hbm, y_ref, kb_ref, vb_ref,
                q_ref, q_send, q_recv, wkv, bqf, kf_ref, vf_ref, in_sem, wkv_sem, q_s, q_r, o_buf, rd, rx, att, lhs, s_sc, p_sc, new_sc, p_buf, p_recv, y_send, y_core, y_chip, y_fwd, wo, hid,
                kbuf, vbuf, k_sem, v_sem, wo_sem, hid_sem, rd_s, rd_r, rx_s, rx_r, at_s, at_r, p_s, p_r,
                yc_s, yc_r, yx_s, yx_r, yf_s, yf_r):
    n_rows, d_model = y_ref.shape
    s_dev, head_dim = kbuf.shape[2], kbuf.shape[3]
    heads = q_ref.shape[0] // n_rows
    n_tiles = wo.shape[0]
    half = n_tiles * TN
    quarter = n_rows // (4 * NC)
    o_rows = quarter * heads
    chip_rows = n_rows // 2
    bq = quarter // BR
    n_blk = n_rows // BR
    coef = head_dim ** -0.5 * LOG2E

    dp, tp, sp = lax.axis_index("dp"), lax.axis_index("tp"), lax.axis_index("sp")
    chip, core = sp // 2, sp % 2
    to_core = (dp, tp, 2 * chip + (1 - core))
    to_chip = (dp, tp, 2 * (1 - chip) + core)
    to_tp = (dp, 1 - tp, sp)

    def remote(src, dst, s_sem, r_sem, dev):
        return pltpu.make_async_remote_copy(src_ref=src, dst_ref=dst, send_sem=s_sem, recv_sem=r_sem,
                                            device_id=dev, device_id_type=MESH)

    per_part = NC // NH
    part_rows = chip_rows // NH

    def group_piece(u):
        return (u // (4 * per_part)) * per_part + (u % (2 * per_part)) // 2

    def group_far(u):
        return u % (4 * per_part) < 2 * per_part

    def group_row(u):
        near = (u % (4 * per_part)) // (2 * per_part)
        own = u % 2
        on_chip = near * chip + (1 - near) * (1 - chip)
        on_core = own * core + (1 - own) * (1 - core)
        return on_chip * chip_rows + group_piece(u) * 2 * quarter + on_core * quarter

    def kept_group(n, near):
        return (n // per_part) * 4 * per_part + near * 2 * per_part + 2 * (n % per_part) + 1

    def block_row(b):
        return pl.multiple_of(group_row(b // bq) + (b % bq) * BR, BR)

    def k_copy(b):
        return pltpu.make_async_copy(k_hbm.at[pl.ds(block_row(b), BR)], kbuf.at[b % NBK], k_sem.at[b % NBK])

    def v_copy(b):
        return pltpu.make_async_copy(v_hbm.at[pl.ds(block_row(b), BR)], vbuf.at[b % NBV], v_sem.at[b % NBV])

    def wo_copy(t):
        cols = pl.ds(pl.multiple_of(core * half + t * TN, 128), TN)
        return pltpu.make_async_copy(wo_hbm.at[:, cols], wo.at[t], wo_sem.at[t])

    hid_copy = pltpu.make_async_copy(
        hid_hbm.at[pl.ds(pl.multiple_of(chip * chip_rows, 128), chip_rows),
                   pl.ds(pl.multiple_of(core * half, 128), half)], hid, hid_sem)

    n_q = q_send.shape[0]
    tile_heads = TN // head_dim
    k_half = wo.shape[1]

    def in_copy(i):
        rows = pl.ds(pl.multiple_of(i * NORM_ROWS, NORM_ROWS), NORM_ROWS)
        return pltpu.make_async_copy(hid_hbm.at[rows], y_ref.at[rows], in_sem.at[i])

    wk_copy = pltpu.make_async_copy(wk_hbm, wkv.at[:, :head_dim], wkv_sem.at[0])
    wv_copy = pltpu.make_async_copy(wv_hbm, wkv.at[:, head_dim:], wkv_sem.at[1])

    def wq_copy(i):
        cols = pl.ds(pl.multiple_of((core * n_q + i // 2) * TN, TN), TN)
        return pltpu.make_async_copy(wq_hbm.at[pl.ds((i % 2) * k_half, k_half), cols], wo.at[i], wo_sem.at[i])

    n_norm = n_rows // NORM_ROWS
    for i in range(n_norm):
        in_copy(i).start()

    barrier = pltpu.get_barrier_semaphore()
    for dev in (to_core, to_chip, to_tp):
        pl.semaphore_signal(barrier, inc=1, device_id=dev, device_id_type=MESH)

    bqf[...] = bq_ref[...].astype(jnp.float32)

    def norm_rows(i, _):
        rows = pl.ds(pl.multiple_of(i * NORM_ROWS, NORM_ROWS), NORM_ROWS)
        in_copy(i).wait()

        @pl.when(i < 2 * n_q)
        def _():
            wq_copy(i).start()

        @pl.when(i == n_norm - 1)
        def _():
            wk_copy.start()
            wv_copy.start()
        sq = jnp.zeros((NORM_ROWS, 128), jnp.float32)
        for c in range(d_model // 128):
            x = y_ref[rows, c * 128:(c + 1) * 128].astype(jnp.float32)
            sq = sq + x * x
        inv = lax.rsqrt(jnp.sum(sq, axis=-1, keepdims=True) / d_model + RMS_EPS)
        for c in range(d_model // 128):
            x = y_ref[rows, c * 128:(c + 1) * 128].astype(jnp.float32)
            x = x * inv * nw_ref[c:c + 1, :].astype(jnp.float32)
            y_ref[rows, c * 128:(c + 1) * 128] = x.astype(jnp.bfloat16)
        return 0
    lax.fori_loop(0, n_norm, norm_rows, 0)
    pl.semaphore_wait(barrier, 3)

    even = lax.broadcasted_iota(jnp.int32, (n_rows, head_dim), 1) % 2 == 0

    def round_f32(x):
        return x.astype(jnp.bfloat16).astype(jnp.float32)

    def q_copy(t):
        return remote(q_send.at[t], q_recv.at[t], q_s.at[t], q_r.at[t], to_core)

    def q_tile(t, _):
        wq_copy(2 * t).wait()
        wq_copy(2 * t + 1).wait()

        @pl.when(t == n_q - 1)
        def _():
            for b in range(NBV):
                if b < NBK:
                    k_copy(b).start()
                v_copy(b).start()
        acc = jnp.dot(y_ref[:, :k_half], wo[2 * t], preferred_element_type=jnp.float32)
        acc = acc + jnp.dot(y_ref[:, k_half:], wo[2 * t + 1], preferred_element_type=jnp.float32)
        for h in range(tile_heads):
            head = core * (heads // 2) + t * tile_heads + h
            val = round_f32(acc[:, h * head_dim:(h + 1) * head_dim] + bqf[pl.ds(head, 1), :])
            val = rope(val, cos_ref[...], sin_ref[...], even)
            q_ref[pl.ds(head, n_rows, stride=heads), :] = val
            q_send[t, pl.ds(h, n_rows, stride=tile_heads), :] = val
        q_copy(t).start()
        return 0
    lax.fori_loop(0, n_q, q_tile, 0)

    wk_copy.wait()
    wv_copy.wait()
    kv = jnp.dot(y_ref[...], wkv[...], preferred_element_type=jnp.float32)
    k_rot = rope(round_f32(kv[:, :head_dim] + bk_ref[...].astype(jnp.float32)), cos_ref[...], sin_ref[...], even)
    kf_ref[...] = k_rot
    kb_ref[...] = k_rot.astype(jnp.bfloat16)
    v_val = round_f32(kv[:, head_dim:] + bv_ref[...].astype(jnp.float32))
    vf_ref[...] = v_val
    vb_ref[...] = v_val.astype(jnp.bfloat16)

    def q_take(t, _):
        q_copy(t).wait_recv()
        for h in range(tile_heads):
            head = (1 - core) * (heads // 2) + t * tile_heads + h
            q_ref[pl.ds(head, n_rows, stride=heads), :] = q_recv[t, pl.ds(h, n_rows, stride=tile_heads), :]
        return 0
    lax.fori_loop(0, n_q, q_take, 0)

    lane = lax.broadcasted_iota(jnp.int32, (heads, head_dim), 1)
    pos = lax.broadcasted_iota(jnp.int32, (heads, s_dev), 1) + sp * s_dev
    zeros_q = jnp.zeros((heads, head_dim), jnp.float32)

    def q_rows(row):
        return q_ref[pl.ds(pl.multiple_of(row * heads, 8), heads), :]

    def new_scores(n):
        row0 = chip * chip_rows + n * 2 * quarter + core * quarter

        def rows8(g, acc):
            base = pl.multiple_of(row0 + g * 8, 8)
            k_new = kf_ref[pl.ds(base, 8), :]
            for r in range(8):
                s_new = jnp.sum(q_rows(base + r) * k_new[r:r + 1], axis=-1, keepdims=True)
                acc = jnp.where(lane == g * 8 + r, s_new, acc)
            return acc
        new_sc[n] = lax.fori_loop(0, quarter // 8, rows8, zeros_q)

    def column(vals, j):
        return jnp.broadcast_to(vals[:, j:j + 1], (heads, head_dim))

    def d2d(k):
        return remote(o_buf.at[2 * k], rd.at[k], rd_s.at[k], rd_r.at[k], to_core)

    def xsend(n):
        return remote(o_buf.at[kept_group(n, 0)], rx.at[n], rx_s.at[n], rx_r.at[n], to_chip)

    def at_copy(n):
        return remote(att.at[n * 2 + core], att.at[n * 2 + core], at_s.at[n], at_r.at[n], to_core)

    def merge_core(u):
        k = u // 2
        st1 = o_buf[u, o_rows:o_rows + heads, :]
        st2 = rd[k, o_rows:o_rows + heads, :]
        m = jnp.maximum(st1, st2)
        f1 = jnp.exp2((st1 - m) * coef)
        f2 = jnp.exp2((st2 - m) * coef)
        l = st1 * pltpu.roll(f1, quarter, 1) + st2 * pltpu.roll(f2, quarter, 1)
        o_buf[u, o_rows:o_rows + heads, :] = jnp.where(lane < quarter, m, l)

        for j in range(quarter):
            rows = pl.ds(j * heads, heads)
            o_buf[u, rows, :] = o_buf[u, rows, :] * column(f1, j) + rd[k, rows, :] * column(f2, j)

    def finish(n):
        u = kept_group(n, 1)
        row0 = chip * chip_rows + n * 2 * quarter + core * quarter
        st1 = o_buf[u, o_rows:o_rows + heads, :]
        st2 = rx[n, o_rows:o_rows + heads, :]
        m3 = new_sc[n]
        m = jnp.maximum(jnp.maximum(st1, st2), m3)
        f1 = jnp.exp2((st1 - m) * coef)
        f2 = jnp.exp2((st2 - m) * coef)
        f3 = jnp.exp2((m3 - m) * coef)
        l = st1 * pltpu.roll(f1, quarter, 1) + st2 * pltpu.roll(f2, quarter, 1) + pltpu.roll(f3, quarter, 1)
        l = pltpu.roll(l, head_dim - quarter, 1)
        f1, f2, f3 = f1 / l, f2 / l, f3 / l

        for j in range(quarter):
            if j % 8 == 0:
                v_new = vf_ref[pl.ds(pl.multiple_of(row0 + j, 8), 8), :]
            rows = pl.ds(j * heads, heads)
            o = o_buf[u, rows, :] * column(f1, j) + rx[n, rows, :] * column(f2, j)
            o = o + column(f3, j) * v_new[j % 8:j % 8 + 1]
            att[n * 2 + core, rows, :] = round_f32(o)

    def block(b, new, old):
        @pl.when(b < n_blk)
        def _():
            k_copy(b).wait()

        b1 = jnp.minimum(b, n_blk - 1)
        b2 = jnp.clip(b - 1, 0, n_blk - 1)
        b3 = jnp.clip(b - 2, 0, n_blk - 1)

        @pl.when(jnp.logical_or(b == 0, b >= 3))
        def _():
            v_copy(b3).wait()

        u2, row2 = b2 // bq, block_row(b2)
        stats = o_buf[u2, o_rows:o_rows + heads, :]
        for pair in range(BR // 2):
            p_list = []
            for i in range(2):
                r = 2 * pair + i
                s = s_sc[old, pair, i * heads:(i + 1) * heads, :]
                s = jnp.where(pos < seq_ref[row2 + r], s, NEG)
                m = jnp.maximum(jnp.max(s, axis=-1, keepdims=True), NEG_FLOOR)
                p = jnp.exp2((s - m) * coef)
                l = jnp.sum(p, axis=-1, keepdims=True)
                j = (b2 % bq) * BR + r
                stats = jnp.where(lane == j, m, jnp.where(lane == quarter + j, l, stats))
                p_list.append(p)
            p_sc[new, pair] = jnp.concatenate(p_list, axis=0).astype(jnp.bfloat16)
        o_buf[u2, o_rows:o_rows + heads, :] = stats
        row1, kslot = block_row(b1), b1 % NBK
        for pair in range(BR // 2):
            r = 2 * pair
            left = jnp.concatenate([q_rows(row1 + r), zeros_q], axis=0)
            right = jnp.concatenate([zeros_q, q_rows(row1 + r + 1)], axis=0)
            q_pair = jnp.concatenate([left, right], axis=1).astype(jnp.bfloat16)
            k_pair = jnp.concatenate([kbuf[kslot, r], kbuf[kslot, r + 1]], axis=1)
            s_sc[new, pair] = lax.dot_general(q_pair, k_pair, (((1,), (1,)), ((), ())),
                                         preferred_element_type=jnp.float32)
        u3, vslot = b3 // bq, b3 % NBV
        for pair in range(BR // 2):
            r = 2 * pair
            v_pair = jnp.concatenate([vbuf[vslot, r], vbuf[vslot, r + 1]], axis=1)
            o_pair = jnp.dot(p_sc[old, pair], v_pair, preferred_element_type=jnp.float32)
            for i in range(2):
                o = o_pair[i * heads:(i + 1) * heads, i * head_dim:(i + 1) * head_dim]
                o_buf[u3, pl.ds(pl.multiple_of(((b3 % bq) * BR + r + i) * heads, 8), heads), :] = o

        @pl.when(b + NBK < n_blk)
        def _():
            k_copy(b + NBK).start()

        @pl.when(jnp.logical_and(b >= 2, b - 2 + NBV < n_blk))
        def _():
            v_copy(b - 2 + NBV).start()

        w = b - WO_FROM

        @pl.when(jnp.logical_and(w >= 0, jnp.logical_and(w % 2 == 0, w < 2 * n_tiles)))
        def _():
            wo_copy(w // 2).start()

        @pl.when(w == 0)
        def _():
            hid_copy.start()

        done = jnp.logical_and(b >= 2, (b - 2) % bq == bq - 1)
        u = b3 // bq

        @pl.when(jnp.logical_and(done, u % 2 == 0))
        def _():
            d2d(u // 2).start()

        @pl.when(jnp.logical_and(done, u % 2 == 1))
        def _():
            d2d(u // 2).wait_recv()
            merge_core(u)

            @pl.when(group_far(u))
            def _():
                xsend(group_piece(u)).start()

    def two_blocks(g, _):
        block(2 * g, 0, 1)
        block(2 * g + 1, 1, 0)
        return 0

    def p_copy(i):
        return remote(p_buf.at[i], p_recv.at[i], p_s.at[i], p_r.at[i], to_tp)

    def yc_copy(i):
        return remote(y_send.at[i], y_core.at[i], yc_s.at[i], yc_r.at[i], to_core)

    def yx_copy(i):
        return remote(y_send.at[i], y_chip.at[i], yx_s.at[i], yx_r.at[i], to_chip)

    def yf_copy(i):
        return remote(y_chip.at[i], y_fwd.at[i], yf_s.at[i], yf_r.at[i], to_core)

    per = TN // TS
    n_sub = n_tiles * per

    def finish_part(h):
        for k in range(per_part):
            n = h * per_part + k
            xsend(n).wait_recv()
            finish(n)
            at_copy(n).start()

    def project_part(h):
        for k in range(per_part):
            n = h * per_part + k
            at_copy(n).wait_recv()
            for hd in range(heads):
                cols = [att[n * 2 + c, pl.ds(hd, quarter, stride=heads), :] for c in range(2)]
                lhs[k * 2 * quarter:(k + 1) * 2 * quarter, hd * head_dim:(hd + 1) * head_dim] = (
                    jnp.concatenate(cols, axis=0).astype(jnp.bfloat16))

        def tile(t, _):
            if h == 0:
                wo_copy(t).wait()
            res = jnp.dot(lhs[...], wo[t], preferred_element_type=jnp.float32)
            for k in range(per):
                i = h * n_sub + t * per + k
                p_buf[i] = res[:, k * TS:(k + 1) * TS]
                p_copy(i).start()
            if h == 1:
                @pl.when(t % 2 == 1)
                def _():
                    y_tile(early + t // 2)
            return 0
        lax.fori_loop(0, n_tiles, tile, 0)

    def out_cols(i, on_core):
        return pl.ds(pl.multiple_of(on_core * half + (i % n_sub) * TS, TS), TS)

    def out_rows(i, on_chip):
        return pl.ds(pl.multiple_of(on_chip * chip_rows + (i // n_sub) * part_rows, part_rows), part_rows)

    def y_tile(i):
        p_copy(i).wait_recv()
        res = hid[pl.ds(pl.multiple_of((i // n_sub) * part_rows, part_rows), part_rows),
                  pl.ds(pl.multiple_of((i % n_sub) * TS, TS), TS)].astype(jnp.float32)
        y = (res + (p_buf[i] + p_recv[i])).astype(jnp.bfloat16)
        y_send[i] = y.astype(jnp.float32)
        y_ref[out_rows(i, chip), out_cols(i, core)] = y
        yx_copy(i).start()
        yc_copy(i).start()

    def y_from_chip(i):
        yx_copy(i).wait_recv()
        yf_copy(i).start()
        y_ref[out_rows(i, 1 - chip), out_cols(i, core)] = y_chip[i].astype(jnp.bfloat16)
        yc_copy(i).wait_recv()
        y_ref[out_rows(i, chip), out_cols(i, 1 - core)] = y_core[i].astype(jnp.bfloat16)

    def y_from_fwd(i):
        yf_copy(i).wait_recv()
        y_ref[out_rows(i, 1 - chip), out_cols(i, 1 - core)] = y_fwd[i].astype(jnp.bfloat16)

    total = NH * n_sub
    last = (n_blk + 2) // 2
    lax.fori_loop(0, G_FINISH, two_blocks, 0)
    for n in range(NC):
        new_scores(n)
    finish_part(0)
    lax.fori_loop(G_FINISH, G_PROJECT, two_blocks, 0)
    early = last - G_PROJECT + 2
    project_part(0)
    hid_copy.wait()

    def two_blocks_and_tile(g, _):
        two_blocks(g, 0)
        y_tile(g - G_PROJECT)
        return 0
    lax.fori_loop(G_PROJECT, last, two_blocks_and_tile, 0)
    finish_part(1)
    y_tile(early - 2)
    y_tile(early - 1)
    project_part(1)
    early = early + n_tiles // 2

    def step(s, _):
        @pl.when(s + early < total)
        def _():
            y_tile(s + early)

        @pl.when(s < total)
        def _():
            y_from_chip(s)

        @pl.when(s >= 1)
        def _():
            y_from_fwd(s - 1)
        return 0
    lax.fori_loop(0, total + 1, step, 0)

    for t in range(n_q):
        q_copy(t).wait_send()
    for k in range(2 * NC):
        d2d(k).wait_send()
    for n in range(NC):
        xsend(n).wait_send()
        at_copy(n).wait_send()

    def drain(i, _):
        p_copy(i).wait_send()
        yc_copy(i).wait_send()
        yx_copy(i).wait_send()
        yf_copy(i).wait_send()
        return 0
    lax.fori_loop(0, total, drain, 0)


def attention(seq_lens, cos_t, sin_t, norm_w, b_q, b_k, b_v, hidden, w_q, w_k, w_v, k_cache, v_cache, w_o):
    n_rows, d_model = hidden.shape
    s_dev, head_dim = k_cache.shape[1], k_cache.shape[2]
    heads = w_q.shape[1] // head_dim
    half = d_model // 2
    n_tiles = half // TN
    n_q = w_q.shape[1] // (2 * TN)
    quarter = n_rows // (4 * NC)
    msg = quarter * heads + heads
    total = NH * n_tiles * (TN // TS)
    vmem = pl.BlockSpec(memory_space=pltpu.VMEM)
    hbm = pl.BlockSpec(memory_space=pl.ANY)
    f32, bf16 = jnp.float32, jnp.bfloat16
    dma = pltpu.SemaphoreType.DMA
    tile_f32 = pltpu.VMEM((total, n_rows // (2 * NH), TS), f32)
    return pl.pallas_call(
        attn_kernel,
        out_shape=[jax.ShapeDtypeStruct((n_rows, d_model), bf16)] + [jax.ShapeDtypeStruct((n_rows, head_dim), bf16)] * 2,
        in_specs=[pl.BlockSpec(memory_space=pltpu.SMEM)] + [vmem] * 6 + [hbm] * 7,
        out_specs=[vmem] * 3,
        scratch_shapes=[
            pltpu.VMEM((n_rows * heads, head_dim), f32),
            pltpu.VMEM((n_q, n_rows * TN // head_dim, head_dim), f32),
            pltpu.VMEM((n_q, n_rows * TN // head_dim, head_dim), f32),
            pltpu.VMEM((d_model, 2 * head_dim), bf16),
            pltpu.VMEM((heads, head_dim), f32),
            pltpu.VMEM((n_rows, head_dim), f32), pltpu.VMEM((n_rows, head_dim), f32),
            dma((n_rows // NORM_ROWS,)), dma((2,)), dma((n_q,)), dma((n_q,)),
            pltpu.VMEM((NC * 4, msg, head_dim), f32),
            pltpu.VMEM((NC * 2, msg, head_dim), f32),
            pltpu.VMEM((NC, msg, head_dim), f32),
            pltpu.VMEM((NC * 2, quarter * heads, head_dim), f32),
            pltpu.VMEM((n_rows // (2 * NH), heads * head_dim), bf16),
            pltpu.VMEM((2, BR // 2, 2 * heads, s_dev), f32),
            pltpu.VMEM((2, BR // 2, 2 * heads, s_dev), bf16),
            pltpu.VMEM((NC, heads, head_dim), f32),
            tile_f32, tile_f32, tile_f32, tile_f32, tile_f32, tile_f32,
            pltpu.VMEM((n_tiles, heads * head_dim, TN), bf16),
            pltpu.VMEM((n_rows // 2, half), bf16),
            pltpu.VMEM((NBK, BR, s_dev, head_dim), bf16),
            pltpu.VMEM((NBV, BR, s_dev, head_dim), bf16),
            dma((NBK,)), dma((NBV,)), dma((n_tiles,)), dma,
            dma((NC * 2,)), dma((NC * 2,)), dma((NC,)), dma((NC,)), dma((NC,)), dma((NC,)),
            dma((total,)), dma((total,)), dma((total,)), dma((total,)), dma((total,)), dma((total,)),
            dma((total,)), dma((total,)),
        ],
        compiler_params=pltpu.CompilerParams(
            collective_id=0, has_side_effects=True, vmem_limit_bytes=VMEM_LIMIT),
        name="attend",
    )(seq_lens, cos_t, sin_t, norm_w.reshape(-1, 128), b_q.reshape(heads, head_dim), b_k[None], b_v[None], hidden,
      w_q, w_k, w_v, k_cache, v_cache, w_o)


def copy_kernel(parts, y_in, k_in, v_in, y_out, k_out, v_out, buf, kv_buf, in_sem, out_sem):
    rows = y_in.shape[0] // parts
    pairs = [(y_in.at[pl.ds(p * rows, rows)], buf.at[p], y_out.at[pl.ds(p * rows, rows)]) for p in range(parts)]
    pairs += [(k_in, kv_buf.at[0], k_out), (v_in, kv_buf.at[1], v_out)]
    loads = [pltpu.make_async_copy(a, m, in_sem.at[i]) for i, (a, m, _) in enumerate(pairs)]
    stores = [pltpu.make_async_copy(m, z, out_sem.at[i]) for i, (_, m, z) in enumerate(pairs)]
    for c in loads:
        c.start()
    for c, d in zip(loads, stores):
        c.wait()
        d.start()
    for d in stores:
        d.wait()


def copy_out(y, k, v):
    parts = 8
    hbm = pl.BlockSpec(memory_space=pl.ANY)
    dma = pltpu.SemaphoreType.DMA
    return pl.pallas_call(
        functools.partial(copy_kernel, parts),
        out_shape=[jax.ShapeDtypeStruct(a.shape, a.dtype) for a in (y, k, v)],
        in_specs=[hbm] * 3, out_specs=[hbm] * 3,
        scratch_shapes=[pltpu.VMEM((parts, y.shape[0] // parts, y.shape[1]), y.dtype),
                        pltpu.VMEM((2,) + k.shape, k.dtype), dma((parts + 2,)), dma((parts + 2,))],
        name="copy_out",
    )(y, k, v)


def solution(mesh):
    def device_step(hidden, norm_w, w_q, b_q, w_k, b_k, w_v, b_v, w_o, k_cache, v_cache, positions, seq_lens):
        n_rows = hidden.shape[0]
        s_dev, head_dim = k_cache.shape[1], k_cache.shape[3]
        cos_t, sin_t = rope_tables(positions, head_dim)
        outs = attention(seq_lens, cos_t, sin_t, norm_w, b_q, b_k, b_v, hidden, w_q, w_k, w_v,
                         k_cache.reshape(n_rows, s_dev, head_dim), v_cache.reshape(n_rows, s_dev, head_dim), w_o)
        y_out, kb, vb = copy_out(*outs)
        return y_out, kb.reshape(n_rows, 1, head_dim), vb.reshape(n_rows, 1, head_dim)

    col_spec = P(None, 'tp')
    vec_spec = P('tp')
    cache_spec = P('dp', 'sp', 'tp', None)
    group_spec = P('dp', 'tp', None)
    in_specs = (P('dp', None), P(None), col_spec, vec_spec, col_spec, vec_spec, col_spec, vec_spec,
                P('tp', None), cache_spec, cache_spec, P('dp'), P('dp'))
    out_specs = (P('dp', None), group_spec, group_spec)
    return jax.shard_map(device_step, mesh=mesh, in_specs=in_specs, out_specs=out_specs, check_vma=False)
```

```python
import functools

import jax
import jax.numpy as jnp
from jax import lax
from jax.experimental import pallas as pl
from jax.experimental.pallas import tpu as pltpu
from jax.sharding import PartitionSpec as P

RMS_EPS = 1.5625e-7
ROPE_BASE = 10000.0
LOG2E = 1.4426950408889634
NEG = -3e38
NEG_FLOOR = -1e38
MESH = pl.DeviceIdType.MESH
VMEM_LIMIT = 67_043_328


WO_FROM = 12
NORM_ROWS = 32
NC = 4
NH = 2
BR = 8
NBK, NBV = 6, 7
TN = 512
TS = 256
G_FINISH, G_PROJECT = 12, 13


def rope_tables(positions, head_dim):
    rot_dim = head_dim // 2
    lane = jnp.arange(head_dim, dtype=jnp.int32)
    freq = ROPE_BASE ** (-2.0 * (lane // 2).astype(jnp.float32) / rot_dim)
    freq = jnp.where(lane < rot_dim, freq, 0.0)
    angles = positions.astype(jnp.float32)[:, None] * freq
    sign = jnp.where(lane % 2 == 0, -1.0, 1.0)
    return jnp.cos(angles), jnp.sin(angles) * sign


def rope(x, cos_t, sin_t, even):
    width = x.shape[-1]
    swapped = jnp.where(even, pltpu.roll(x, width - 1, 1), pltpu.roll(x, 1, 1))
    return (x * cos_t + swapped * sin_t).astype(jnp.bfloat16).astype(jnp.float32)


def attn_kernel(seq_ref, cos_ref, sin_ref, nw_ref, bq_ref, bk_ref, bv_ref, hid_hbm, wq_hbm, wk_hbm, wv_hbm,
                k_hbm, v_hbm, wo_hbm, y_ref, kb_ref, vb_ref,
                q_ref, q_send, q_recv, bqf, kf_ref, vf_ref, in_sem, wkv_sem, q_s, q_r, o_buf, rd, rx, att, lhs, s_sc, p_sc, new_sc, p_buf, p_recv, y_send, y_core, y_chip, y_fwd, wo, hid,
                kbuf, vbuf, k_sem, v_sem, wo_sem, hid_sem, rd_s, rd_r, rx_s, rx_r, at_s, at_r, p_s, p_r,
                yc_s, yc_r, yx_s, yx_r, yf_s, yf_r):
    n_rows, d_model = y_ref.shape
    s_dev, head_dim = kbuf.shape[2], kbuf.shape[3]
    heads = q_ref.shape[0] // n_rows
    n_tiles = wo.shape[0]
    half = n_tiles * TN
    quarter = n_rows // (4 * NC)
    o_rows = quarter * heads
    chip_rows = n_rows // 2
    bq = quarter // BR
    n_blk = n_rows // BR
    coef = head_dim ** -0.5 * LOG2E

    dp, tp, sp = lax.axis_index("dp"), lax.axis_index("tp"), lax.axis_index("sp")
    chip, core = sp // 2, sp % 2
    to_core = (dp, tp, 2 * chip + (1 - core))
    to_chip = (dp, tp, 2 * (1 - chip) + core)
    to_tp = (dp, 1 - tp, sp)

    def remote(src, dst, s_sem, r_sem, dev):
        return pltpu.make_async_remote_copy(src_ref=src, dst_ref=dst, send_sem=s_sem, recv_sem=r_sem,
                                            device_id=dev, device_id_type=MESH)

    per_part = NC // NH
    part_rows = chip_rows // NH

    def group_piece(u):
        return (u // (4 * per_part)) * per_part + (u % (2 * per_part)) // 2

    def group_far(u):
        return u % (4 * per_part) < 2 * per_part

    def group_row(u):
        near = (u % (4 * per_part)) // (2 * per_part)
        own = u % 2
        on_chip = near * chip + (1 - near) * (1 - chip)
        on_core = own * core + (1 - own) * (1 - core)
        return on_chip * chip_rows + group_piece(u) * 2 * quarter + on_core * quarter

    def kept_group(n, near):
        return (n // per_part) * 4 * per_part + near * 2 * per_part + 2 * (n % per_part) + 1

    def block_row(b):
        return pl.multiple_of(group_row(b // bq) + (b % bq) * BR, BR)

    def k_copy(b):
        return pltpu.make_async_copy(k_hbm.at[pl.ds(block_row(b), BR)], kbuf.at[b % NBK], k_sem.at[b % NBK])

    def v_copy(b):
        return pltpu.make_async_copy(v_hbm.at[pl.ds(block_row(b), BR)], vbuf.at[b % NBV], v_sem.at[b % NBV])

    def wo_copy(t):
        cols = pl.ds(pl.multiple_of(core * half + t * TN, 128), TN)
        return pltpu.make_async_copy(wo_hbm.at[:, cols], wo.at[t], wo_sem.at[t])

    hid_copy = pltpu.make_async_copy(
        hid_hbm.at[pl.ds(pl.multiple_of(chip * chip_rows, 128), chip_rows),
                   pl.ds(pl.multiple_of(core * half, 128), half)], hid, hid_sem)

    n_q = q_send.shape[0]
    tile_heads = TN // head_dim
    k_half = wo.shape[1]

    def in_copy(i):
        rows = pl.ds(pl.multiple_of(i * NORM_ROWS, NORM_ROWS), NORM_ROWS)
        return pltpu.make_async_copy(hid_hbm.at[rows], y_ref.at[rows], in_sem.at[i])


    def wkv_copies():
        parts = [(w, r) for r in range(2) for w in (wk_hbm, wv_hbm)]
        return [pltpu.make_async_copy(w.at[pl.ds(r * k_half, k_half)],
                                      wo.at[0, :, i * head_dim:(i + 1) * head_dim], wkv_sem.at[i])
                for i, (w, r) in enumerate(parts)]

    def wq_copy(i):
        cols = pl.ds(pl.multiple_of((core * n_q + i // 2) * TN, TN), TN)
        return pltpu.make_async_copy(wq_hbm.at[pl.ds((i % 2) * k_half, k_half), cols], wo.at[i], wo_sem.at[i])

    n_norm = n_rows // NORM_ROWS
    for i in range(n_norm):
        in_copy(i).start()

    barrier = pltpu.get_barrier_semaphore()
    for dev in (to_core, to_chip, to_tp):
        pl.semaphore_signal(barrier, inc=1, device_id=dev, device_id_type=MESH)

    bqf[...] = bq_ref[...].astype(jnp.float32)

    def norm_rows(i, _):
        rows = pl.ds(pl.multiple_of(i * NORM_ROWS, NORM_ROWS), NORM_ROWS)
        in_copy(i).wait()

        @pl.when(i < 2 * n_q)
        def _():
            wq_copy(i).start()
        sq = jnp.zeros((NORM_ROWS, 128), jnp.float32)
        for c in range(d_model // 128):
            x = y_ref[rows, c * 128:(c + 1) * 128].astype(jnp.float32)
            sq = sq + x * x
        inv = lax.rsqrt(jnp.sum(sq, axis=-1, keepdims=True) / d_model + RMS_EPS)
        for c in range(d_model // 128):
            x = y_ref[rows, c * 128:(c + 1) * 128].astype(jnp.float32)
            x = x * inv * nw_ref[c:c + 1, :].astype(jnp.float32)
            y_ref[rows, c * 128:(c + 1) * 128] = x.astype(jnp.bfloat16)
        return 0
    lax.fori_loop(0, n_norm, norm_rows, 0)
    pl.semaphore_wait(barrier, 3)

    even = lax.broadcasted_iota(jnp.int32, (n_rows, head_dim), 1) % 2 == 0

    def round_f32(x):
        return x.astype(jnp.bfloat16).astype(jnp.float32)

    def q_copy(t):
        return remote(q_send.at[t], q_recv.at[t], q_s.at[t], q_r.at[t], to_core)

    def q_tile(t, _):
        wq_copy(2 * t).wait()
        wq_copy(2 * t + 1).wait()

        @pl.when(t == n_q - 1)
        def _():
            for b in range(NBV):
                if b < NBK:
                    k_copy(b).start()
                v_copy(b).start()
        acc = jnp.dot(y_ref[:, :k_half], wo[2 * t], preferred_element_type=jnp.float32)
        acc = acc + jnp.dot(y_ref[:, k_half:], wo[2 * t + 1], preferred_element_type=jnp.float32)
        for h in range(tile_heads):
            head = core * (heads // 2) + t * tile_heads + h
            val = round_f32(acc[:, h * head_dim:(h + 1) * head_dim] + bqf[pl.ds(head, 1), :])
            val = rope(val, cos_ref[...], sin_ref[...], even)
            q_ref[pl.ds(head, n_rows, stride=heads), :] = val
            q_send[t, pl.ds(h, n_rows, stride=tile_heads), :] = val
        q_copy(t).start()

        @pl.when(t == 0)
        def _():
            for c in wkv_copies():
                c.start()
        return 0
    lax.fori_loop(0, n_q, q_tile, 0)

    for c in wkv_copies():
        c.wait()
    kv = jnp.dot(y_ref[:, :k_half], wo[0, :, :2 * head_dim], preferred_element_type=jnp.float32)
    kv = kv + jnp.dot(y_ref[:, k_half:], wo[0, :, 2 * head_dim:], preferred_element_type=jnp.float32)
    k_rot = rope(round_f32(kv[:, :head_dim] + bk_ref[...].astype(jnp.float32)), cos_ref[...], sin_ref[...], even)
    kf_ref[...] = k_rot
    kb_ref[...] = k_rot.astype(jnp.bfloat16)
    v_val = round_f32(kv[:, head_dim:] + bv_ref[...].astype(jnp.float32))
    vf_ref[...] = v_val
    vb_ref[...] = v_val.astype(jnp.bfloat16)

    def q_take(t, _):
        q_copy(t).wait_recv()
        for h in range(tile_heads):
            head = (1 - core) * (heads // 2) + t * tile_heads + h
            q_ref[pl.ds(head, n_rows, stride=heads), :] = q_recv[t, pl.ds(h, n_rows, stride=tile_heads), :]
        return 0
    lax.fori_loop(0, n_q, q_take, 0)

    lane = lax.broadcasted_iota(jnp.int32, (heads, head_dim), 1)
    pos = lax.broadcasted_iota(jnp.int32, (heads, s_dev), 1) + sp * s_dev
    zeros_q = jnp.zeros((heads, head_dim), jnp.float32)

    def q_rows(row):
        return q_ref[pl.ds(pl.multiple_of(row * heads, 8), heads), :]

    def new_scores(n):
        row0 = chip * chip_rows + n * 2 * quarter + core * quarter

        def rows8(g, acc):
            base = pl.multiple_of(row0 + g * 8, 8)
            k_new = kf_ref[pl.ds(base, 8), :]
            for r in range(8):
                s_new = jnp.sum(q_rows(base + r) * k_new[r:r + 1], axis=-1, keepdims=True)
                acc = jnp.where(lane == g * 8 + r, s_new, acc)
            return acc
        new_sc[n] = lax.fori_loop(0, quarter // 8, rows8, zeros_q)

    def column(vals, j):
        return jnp.broadcast_to(vals[:, j:j + 1], (heads, head_dim))

    def d2d(k):
        return remote(o_buf.at[2 * k], rd.at[k], rd_s.at[k], rd_r.at[k], to_core)

    def xsend(n):
        return remote(o_buf.at[kept_group(n, 0)], rx.at[n], rx_s.at[n], rx_r.at[n], to_chip)

    def at_copy(n):
        return remote(att.at[n * 2 + core], att.at[n * 2 + core], at_s.at[n], at_r.at[n], to_core)

    def merge_core(u):
        k = u // 2
        st1 = o_buf[u, o_rows:o_rows + heads, :]
        st2 = rd[k, o_rows:o_rows + heads, :]
        m = jnp.maximum(st1, st2)
        f1 = jnp.exp2((st1 - m) * coef)
        f2 = jnp.exp2((st2 - m) * coef)
        l = st1 * pltpu.roll(f1, quarter, 1) + st2 * pltpu.roll(f2, quarter, 1)
        o_buf[u, o_rows:o_rows + heads, :] = jnp.where(lane < quarter, m, l)

        for j in range(quarter):
            rows = pl.ds(j * heads, heads)
            o_buf[u, rows, :] = o_buf[u, rows, :] * column(f1, j) + rd[k, rows, :] * column(f2, j)

    def finish(n):
        u = kept_group(n, 1)
        row0 = chip * chip_rows + n * 2 * quarter + core * quarter
        st1 = o_buf[u, o_rows:o_rows + heads, :]
        st2 = rx[n, o_rows:o_rows + heads, :]
        m3 = new_sc[n]
        m = jnp.maximum(jnp.maximum(st1, st2), m3)
        f1 = jnp.exp2((st1 - m) * coef)
        f2 = jnp.exp2((st2 - m) * coef)
        f3 = jnp.exp2((m3 - m) * coef)
        l = st1 * pltpu.roll(f1, quarter, 1) + st2 * pltpu.roll(f2, quarter, 1) + pltpu.roll(f3, quarter, 1)
        l = pltpu.roll(l, head_dim - quarter, 1)
        f1, f2, f3 = f1 / l, f2 / l, f3 / l

        for j in range(quarter):
            if j % 8 == 0:
                v_new = vf_ref[pl.ds(pl.multiple_of(row0 + j, 8), 8), :]
            rows = pl.ds(j * heads, heads)
            o = o_buf[u, rows, :] * column(f1, j) + rx[n, rows, :] * column(f2, j)
            o = o + column(f3, j) * v_new[j % 8:j % 8 + 1]
            att[n * 2 + core, rows, :] = round_f32(o)

    def block(b, new, old):
        @pl.when(b < n_blk)
        def _():
            k_copy(b).wait()

        b1 = jnp.minimum(b, n_blk - 1)
        b2 = jnp.clip(b - 1, 0, n_blk - 1)
        b3 = jnp.clip(b - 2, 0, n_blk - 1)

        @pl.when(jnp.logical_or(b == 0, b >= 3))
        def _():
            v_copy(b3).wait()

        u2, row2 = b2 // bq, block_row(b2)
        stats = o_buf[u2, o_rows:o_rows + heads, :]
        for pair in range(BR // 2):
            p_list = []
            for i in range(2):
                r = 2 * pair + i
                s = s_sc[old, pair, i * heads:(i + 1) * heads, :]
                s = jnp.where(pos < seq_ref[row2 + r], s, NEG)
                m = jnp.maximum(jnp.max(s, axis=-1, keepdims=True), NEG_FLOOR)
                p = jnp.exp2((s - m) * coef)
                l = jnp.sum(p, axis=-1, keepdims=True)
                j = (b2 % bq) * BR + r
                stats = jnp.where(lane == j, m, jnp.where(lane == quarter + j, l, stats))
                p_list.append(p)
            p_sc[new, pair] = jnp.concatenate(p_list, axis=0).astype(jnp.bfloat16)
        o_buf[u2, o_rows:o_rows + heads, :] = stats
        row1, kslot = block_row(b1), b1 % NBK
        for pair in range(BR // 2):
            r = 2 * pair
            left = jnp.concatenate([q_rows(row1 + r), zeros_q], axis=0)
            right = jnp.concatenate([zeros_q, q_rows(row1 + r + 1)], axis=0)
            q_pair = jnp.concatenate([left, right], axis=1).astype(jnp.bfloat16)
            k_pair = jnp.concatenate([kbuf[kslot, r], kbuf[kslot, r + 1]], axis=1)
            s_sc[new, pair] = lax.dot_general(q_pair, k_pair, (((1,), (1,)), ((), ())),
                                         preferred_element_type=jnp.float32)
        u3, vslot = b3 // bq, b3 % NBV
        for pair in range(BR // 2):
            r = 2 * pair
            v_pair = jnp.concatenate([vbuf[vslot, r], vbuf[vslot, r + 1]], axis=1)
            o_pair = jnp.dot(p_sc[old, pair], v_pair, preferred_element_type=jnp.float32)
            for i in range(2):
                o = o_pair[i * heads:(i + 1) * heads, i * head_dim:(i + 1) * head_dim]
                o_buf[u3, pl.ds(pl.multiple_of(((b3 % bq) * BR + r + i) * heads, 8), heads), :] = o

        @pl.when(b + NBK < n_blk)
        def _():
            k_copy(b + NBK).start()

        @pl.when(jnp.logical_and(b >= 2, b - 2 + NBV < n_blk))
        def _():
            v_copy(b - 2 + NBV).start()

        w = b - WO_FROM

        @pl.when(jnp.logical_and(w >= 0, jnp.logical_and(w % 2 == 0, w < 2 * n_tiles)))
        def _():
            wo_copy(w // 2).start()

        @pl.when(w == 0)
        def _():
            hid_copy.start()

        done = jnp.logical_and(b >= 2, (b - 2) % bq == bq - 1)
        u = b3 // bq

        @pl.when(jnp.logical_and(done, u % 2 == 0))
        def _():
            d2d(u // 2).start()

        @pl.when(jnp.logical_and(done, u % 2 == 1))
        def _():
            d2d(u // 2).wait_recv()
            merge_core(u)

            @pl.when(group_far(u))
            def _():
                xsend(group_piece(u)).start()

    def two_blocks(g, _):
        block(2 * g, 0, 1)
        block(2 * g + 1, 1, 0)
        return 0

    def p_copy(i):
        return remote(p_buf.at[i], p_recv.at[i], p_s.at[i], p_r.at[i], to_tp)

    def yc_copy(i):
        return remote(y_send.at[i], y_core.at[i], yc_s.at[i], yc_r.at[i], to_core)

    def yx_copy(i):
        return remote(y_send.at[i], y_chip.at[i], yx_s.at[i], yx_r.at[i], to_chip)

    def yf_copy(i):
        return remote(y_chip.at[i], y_fwd.at[i], yf_s.at[i], yf_r.at[i], to_core)

    per = TN // TS
    n_sub = n_tiles * per

    def finish_part(h):
        for k in range(per_part):
            n = h * per_part + k
            xsend(n).wait_recv()
            finish(n)
            at_copy(n).start()

    def project_part(h):
        for k in range(per_part):
            n = h * per_part + k
            at_copy(n).wait_recv()
            for hd in range(heads):
                cols = [att[n * 2 + c, pl.ds(hd, quarter, stride=heads), :] for c in range(2)]
                lhs[k * 2 * quarter:(k + 1) * 2 * quarter, hd * head_dim:(hd + 1) * head_dim] = (
                    jnp.concatenate(cols, axis=0).astype(jnp.bfloat16))

        def tile(t, _):
            if h == 0:
                wo_copy(t).wait()
            res = jnp.dot(lhs[...], wo[t], preferred_element_type=jnp.float32)
            for k in range(per):
                i = h * n_sub + t * per + k
                p_buf[i] = res[:, k * TS:(k + 1) * TS]
                p_copy(i).start()
            if h == 1:
                @pl.when(t % 2 == 1)
                def _():
                    y_tile(early + t // 2)
            return 0
        lax.fori_loop(0, n_tiles, tile, 0)

    def out_cols(i, on_core):
        return pl.ds(pl.multiple_of(on_core * half + (i % n_sub) * TS, TS), TS)

    def out_rows(i, on_chip):
        return pl.ds(pl.multiple_of(on_chip * chip_rows + (i // n_sub) * part_rows, part_rows), part_rows)

    def y_tile(i):
        p_copy(i).wait_recv()
        res = hid[pl.ds(pl.multiple_of((i // n_sub) * part_rows, part_rows), part_rows),
                  pl.ds(pl.multiple_of((i % n_sub) * TS, TS), TS)].astype(jnp.float32)
        y = (res + (p_buf[i] + p_recv[i])).astype(jnp.bfloat16)
        y_send[i] = y.astype(jnp.float32)
        y_ref[out_rows(i, chip), out_cols(i, core)] = y
        yx_copy(i).start()
        yc_copy(i).start()

    def y_from_chip(i):
        yx_copy(i).wait_recv()
        yf_copy(i).start()
        y_ref[out_rows(i, 1 - chip), out_cols(i, core)] = y_chip[i].astype(jnp.bfloat16)
        yc_copy(i).wait_recv()
        y_ref[out_rows(i, chip), out_cols(i, 1 - core)] = y_core[i].astype(jnp.bfloat16)

    def y_from_fwd(i):
        yf_copy(i).wait_recv()
        y_ref[out_rows(i, 1 - chip), out_cols(i, 1 - core)] = y_fwd[i].astype(jnp.bfloat16)

    total = NH * n_sub
    last = (n_blk + 2) // 2
    lax.fori_loop(0, G_FINISH, two_blocks, 0)
    for n in range(NC):
        new_scores(n)
    finish_part(0)
    lax.fori_loop(G_FINISH, G_PROJECT, two_blocks, 0)
    early = last - G_PROJECT + 2
    project_part(0)
    hid_copy.wait()

    def two_blocks_and_tile(g, _):
        two_blocks(g, 0)
        y_tile(g - G_PROJECT)
        return 0
    lax.fori_loop(G_PROJECT, last, two_blocks_and_tile, 0)
    finish_part(1)
    y_tile(early - 2)
    y_tile(early - 1)
    project_part(1)
    early = early + n_tiles // 2

    def step(s, _):
        @pl.when(s + early < total)
        def _():
            y_tile(s + early)

        @pl.when(s < total)
        def _():
            y_from_chip(s)

        @pl.when(s >= 1)
        def _():
            y_from_fwd(s - 1)
        return 0
    lax.fori_loop(0, total + 1, step, 0)

    for t in range(n_q):
        q_copy(t).wait_send()
    for k in range(2 * NC):
        d2d(k).wait_send()
    for n in range(NC):
        xsend(n).wait_send()
        at_copy(n).wait_send()

    def drain(i, _):
        p_copy(i).wait_send()
        yc_copy(i).wait_send()
        yx_copy(i).wait_send()
        yf_copy(i).wait_send()
        return 0
    lax.fori_loop(0, total, drain, 0)


def attention(seq_lens, cos_t, sin_t, norm_w, b_q, b_k, b_v, hidden, w_q, w_k, w_v, k_cache, v_cache, w_o):
    n_rows, d_model = hidden.shape
    s_dev, head_dim = k_cache.shape[1], k_cache.shape[2]
    heads = w_q.shape[1] // head_dim
    half = d_model // 2
    n_tiles = half // TN
    n_q = w_q.shape[1] // (2 * TN)
    quarter = n_rows // (4 * NC)
    msg = quarter * heads + heads
    total = NH * n_tiles * (TN // TS)
    vmem = pl.BlockSpec(memory_space=pltpu.VMEM)
    hbm = pl.BlockSpec(memory_space=pl.ANY)
    f32, bf16 = jnp.float32, jnp.bfloat16
    dma = pltpu.SemaphoreType.DMA
    tile_f32 = pltpu.VMEM((total, n_rows // (2 * NH), TS), f32)
    return pl.pallas_call(
        attn_kernel,
        out_shape=[jax.ShapeDtypeStruct((n_rows, d_model), bf16)] + [jax.ShapeDtypeStruct((n_rows, head_dim), bf16)] * 2,
        in_specs=[pl.BlockSpec(memory_space=pltpu.SMEM)] + [vmem] * 6 + [hbm] * 7,
        out_specs=[vmem] * 3,
        scratch_shapes=[
            pltpu.VMEM((n_rows * heads, head_dim), f32),
            pltpu.VMEM((n_q, n_rows * TN // head_dim, head_dim), f32),
            pltpu.VMEM((n_q, n_rows * TN // head_dim, head_dim), f32),
            pltpu.VMEM((heads, head_dim), f32),
            pltpu.VMEM((n_rows, head_dim), f32), pltpu.VMEM((n_rows, head_dim), f32),
            dma((n_rows // NORM_ROWS,)), dma((4,)), dma((n_q,)), dma((n_q,)),
            pltpu.VMEM((NC * 4, msg, head_dim), f32),
            pltpu.VMEM((NC * 2, msg, head_dim), f32),
            pltpu.VMEM((NC, msg, head_dim), f32),
            pltpu.VMEM((NC * 2, quarter * heads, head_dim), f32),
            pltpu.VMEM((n_rows // (2 * NH), heads * head_dim), bf16),
            pltpu.VMEM((2, BR // 2, 2 * heads, s_dev), f32),
            pltpu.VMEM((2, BR // 2, 2 * heads, s_dev), bf16),
            pltpu.VMEM((NC, heads, head_dim), f32),
            tile_f32, tile_f32, tile_f32, tile_f32, tile_f32, tile_f32,
            pltpu.VMEM((n_tiles, heads * head_dim, TN), bf16),
            pltpu.VMEM((n_rows // 2, half), bf16),
            pltpu.VMEM((NBK, BR, s_dev, head_dim), bf16),
            pltpu.VMEM((NBV, BR, s_dev, head_dim), bf16),
            dma((NBK,)), dma((NBV,)), dma((n_tiles,)), dma,
            dma((NC * 2,)), dma((NC * 2,)), dma((NC,)), dma((NC,)), dma((NC,)), dma((NC,)),
            dma((total,)), dma((total,)), dma((total,)), dma((total,)), dma((total,)), dma((total,)),
            dma((total,)), dma((total,)),
        ],
        compiler_params=pltpu.CompilerParams(
            collective_id=0, has_side_effects=True, vmem_limit_bytes=VMEM_LIMIT),
        name="attend",
    )(seq_lens, cos_t, sin_t, norm_w.reshape(-1, 128), b_q.reshape(heads, head_dim), b_k[None], b_v[None], hidden,
      w_q, w_k, w_v, k_cache, v_cache, w_o)


def copy_kernel(parts, y_in, k_in, v_in, y_out, k_out, v_out, buf, kv_buf, in_sem, out_sem):
    rows = y_in.shape[0] // parts
    pairs = [(y_in.at[pl.ds(p * rows, rows)], buf.at[p], y_out.at[pl.ds(p * rows, rows)]) for p in range(parts)]
    pairs += [(k_in, kv_buf.at[0], k_out), (v_in, kv_buf.at[1], v_out)]
    loads = [pltpu.make_async_copy(a, m, in_sem.at[i]) for i, (a, m, _) in enumerate(pairs)]
    stores = [pltpu.make_async_copy(m, z, out_sem.at[i]) for i, (_, m, z) in enumerate(pairs)]
    for c in loads:
        c.start()
    for c, d in zip(loads, stores):
        c.wait()
        d.start()
    for d in stores:
        d.wait()


def copy_out(y, k, v):
    parts = 8
    hbm = pl.BlockSpec(memory_space=pl.ANY)
    dma = pltpu.SemaphoreType.DMA
    return pl.pallas_call(
        functools.partial(copy_kernel, parts),
        out_shape=[jax.ShapeDtypeStruct(a.shape, a.dtype) for a in (y, k, v)],
        in_specs=[hbm] * 3, out_specs=[hbm] * 3,
        scratch_shapes=[pltpu.VMEM((parts, y.shape[0] // parts, y.shape[1]), y.dtype),
                        pltpu.VMEM((2,) + k.shape, k.dtype), dma((parts + 2,)), dma((parts + 2,))],
        name="copy_out",
    )(y, k, v)


def solution(mesh):
    def device_step(hidden, norm_w, w_q, b_q, w_k, b_k, w_v, b_v, w_o, k_cache, v_cache, positions, seq_lens):
        n_rows = hidden.shape[0]
        s_dev, head_dim = k_cache.shape[1], k_cache.shape[3]
        cos_t, sin_t = rope_tables(positions, head_dim)
        outs = attention(seq_lens, cos_t, sin_t, norm_w, b_q, b_k, b_v, hidden, w_q, w_k, w_v,
                         k_cache.reshape(n_rows, s_dev, head_dim), v_cache.reshape(n_rows, s_dev, head_dim), w_o)
        y_out, kb, vb = copy_out(*outs)
        return y_out, kb.reshape(n_rows, 1, head_dim), vb.reshape(n_rows, 1, head_dim)

    col_spec = P(None, 'tp')
    vec_spec = P('tp')
    cache_spec = P('dp', 'sp', 'tp', None)
    group_spec = P('dp', 'tp', None)
    in_specs = (P('dp', None), P(None), col_spec, vec_spec, col_spec, vec_spec, col_spec, vec_spec,
                P('tp', None), cache_spec, cache_spec, P('dp'), P('dp'))
    out_specs = (P('dp', None), group_spec, group_spec)
    return jax.shard_map(device_step, mesh=mesh, in_specs=in_specs, out_specs=out_specs, check_vma=False)
```

```python
import functools

import jax
import jax.numpy as jnp
from jax import lax
from jax.experimental import pallas as pl
from jax.experimental.pallas import tpu as pltpu
from jax.sharding import PartitionSpec as P

RMS_EPS = 1.5625e-7
ROPE_BASE = 10000.0
LOG2E = 1.4426950408889634
NEG = -3e38
NEG_FLOOR = -1e38
MESH = pl.DeviceIdType.MESH
VMEM_LIMIT = 67_043_328


WO_FROM = 12
NORM_ROWS = 32
NC = 4
NH = 2
BR = 8
NBK, NBV = 6, 7
TN = 512
TS = 256
G_FINISH, G_PROJECT = 12, 13


def rope_tables(positions, head_dim):
    rot_dim = head_dim // 2
    lane = jnp.arange(head_dim, dtype=jnp.int32)
    freq = ROPE_BASE ** (-2.0 * (lane // 2).astype(jnp.float32) / rot_dim)
    freq = jnp.where(lane < rot_dim, freq, 0.0)
    angles = positions.astype(jnp.float32)[:, None] * freq
    sign = jnp.where(lane % 2 == 0, -1.0, 1.0)
    return jnp.cos(angles), jnp.sin(angles) * sign


def rope(x, cos_t, sin_t, even):
    width = x.shape[-1]
    swapped = jnp.where(even, pltpu.roll(x, width - 1, 1), pltpu.roll(x, 1, 1))
    return (x * cos_t + swapped * sin_t).astype(jnp.bfloat16).astype(jnp.float32)


def attn_kernel(seq_ref, cos_ref, sin_ref, nw_ref, bq_ref, bk_ref, bv_ref, hid_hbm, wq_hbm, wk_hbm, wv_hbm,
                k_hbm, v_hbm, wo_hbm, y_out, kb_ref, vb_ref,
                y_ref, yo_sem, q_ref, q_send, q_recv, bqf, kf_ref, vf_ref, in_sem, wkv_sem, q_s, q_r, o_buf, rd, rx, att, lhs, s_sc, p_sc, new_sc, p_buf, p_recv, y_send, y_core, y_chip, y_fwd, wo, hid,
                kbuf, vbuf, k_sem, v_sem, wo_sem, hid_sem, rd_s, rd_r, rx_s, rx_r, at_s, at_r, p_s, p_r,
                yc_s, yc_r, yx_s, yx_r, yf_s, yf_r):
    n_rows, d_model = y_ref.shape
    s_dev, head_dim = kbuf.shape[2], kbuf.shape[3]
    heads = q_ref.shape[0] // n_rows
    n_tiles = wo.shape[0]
    half = n_tiles * TN
    quarter = n_rows // (4 * NC)
    o_rows = quarter * heads
    chip_rows = n_rows // 2
    bq = quarter // BR
    n_blk = n_rows // BR
    coef = head_dim ** -0.5 * LOG2E

    dp, tp, sp = lax.axis_index("dp"), lax.axis_index("tp"), lax.axis_index("sp")
    chip, core = sp // 2, sp % 2
    to_core = (dp, tp, 2 * chip + (1 - core))
    to_chip = (dp, tp, 2 * (1 - chip) + core)
    to_tp = (dp, 1 - tp, sp)

    def remote(src, dst, s_sem, r_sem, dev):
        return pltpu.make_async_remote_copy(src_ref=src, dst_ref=dst, send_sem=s_sem, recv_sem=r_sem,
                                            device_id=dev, device_id_type=MESH)

    per_part = NC // NH
    part_rows = chip_rows // NH

    def group_piece(u):
        return (u // (4 * per_part)) * per_part + (u % (2 * per_part)) // 2

    def group_far(u):
        return u % (4 * per_part) < 2 * per_part

    def group_row(u):
        near = (u % (4 * per_part)) // (2 * per_part)
        own = u % 2
        on_chip = near * chip + (1 - near) * (1 - chip)
        on_core = own * core + (1 - own) * (1 - core)
        return on_chip * chip_rows + group_piece(u) * 2 * quarter + on_core * quarter

    def kept_group(n, near):
        return (n // per_part) * 4 * per_part + near * 2 * per_part + 2 * (n % per_part) + 1

    def block_row(b):
        return pl.multiple_of(group_row(b // bq) + (b % bq) * BR, BR)

    def k_copy(b):
        return pltpu.make_async_copy(k_hbm.at[pl.ds(block_row(b), BR)], kbuf.at[b % NBK], k_sem.at[b % NBK])

    def v_copy(b):
        return pltpu.make_async_copy(v_hbm.at[pl.ds(block_row(b), BR)], vbuf.at[b % NBV], v_sem.at[b % NBV])

    def wo_copy(t):
        cols = pl.ds(pl.multiple_of(core * half + t * TN, 128), TN)
        return pltpu.make_async_copy(wo_hbm.at[:, cols], wo.at[t], wo_sem.at[t])

    hid_copy = pltpu.make_async_copy(
        hid_hbm.at[pl.ds(pl.multiple_of(chip * chip_rows, 128), chip_rows),
                   pl.ds(pl.multiple_of(core * half, 128), half)], hid, hid_sem)

    n_q = q_send.shape[0]
    tile_heads = TN // head_dim
    k_half = wo.shape[1]

    def in_copy(i):
        rows = pl.ds(pl.multiple_of(i * NORM_ROWS, NORM_ROWS), NORM_ROWS)
        return pltpu.make_async_copy(hid_hbm.at[rows], y_ref.at[rows], in_sem.at[i])


    def wkv_copies():
        parts = [(w, r) for r in range(2) for w in (wk_hbm, wv_hbm)]
        return [pltpu.make_async_copy(w.at[pl.ds(r * k_half, k_half)],
                                      wo.at[0, :, i * head_dim:(i + 1) * head_dim], wkv_sem.at[i])
                for i, (w, r) in enumerate(parts)]

    def wq_copy(i):
        cols = pl.ds(pl.multiple_of((core * n_q + i // 2) * TN, TN), TN)
        return pltpu.make_async_copy(wq_hbm.at[pl.ds((i % 2) * k_half, k_half), cols], wo.at[i], wo_sem.at[i])

    n_norm = n_rows // NORM_ROWS
    for i in range(n_norm):
        in_copy(i).start()

    barrier = pltpu.get_barrier_semaphore()
    for dev in (to_core, to_chip, to_tp):
        pl.semaphore_signal(barrier, inc=1, device_id=dev, device_id_type=MESH)

    bqf[...] = bq_ref[...].astype(jnp.float32)

    def norm_rows(i, _):
        rows = pl.ds(pl.multiple_of(i * NORM_ROWS, NORM_ROWS), NORM_ROWS)
        in_copy(i).wait()

        @pl.when(i < 2 * n_q)
        def _():
            wq_copy(i).start()
        sq = jnp.zeros((NORM_ROWS, 128), jnp.float32)
        for c in range(d_model // 128):
            x = y_ref[rows, c * 128:(c + 1) * 128].astype(jnp.float32)
            sq = sq + x * x
        inv = lax.rsqrt(jnp.sum(sq, axis=-1, keepdims=True) / d_model + RMS_EPS)
        for c in range(d_model // 128):
            x = y_ref[rows, c * 128:(c + 1) * 128].astype(jnp.float32)
            x = x * inv * nw_ref[c:c + 1, :].astype(jnp.float32)
            y_ref[rows, c * 128:(c + 1) * 128] = x.astype(jnp.bfloat16)
        return 0
    lax.fori_loop(0, n_norm, norm_rows, 0)
    pl.semaphore_wait(barrier, 3)

    even = lax.broadcasted_iota(jnp.int32, (n_rows, head_dim), 1) % 2 == 0

    def round_f32(x):
        return x.astype(jnp.bfloat16).astype(jnp.float32)

    def q_copy(t):
        return remote(q_send.at[t], q_recv.at[t], q_s.at[t], q_r.at[t], to_core)

    def q_tile(t, _):
        wq_copy(2 * t).wait()
        wq_copy(2 * t + 1).wait()

        @pl.when(t == n_q - 1)
        def _():
            for b in range(NBV):
                if b < NBK:
                    k_copy(b).start()
                v_copy(b).start()
        acc = jnp.dot(y_ref[:, :k_half], wo[2 * t], preferred_element_type=jnp.float32)
        acc = acc + jnp.dot(y_ref[:, k_half:], wo[2 * t + 1], preferred_element_type=jnp.float32)
        for h in range(tile_heads):
            head = core * (heads // 2) + t * tile_heads + h
            val = round_f32(acc[:, h * head_dim:(h + 1) * head_dim] + bqf[pl.ds(head, 1), :])
            val = rope(val, cos_ref[...], sin_ref[...], even)
            q_ref[pl.ds(head, n_rows, stride=heads), :] = val
            q_send[t, pl.ds(h, n_rows, stride=tile_heads), :] = val
        q_copy(t).start()

        @pl.when(t == 0)
        def _():
            for c in wkv_copies():
                c.start()
        return 0
    lax.fori_loop(0, n_q, q_tile, 0)

    for c in wkv_copies():
        c.wait()
    kv = jnp.dot(y_ref[:, :k_half], wo[0, :, :2 * head_dim], preferred_element_type=jnp.float32)
    kv = kv + jnp.dot(y_ref[:, k_half:], wo[0, :, 2 * head_dim:], preferred_element_type=jnp.float32)
    k_rot = rope(round_f32(kv[:, :head_dim] + bk_ref[...].astype(jnp.float32)), cos_ref[...], sin_ref[...], even)
    kf_ref[...] = k_rot
    kb_ref[...] = k_rot.astype(jnp.bfloat16)
    v_val = round_f32(kv[:, head_dim:] + bv_ref[...].astype(jnp.float32))
    vf_ref[...] = v_val
    vb_ref[...] = v_val.astype(jnp.bfloat16)

    def q_take(t, _):
        q_copy(t).wait_recv()
        for h in range(tile_heads):
            head = (1 - core) * (heads // 2) + t * tile_heads + h
            q_ref[pl.ds(head, n_rows, stride=heads), :] = q_recv[t, pl.ds(h, n_rows, stride=tile_heads), :]
        return 0
    lax.fori_loop(0, n_q, q_take, 0)

    lane = lax.broadcasted_iota(jnp.int32, (heads, head_dim), 1)
    pos = lax.broadcasted_iota(jnp.int32, (heads, s_dev), 1) + sp * s_dev
    zeros_q = jnp.zeros((heads, head_dim), jnp.float32)

    def q_rows(row):
        return q_ref[pl.ds(pl.multiple_of(row * heads, 8), heads), :]

    def new_scores(n):
        row0 = chip * chip_rows + n * 2 * quarter + core * quarter

        def rows8(g, acc):
            base = pl.multiple_of(row0 + g * 8, 8)
            k_new = kf_ref[pl.ds(base, 8), :]
            for r in range(8):
                s_new = jnp.sum(q_rows(base + r) * k_new[r:r + 1], axis=-1, keepdims=True)
                acc = jnp.where(lane == g * 8 + r, s_new, acc)
            return acc
        new_sc[n] = lax.fori_loop(0, quarter // 8, rows8, zeros_q)

    def column(vals, j):
        return jnp.broadcast_to(vals[:, j:j + 1], (heads, head_dim))

    def d2d(k):
        return remote(o_buf.at[2 * k], rd.at[k], rd_s.at[k], rd_r.at[k], to_core)

    def xsend(n):
        return remote(o_buf.at[kept_group(n, 0)], rx.at[n], rx_s.at[n], rx_r.at[n], to_chip)

    def at_copy(n):
        return remote(att.at[n * 2 + core], att.at[n * 2 + core], at_s.at[n], at_r.at[n], to_core)

    def merge_core(u):
        k = u // 2
        st1 = o_buf[u, o_rows:o_rows + heads, :]
        st2 = rd[k, o_rows:o_rows + heads, :]
        m = jnp.maximum(st1, st2)
        f1 = jnp.exp2((st1 - m) * coef)
        f2 = jnp.exp2((st2 - m) * coef)
        l = st1 * pltpu.roll(f1, quarter, 1) + st2 * pltpu.roll(f2, quarter, 1)
        o_buf[u, o_rows:o_rows + heads, :] = jnp.where(lane < quarter, m, l)

        for j in range(quarter):
            rows = pl.ds(j * heads, heads)
            o_buf[u, rows, :] = o_buf[u, rows, :] * column(f1, j) + rd[k, rows, :] * column(f2, j)

    def finish(n):
        u = kept_group(n, 1)
        row0 = chip * chip_rows + n * 2 * quarter + core * quarter
        st1 = o_buf[u, o_rows:o_rows + heads, :]
        st2 = rx[n, o_rows:o_rows + heads, :]
        m3 = new_sc[n]
        m = jnp.maximum(jnp.maximum(st1, st2), m3)
        f1 = jnp.exp2((st1 - m) * coef)
        f2 = jnp.exp2((st2 - m) * coef)
        f3 = jnp.exp2((m3 - m) * coef)
        l = st1 * pltpu.roll(f1, quarter, 1) + st2 * pltpu.roll(f2, quarter, 1) + pltpu.roll(f3, quarter, 1)
        l = pltpu.roll(l, head_dim - quarter, 1)
        f1, f2, f3 = f1 / l, f2 / l, f3 / l

        for j in range(quarter):
            if j % 8 == 0:
                v_new = vf_ref[pl.ds(pl.multiple_of(row0 + j, 8), 8), :]
            rows = pl.ds(j * heads, heads)
            o = o_buf[u, rows, :] * column(f1, j) + rx[n, rows, :] * column(f2, j)
            o = o + column(f3, j) * v_new[j % 8:j % 8 + 1]
            att[n * 2 + core, rows, :] = round_f32(o)

    def block(b, new, old):
        @pl.when(b < n_blk)
        def _():
            k_copy(b).wait()

        b1 = jnp.minimum(b, n_blk - 1)
        b2 = jnp.clip(b - 1, 0, n_blk - 1)
        b3 = jnp.clip(b - 2, 0, n_blk - 1)

        @pl.when(jnp.logical_or(b == 0, b >= 3))
        def _():
            v_copy(b3).wait()

        u2, row2 = b2 // bq, block_row(b2)
        stats = o_buf[u2, o_rows:o_rows + heads, :]
        for pair in range(BR // 2):
            p_list = []
            for i in range(2):
                r = 2 * pair + i
                s = s_sc[old, pair, i * heads:(i + 1) * heads, :]
                s = jnp.where(pos < seq_ref[row2 + r], s, NEG)
                m = jnp.maximum(jnp.max(s, axis=-1, keepdims=True), NEG_FLOOR)
                p = jnp.exp2((s - m) * coef)
                l = jnp.sum(p, axis=-1, keepdims=True)
                j = (b2 % bq) * BR + r
                stats = jnp.where(lane == j, m, jnp.where(lane == quarter + j, l, stats))
                p_list.append(p)
            p_sc[new, pair] = jnp.concatenate(p_list, axis=0).astype(jnp.bfloat16)
        o_buf[u2, o_rows:o_rows + heads, :] = stats
        row1, kslot = block_row(b1), b1 % NBK
        for pair in range(BR // 2):
            r = 2 * pair
            left = jnp.concatenate([q_rows(row1 + r), zeros_q], axis=0)
            right = jnp.concatenate([zeros_q, q_rows(row1 + r + 1)], axis=0)
            q_pair = jnp.concatenate([left, right], axis=1).astype(jnp.bfloat16)
            k_pair = jnp.concatenate([kbuf[kslot, r], kbuf[kslot, r + 1]], axis=1)
            s_sc[new, pair] = lax.dot_general(q_pair, k_pair, (((1,), (1,)), ((), ())),
                                         preferred_element_type=jnp.float32)
        u3, vslot = b3 // bq, b3 % NBV
        for pair in range(BR // 2):
            r = 2 * pair
            v_pair = jnp.concatenate([vbuf[vslot, r], vbuf[vslot, r + 1]], axis=1)
            o_pair = jnp.dot(p_sc[old, pair], v_pair, preferred_element_type=jnp.float32)
            for i in range(2):
                o = o_pair[i * heads:(i + 1) * heads, i * head_dim:(i + 1) * head_dim]
                o_buf[u3, pl.ds(pl.multiple_of(((b3 % bq) * BR + r + i) * heads, 8), heads), :] = o

        @pl.when(b + NBK < n_blk)
        def _():
            k_copy(b + NBK).start()

        @pl.when(jnp.logical_and(b >= 2, b - 2 + NBV < n_blk))
        def _():
            v_copy(b - 2 + NBV).start()

        w = b - WO_FROM

        @pl.when(jnp.logical_and(w >= 0, jnp.logical_and(w % 2 == 0, w < 2 * n_tiles)))
        def _():
            wo_copy(w // 2).start()

        @pl.when(w == 0)
        def _():
            hid_copy.start()

        done = jnp.logical_and(b >= 2, (b - 2) % bq == bq - 1)
        u = b3 // bq

        @pl.when(jnp.logical_and(done, u % 2 == 0))
        def _():
            d2d(u // 2).start()

        @pl.when(jnp.logical_and(done, u % 2 == 1))
        def _():
            d2d(u // 2).wait_recv()
            merge_core(u)

            @pl.when(group_far(u))
            def _():
                xsend(group_piece(u)).start()

    def two_blocks(g, _):
        block(2 * g, 0, 1)
        block(2 * g + 1, 1, 0)
        return 0

    def p_copy(i):
        return remote(p_buf.at[i], p_recv.at[i], p_s.at[i], p_r.at[i], to_tp)

    def yc_copy(i):
        return remote(y_send.at[i], y_core.at[i], yc_s.at[i], yc_r.at[i], to_core)

    def yx_copy(i):
        return remote(y_send.at[i], y_chip.at[i], yx_s.at[i], yx_r.at[i], to_chip)

    def yf_copy(i):
        return remote(y_chip.at[i], y_fwd.at[i], yf_s.at[i], yf_r.at[i], to_core)

    per = TN // TS
    n_sub = n_tiles * per

    def finish_part(h):
        for k in range(per_part):
            n = h * per_part + k
            xsend(n).wait_recv()
            finish(n)
            at_copy(n).start()

    def project_part(h):
        for k in range(per_part):
            n = h * per_part + k
            at_copy(n).wait_recv()
            for hd in range(heads):
                cols = [att[n * 2 + c, pl.ds(hd, quarter, stride=heads), :] for c in range(2)]
                lhs[k * 2 * quarter:(k + 1) * 2 * quarter, hd * head_dim:(hd + 1) * head_dim] = (
                    jnp.concatenate(cols, axis=0).astype(jnp.bfloat16))

        def tile(t, _):
            if h == 0:
                wo_copy(t).wait()
            res = jnp.dot(lhs[...], wo[t], preferred_element_type=jnp.float32)
            for k in range(per):
                i = h * n_sub + t * per + k
                p_buf[i] = res[:, k * TS:(k + 1) * TS]
                p_copy(i).start()
            if h == 1:
                @pl.when(t % 2 == 1)
                def _():
                    y_tile(early + t // 2)
            return 0
        lax.fori_loop(0, n_tiles, tile, 0)

    def out_cols(i, on_core):
        return pl.ds(pl.multiple_of(on_core * half + (i % n_sub) * TS, TS), TS)

    def out_rows(i, on_chip):
        return pl.ds(pl.multiple_of(on_chip * chip_rows + (i // n_sub) * part_rows, part_rows), part_rows)

    def out_copy(i, kind):
        rows, cols = out_rows(i, (chip, 1 - chip)[kind % 2]), out_cols(i, (core, 1 - core)[kind // 2])
        return pltpu.make_async_copy(y_ref.at[rows, cols], y_out.at[rows, cols], yo_sem.at[kind, i])

    def y_tile(i):
        p_copy(i).wait_recv()
        res = hid[pl.ds(pl.multiple_of((i // n_sub) * part_rows, part_rows), part_rows),
                  pl.ds(pl.multiple_of((i % n_sub) * TS, TS), TS)].astype(jnp.float32)
        y = (res + (p_buf[i] + p_recv[i])).astype(jnp.bfloat16)
        y_send[i] = y.astype(jnp.float32)
        y_ref[out_rows(i, chip), out_cols(i, core)] = y
        yx_copy(i).start()
        yc_copy(i).start()
        out_copy(i, 0).start()

    def y_from_chip(i):
        yx_copy(i).wait_recv()
        yf_copy(i).start()
        y_ref[out_rows(i, 1 - chip), out_cols(i, core)] = y_chip[i].astype(jnp.bfloat16)
        out_copy(i, 1).start()
        yc_copy(i).wait_recv()
        y_ref[out_rows(i, chip), out_cols(i, 1 - core)] = y_core[i].astype(jnp.bfloat16)
        out_copy(i, 2).start()

    def y_from_fwd(i):
        yf_copy(i).wait_recv()
        y_ref[out_rows(i, 1 - chip), out_cols(i, 1 - core)] = y_fwd[i].astype(jnp.bfloat16)
        out_copy(i, 3).start()

    total = NH * n_sub
    last = (n_blk + 2) // 2
    lax.fori_loop(0, G_FINISH, two_blocks, 0)
    for n in range(NC):
        new_scores(n)
    finish_part(0)
    lax.fori_loop(G_FINISH, G_PROJECT, two_blocks, 0)
    early = last - G_PROJECT + 2
    project_part(0)
    hid_copy.wait()

    def two_blocks_and_tile(g, _):
        two_blocks(g, 0)
        y_tile(g - G_PROJECT)
        return 0
    lax.fori_loop(G_PROJECT, last, two_blocks_and_tile, 0)
    finish_part(1)
    y_tile(early - 2)
    y_tile(early - 1)
    project_part(1)
    early = early + n_tiles // 2

    def step(s, _):
        @pl.when(s + early < total)
        def _():
            y_tile(s + early)

        @pl.when(s < total)
        def _():
            y_from_chip(s)

        @pl.when(s >= 1)
        def _():
            y_from_fwd(s - 1)
        return 0
    lax.fori_loop(0, total + 1, step, 0)

    for t in range(n_q):
        q_copy(t).wait_send()
    for k in range(2 * NC):
        d2d(k).wait_send()
    for n in range(NC):
        xsend(n).wait_send()
        at_copy(n).wait_send()

    def drain(i, _):
        p_copy(i).wait_send()
        yc_copy(i).wait_send()
        yx_copy(i).wait_send()
        yf_copy(i).wait_send()
        for kind in range(4):
            out_copy(i, kind).wait()
        return 0
    lax.fori_loop(0, total, drain, 0)


def attention(seq_lens, cos_t, sin_t, norm_w, b_q, b_k, b_v, hidden, w_q, w_k, w_v, k_cache, v_cache, w_o):
    n_rows, d_model = hidden.shape
    s_dev, head_dim = k_cache.shape[1], k_cache.shape[2]
    heads = w_q.shape[1] // head_dim
    half = d_model // 2
    n_tiles = half // TN
    n_q = w_q.shape[1] // (2 * TN)
    quarter = n_rows // (4 * NC)
    msg = quarter * heads + heads
    total = NH * n_tiles * (TN // TS)
    vmem = pl.BlockSpec(memory_space=pltpu.VMEM)
    hbm = pl.BlockSpec(memory_space=pl.ANY)
    f32, bf16 = jnp.float32, jnp.bfloat16
    dma = pltpu.SemaphoreType.DMA
    tile_f32 = pltpu.VMEM((total, n_rows // (2 * NH), TS), f32)
    return pl.pallas_call(
        attn_kernel,
        out_shape=[jax.ShapeDtypeStruct((n_rows, d_model), bf16)] + [jax.ShapeDtypeStruct((n_rows, head_dim), bf16)] * 2,
        in_specs=[pl.BlockSpec(memory_space=pltpu.SMEM)] + [vmem] * 6 + [hbm] * 7,
        out_specs=[hbm, vmem, vmem],
        scratch_shapes=[
            pltpu.VMEM((n_rows, d_model), bf16), dma((4, total)),
            pltpu.VMEM((n_rows * heads, head_dim), f32),
            pltpu.VMEM((n_q, n_rows * TN // head_dim, head_dim), f32),
            pltpu.VMEM((n_q, n_rows * TN // head_dim, head_dim), f32),
            pltpu.VMEM((heads, head_dim), f32),
            pltpu.VMEM((n_rows, head_dim), f32), pltpu.VMEM((n_rows, head_dim), f32),
            dma((n_rows // NORM_ROWS,)), dma((4,)), dma((n_q,)), dma((n_q,)),
            pltpu.VMEM((NC * 4, msg, head_dim), f32),
            pltpu.VMEM((NC * 2, msg, head_dim), f32),
            pltpu.VMEM((NC, msg, head_dim), f32),
            pltpu.VMEM((NC * 2, quarter * heads, head_dim), f32),
            pltpu.VMEM((n_rows // (2 * NH), heads * head_dim), bf16),
            pltpu.VMEM((2, BR // 2, 2 * heads, s_dev), f32),
            pltpu.VMEM((2, BR // 2, 2 * heads, s_dev), bf16),
            pltpu.VMEM((NC, heads, head_dim), f32),
            tile_f32, tile_f32, tile_f32, tile_f32, tile_f32, tile_f32,
            pltpu.VMEM((n_tiles, heads * head_dim, TN), bf16),
            pltpu.VMEM((n_rows // 2, half), bf16),
            pltpu.VMEM((NBK, BR, s_dev, head_dim), bf16),
            pltpu.VMEM((NBV, BR, s_dev, head_dim), bf16),
            dma((NBK,)), dma((NBV,)), dma((n_tiles,)), dma,
            dma((NC * 2,)), dma((NC * 2,)), dma((NC,)), dma((NC,)), dma((NC,)), dma((NC,)),
            dma((total,)), dma((total,)), dma((total,)), dma((total,)), dma((total,)), dma((total,)),
            dma((total,)), dma((total,)),
        ],
        compiler_params=pltpu.CompilerParams(
            collective_id=0, has_side_effects=True, vmem_limit_bytes=VMEM_LIMIT),
        name="attend",
    )(seq_lens, cos_t, sin_t, norm_w.reshape(-1, 128), b_q.reshape(heads, head_dim), b_k[None], b_v[None], hidden,
      w_q, w_k, w_v, k_cache, v_cache, w_o)


def copy_kernel(parts, y_in, k_in, v_in, y_out, k_out, v_out, buf, kv_buf, in_sem, out_sem):
    rows = y_in.shape[0] // parts
    pairs = [(y_in.at[pl.ds(p * rows, rows)], buf.at[p], y_out.at[pl.ds(p * rows, rows)]) for p in range(parts)]
    pairs += [(k_in, kv_buf.at[0], k_out), (v_in, kv_buf.at[1], v_out)]
    loads = [pltpu.make_async_copy(a, m, in_sem.at[i]) for i, (a, m, _) in enumerate(pairs)]
    stores = [pltpu.make_async_copy(m, z, out_sem.at[i]) for i, (_, m, z) in enumerate(pairs)]
    for c in loads:
        c.start()
    for c, d in zip(loads, stores):
        c.wait()
        d.start()
    for d in stores:
        d.wait()


def copy_out(y, k, v):
    parts = 8
    hbm = pl.BlockSpec(memory_space=pl.ANY)
    dma = pltpu.SemaphoreType.DMA
    return pl.pallas_call(
        functools.partial(copy_kernel, parts),
        out_shape=[jax.ShapeDtypeStruct(a.shape, a.dtype) for a in (y, k, v)],
        in_specs=[hbm] * 3, out_specs=[hbm] * 3,
        scratch_shapes=[pltpu.VMEM((parts, y.shape[0] // parts, y.shape[1]), y.dtype),
                        pltpu.VMEM((2,) + k.shape, k.dtype), dma((parts + 2,)), dma((parts + 2,))],
        name="copy_out",
    )(y, k, v)


def solution(mesh):
    def device_step(hidden, norm_w, w_q, b_q, w_k, b_k, w_v, b_v, w_o, k_cache, v_cache, positions, seq_lens):
        n_rows = hidden.shape[0]
        s_dev, head_dim = k_cache.shape[1], k_cache.shape[3]
        cos_t, sin_t = rope_tables(positions, head_dim)
        outs = attention(seq_lens, cos_t, sin_t, norm_w, b_q, b_k, b_v, hidden, w_q, w_k, w_v,
                         k_cache.reshape(n_rows, s_dev, head_dim), v_cache.reshape(n_rows, s_dev, head_dim), w_o)
        y_out, kb, vb = copy_out(*outs)
        return y_out, kb.reshape(n_rows, 1, head_dim), vb.reshape(n_rows, 1, head_dim)

    col_spec = P(None, 'tp')
    vec_spec = P('tp')
    cache_spec = P('dp', 'sp', 'tp', None)
    group_spec = P('dp', 'tp', None)
    in_specs = (P('dp', None), P(None), col_spec, vec_spec, col_spec, vec_spec, col_spec, vec_spec,
                P('tp', None), cache_spec, cache_spec, P('dp'), P('dp'))
    out_specs = (P('dp', None), group_spec, group_spec)
    return jax.shard_map(device_step, mesh=mesh, in_specs=in_specs, out_specs=out_specs, check_vma=False)
```

```python
import functools

import jax
import jax.numpy as jnp
from jax import lax
from jax.experimental import pallas as pl
from jax.experimental.pallas import tpu as pltpu
from jax.sharding import PartitionSpec as P

RMS_EPS = 1.5625e-7
ROPE_BASE = 10000.0
LOG2E = 1.4426950408889634
NEG = -3e38
NEG_FLOOR = -1e38
MESH = pl.DeviceIdType.MESH
VMEM_LIMIT = 67_043_328


WO_FROM = 12
NORM_ROWS = 32
NC = 4
NH = 2
BR = 8
NBK, NBV = 6, 8
TN = 512
TS = 256
G_FINISH, G_PROJECT = 12, 13


def rope_tables(positions, head_dim):
    rot_dim = head_dim // 2
    lane = jnp.arange(head_dim, dtype=jnp.int32)
    freq = ROPE_BASE ** (-2.0 * (lane // 2).astype(jnp.float32) / rot_dim)
    freq = jnp.where(lane < rot_dim, freq, 0.0)
    angles = positions.astype(jnp.float32)[:, None] * freq
    sign = jnp.where(lane % 2 == 0, -1.0, 1.0)
    return jnp.cos(angles), jnp.sin(angles) * sign


def rope(x, cos_t, sin_t, even):
    width = x.shape[-1]
    swapped = jnp.where(even, pltpu.roll(x, width - 1, 1), pltpu.roll(x, 1, 1))
    return (x * cos_t + swapped * sin_t).astype(jnp.bfloat16).astype(jnp.float32)


def attn_kernel(seq_ref, cos_ref, sin_ref, nw_ref, bq_ref, bk_ref, bv_ref, hid_hbm, wq_hbm, wk_hbm, wv_hbm,
                k_hbm, v_hbm, wo_hbm, y_out, kb_ref, vb_ref,
                y_ref, yo_sem, q_ref, q_send, q_recv, bqf, kf_ref, vf_ref, in_sem, wkv_sem, q_s, q_r, o_buf, rd, rx, att, lhs, s_sc, p_sc, new_sc, p_buf, p_recv, y_core, y_chip, y_fwd, wo, hid,
                kbuf, vbuf, k_sem, v_sem, wo_sem, hid_sem, rd_s, rd_r, rx_s, rx_r, at_s, at_r, p_s, p_r,
                yc_s, yc_r, yx_s, yx_r, yf_s, yf_r):
    n_rows, d_model = y_ref.shape
    s_dev, head_dim = kbuf.shape[2], kbuf.shape[3]
    heads = q_ref.shape[0] // n_rows
    n_tiles = wo.shape[0]
    half = n_tiles * TN
    quarter = n_rows // (4 * NC)
    o_rows = quarter * heads
    chip_rows = n_rows // 2
    bq = quarter // BR
    n_blk = n_rows // BR
    coef = head_dim ** -0.5 * LOG2E

    dp, tp, sp = lax.axis_index("dp"), lax.axis_index("tp"), lax.axis_index("sp")
    chip, core = sp // 2, sp % 2
    to_core = (dp, tp, 2 * chip + (1 - core))
    to_chip = (dp, tp, 2 * (1 - chip) + core)
    to_tp = (dp, 1 - tp, sp)

    def remote(src, dst, s_sem, r_sem, dev):
        return pltpu.make_async_remote_copy(src_ref=src, dst_ref=dst, send_sem=s_sem, recv_sem=r_sem,
                                            device_id=dev, device_id_type=MESH)

    per_part = NC // NH
    part_rows = chip_rows // NH

    def group_piece(u):
        return (u // (4 * per_part)) * per_part + (u % (2 * per_part)) // 2

    def group_far(u):
        return u % (4 * per_part) < 2 * per_part

    def group_row(u):
        near = (u % (4 * per_part)) // (2 * per_part)
        own = u % 2
        on_chip = near * chip + (1 - near) * (1 - chip)
        on_core = own * core + (1 - own) * (1 - core)
        return on_chip * chip_rows + group_piece(u) * 2 * quarter + on_core * quarter

    def kept_group(n, near):
        return (n // per_part) * 4 * per_part + near * 2 * per_part + 2 * (n % per_part) + 1

    def block_row(b):
        return pl.multiple_of(group_row(b // bq) + (b % bq) * BR, BR)

    def k_copy(b):
        return pltpu.make_async_copy(k_hbm.at[pl.ds(block_row(b), BR)], kbuf.at[b % NBK], k_sem.at[b % NBK])

    def v_copy(b):
        return pltpu.make_async_copy(v_hbm.at[pl.ds(block_row(b), BR)], vbuf.at[b % NBV], v_sem.at[b % NBV])

    def wo_copy(t):
        cols = pl.ds(pl.multiple_of(core * half + t * TN, 128), TN)
        return pltpu.make_async_copy(wo_hbm.at[:, cols], wo.at[t], wo_sem.at[t])

    hid_copy = pltpu.make_async_copy(
        hid_hbm.at[pl.ds(pl.multiple_of(chip * chip_rows, 128), chip_rows),
                   pl.ds(pl.multiple_of(core * half, 128), half)], hid, hid_sem)

    n_q = q_send.shape[0]
    tile_heads = TN // head_dim
    k_half = wo.shape[1]

    def in_copy(i):
        rows = pl.ds(pl.multiple_of(i * NORM_ROWS, NORM_ROWS), NORM_ROWS)
        return pltpu.make_async_copy(hid_hbm.at[rows], y_ref.at[rows], in_sem.at[i])


    def wkv_copies():
        parts = [(w, r) for r in range(2) for w in (wk_hbm, wv_hbm)]
        return [pltpu.make_async_copy(w.at[pl.ds(r * k_half, k_half)],
                                      wo.at[0, :, i * head_dim:(i + 1) * head_dim], wkv_sem.at[i])
                for i, (w, r) in enumerate(parts)]

    def wq_copy(i):
        cols = pl.ds(pl.multiple_of((core * n_q + i // 2) * TN, TN), TN)
        return pltpu.make_async_copy(wq_hbm.at[pl.ds((i % 2) * k_half, k_half), cols], wo.at[i], wo_sem.at[i])

    n_norm = n_rows // NORM_ROWS
    for i in range(n_norm):
        in_copy(i).start()

    barrier = pltpu.get_barrier_semaphore()
    for dev in (to_core, to_chip, to_tp):
        pl.semaphore_signal(barrier, inc=1, device_id=dev, device_id_type=MESH)

    bqf[...] = bq_ref[...].astype(jnp.float32)

    def norm_rows(i, _):
        rows = pl.ds(pl.multiple_of(i * NORM_ROWS, NORM_ROWS), NORM_ROWS)
        in_copy(i).wait()

        @pl.when(i < 2 * n_q)
        def _():
            wq_copy(i).start()
        sq = jnp.zeros((NORM_ROWS, 128), jnp.float32)
        for c in range(d_model // 128):
            x = y_ref[rows, c * 128:(c + 1) * 128].astype(jnp.float32)
            sq = sq + x * x
        inv = lax.rsqrt(jnp.sum(sq, axis=-1, keepdims=True) / d_model + RMS_EPS)
        for c in range(d_model // 128):
            x = y_ref[rows, c * 128:(c + 1) * 128].astype(jnp.float32)
            x = x * inv * nw_ref[c:c + 1, :].astype(jnp.float32)
            y_ref[rows, c * 128:(c + 1) * 128] = x.astype(jnp.bfloat16)
        return 0
    lax.fori_loop(0, n_norm, norm_rows, 0)
    pl.semaphore_wait(barrier, 3)

    even = lax.broadcasted_iota(jnp.int32, (n_rows, head_dim), 1) % 2 == 0

    def round_f32(x):
        return x.astype(jnp.bfloat16).astype(jnp.float32)

    def q_copy(t):
        return remote(q_send.at[t], q_recv.at[t], q_s.at[t], q_r.at[t], to_core)

    def q_tile(t, _):
        wq_copy(2 * t).wait()
        wq_copy(2 * t + 1).wait()

        @pl.when(t == n_q - 1)
        def _():
            for b in range(NBV):
                if b < NBK:
                    k_copy(b).start()
                v_copy(b).start()
        acc = jnp.dot(y_ref[:, :k_half], wo[2 * t], preferred_element_type=jnp.float32)
        acc = acc + jnp.dot(y_ref[:, k_half:], wo[2 * t + 1], preferred_element_type=jnp.float32)
        for h in range(tile_heads):
            head = core * (heads // 2) + t * tile_heads + h
            val = round_f32(acc[:, h * head_dim:(h + 1) * head_dim] + bqf[pl.ds(head, 1), :])
            val = rope(val, cos_ref[...], sin_ref[...], even)
            q_ref[pl.ds(head, n_rows, stride=heads), :] = val
            q_send[t, pl.ds(h, n_rows, stride=tile_heads), :] = val
        q_copy(t).start()

        @pl.when(t == 0)
        def _():
            for c in wkv_copies():
                c.start()
        return 0
    lax.fori_loop(0, n_q, q_tile, 0)

    for c in wkv_copies():
        c.wait()
    kv = jnp.dot(y_ref[:, :k_half], wo[0, :, :2 * head_dim], preferred_element_type=jnp.float32)
    kv = kv + jnp.dot(y_ref[:, k_half:], wo[0, :, 2 * head_dim:], preferred_element_type=jnp.float32)
    k_rot = rope(round_f32(kv[:, :head_dim] + bk_ref[...].astype(jnp.float32)), cos_ref[...], sin_ref[...], even)
    kf_ref[...] = k_rot
    kb_ref[...] = k_rot.astype(jnp.bfloat16)
    v_val = round_f32(kv[:, head_dim:] + bv_ref[...].astype(jnp.float32))
    vf_ref[...] = v_val
    vb_ref[...] = v_val.astype(jnp.bfloat16)

    def q_take(t, _):
        q_copy(t).wait_recv()
        for h in range(tile_heads):
            head = (1 - core) * (heads // 2) + t * tile_heads + h
            q_ref[pl.ds(head, n_rows, stride=heads), :] = q_recv[t, pl.ds(h, n_rows, stride=tile_heads), :]
        return 0
    lax.fori_loop(0, n_q, q_take, 0)

    lane = lax.broadcasted_iota(jnp.int32, (heads, head_dim), 1)
    pos = lax.broadcasted_iota(jnp.int32, (heads, s_dev), 1) + sp * s_dev
    zeros_q = jnp.zeros((heads, head_dim), jnp.float32)

    def q_rows(row):
        return q_ref[pl.ds(pl.multiple_of(row * heads, 8), heads), :]

    def new_scores(n):
        row0 = chip * chip_rows + n * 2 * quarter + core * quarter

        def rows8(g, acc):
            base = pl.multiple_of(row0 + g * 8, 8)
            k_new = kf_ref[pl.ds(base, 8), :]
            for r in range(8):
                s_new = jnp.sum(q_rows(base + r) * k_new[r:r + 1], axis=-1, keepdims=True)
                acc = jnp.where(lane == g * 8 + r, s_new, acc)
            return acc
        new_sc[n] = lax.fori_loop(0, quarter // 8, rows8, zeros_q)

    def column(vals, j):
        return jnp.broadcast_to(vals[:, j:j + 1], (heads, head_dim))

    def d2d(k):
        return remote(o_buf.at[2 * k], rd.at[k], rd_s.at[k], rd_r.at[k], to_core)

    def xsend(n):
        return remote(o_buf.at[kept_group(n, 0)], rx.at[n], rx_s.at[n], rx_r.at[n], to_chip)

    def at_copy(n):
        return remote(att.at[n * 2 + core], att.at[n * 2 + core], at_s.at[n], at_r.at[n], to_core)

    def merge_core(u):
        k = u // 2
        st1 = o_buf[u, o_rows:o_rows + heads, :]
        st2 = rd[k, o_rows:o_rows + heads, :]
        m = jnp.maximum(st1, st2)
        f1 = jnp.exp2((st1 - m) * coef)
        f2 = jnp.exp2((st2 - m) * coef)
        l = st1 * pltpu.roll(f1, quarter, 1) + st2 * pltpu.roll(f2, quarter, 1)
        o_buf[u, o_rows:o_rows + heads, :] = jnp.where(lane < quarter, m, l)

        for j in range(quarter):
            rows = pl.ds(j * heads, heads)
            o_buf[u, rows, :] = o_buf[u, rows, :] * column(f1, j) + rd[k, rows, :] * column(f2, j)

    def finish(n):
        u = kept_group(n, 1)
        row0 = chip * chip_rows + n * 2 * quarter + core * quarter
        st1 = o_buf[u, o_rows:o_rows + heads, :]
        st2 = rx[n, o_rows:o_rows + heads, :]
        m3 = new_sc[n]
        m = jnp.maximum(jnp.maximum(st1, st2), m3)
        f1 = jnp.exp2((st1 - m) * coef)
        f2 = jnp.exp2((st2 - m) * coef)
        f3 = jnp.exp2((m3 - m) * coef)
        l = st1 * pltpu.roll(f1, quarter, 1) + st2 * pltpu.roll(f2, quarter, 1) + pltpu.roll(f3, quarter, 1)
        l = pltpu.roll(l, head_dim - quarter, 1)
        f1, f2, f3 = f1 / l, f2 / l, f3 / l

        for j in range(quarter):
            if j % 8 == 0:
                v_new = vf_ref[pl.ds(pl.multiple_of(row0 + j, 8), 8), :]
            rows = pl.ds(j * heads, heads)
            o = o_buf[u, rows, :] * column(f1, j) + rx[n, rows, :] * column(f2, j)
            o = o + column(f3, j) * v_new[j % 8:j % 8 + 1]
            att[n * 2 + core, rows, :] = round_f32(o)

    def block(b, new, old):
        @pl.when(b < n_blk)
        def _():
            k_copy(b).wait()

        b1 = jnp.minimum(b, n_blk - 1)
        b2 = jnp.clip(b - 1, 0, n_blk - 1)
        b3 = jnp.clip(b - 2, 0, n_blk - 1)

        @pl.when(jnp.logical_or(b == 0, b >= 3))
        def _():
            v_copy(b3).wait()

        u2, row2 = b2 // bq, block_row(b2)
        stats = o_buf[u2, o_rows:o_rows + heads, :]
        for pair in range(BR // 2):
            p_list = []
            for i in range(2):
                r = 2 * pair + i
                s = s_sc[old, pair, i * heads:(i + 1) * heads, :]
                s = jnp.where(pos < seq_ref[row2 + r], s, NEG)
                m = jnp.maximum(jnp.max(s, axis=-1, keepdims=True), NEG_FLOOR)
                p = jnp.exp2((s - m) * coef)
                l = jnp.sum(p, axis=-1, keepdims=True)
                j = (b2 % bq) * BR + r
                stats = jnp.where(lane == j, m, jnp.where(lane == quarter + j, l, stats))
                p_list.append(p)
            p_sc[new, pair] = jnp.concatenate(p_list, axis=0).astype(jnp.bfloat16)
        o_buf[u2, o_rows:o_rows + heads, :] = stats
        row1, kslot = block_row(b1), b1 % NBK
        for pair in range(BR // 2):
            r = 2 * pair
            left = jnp.concatenate([q_rows(row1 + r), zeros_q], axis=0)
            right = jnp.concatenate([zeros_q, q_rows(row1 + r + 1)], axis=0)
            q_pair = jnp.concatenate([left, right], axis=1).astype(jnp.bfloat16)
            k_pair = jnp.concatenate([kbuf[kslot, r], kbuf[kslot, r + 1]], axis=1)
            s_sc[new, pair] = lax.dot_general(q_pair, k_pair, (((1,), (1,)), ((), ())),
                                         preferred_element_type=jnp.float32)
        u3, vslot = b3 // bq, b3 % NBV
        for pair in range(BR // 2):
            r = 2 * pair
            v_pair = jnp.concatenate([vbuf[vslot, r], vbuf[vslot, r + 1]], axis=1)
            o_pair = jnp.dot(p_sc[old, pair], v_pair, preferred_element_type=jnp.float32)
            for i in range(2):
                o = o_pair[i * heads:(i + 1) * heads, i * head_dim:(i + 1) * head_dim]
                o_buf[u3, pl.ds(pl.multiple_of(((b3 % bq) * BR + r + i) * heads, 8), heads), :] = o

        @pl.when(b + NBK < n_blk)
        def _():
            k_copy(b + NBK).start()

        @pl.when(jnp.logical_and(b >= 2, b - 2 + NBV < n_blk))
        def _():
            v_copy(b - 2 + NBV).start()

        w = b - WO_FROM

        @pl.when(jnp.logical_and(w >= 0, jnp.logical_and(w % 2 == 0, w < 2 * n_tiles)))
        def _():
            wo_copy(w // 2).start()

        @pl.when(w == 0)
        def _():
            hid_copy.start()

        done = jnp.logical_and(b >= 2, (b - 2) % bq == bq - 1)
        u = b3 // bq

        @pl.when(jnp.logical_and(done, u % 2 == 0))
        def _():
            d2d(u // 2).start()

        @pl.when(jnp.logical_and(done, u % 2 == 1))
        def _():
            d2d(u // 2).wait_recv()
            merge_core(u)

            @pl.when(group_far(u))
            def _():
                xsend(group_piece(u)).start()

    def two_blocks(g, _):
        block(2 * g, 0, 1)
        block(2 * g + 1, 1, 0)
        return 0

    def p_copy(i):
        return remote(p_buf.at[i], p_recv.at[i], p_s.at[i], p_r.at[i], to_tp)

    def yc_copy(i):
        return remote(p_buf.at[i], y_core.at[i], yc_s.at[i], yc_r.at[i], to_core)

    def yx_copy(i):
        return remote(p_buf.at[i], y_chip.at[i], yx_s.at[i], yx_r.at[i], to_chip)

    def yf_copy(i):
        return remote(y_chip.at[i], y_fwd.at[i], yf_s.at[i], yf_r.at[i], to_core)

    per = TN // TS
    n_sub = n_tiles * per

    def finish_part(h):
        for k in range(per_part):
            n = h * per_part + k
            xsend(n).wait_recv()
            finish(n)
            at_copy(n).start()

    def project_part(h):
        for k in range(per_part):
            n = h * per_part + k
            at_copy(n).wait_recv()
            for hd in range(heads):
                cols = [att[n * 2 + c, pl.ds(hd, quarter, stride=heads), :] for c in range(2)]
                lhs[k * 2 * quarter:(k + 1) * 2 * quarter, hd * head_dim:(hd + 1) * head_dim] = (
                    jnp.concatenate(cols, axis=0).astype(jnp.bfloat16))

        def tile(t, _):
            if h == 0:
                wo_copy(t).wait()
            res = jnp.dot(lhs[...], wo[t], preferred_element_type=jnp.float32)
            for k in range(per):
                i = h * n_sub + t * per + k
                p_buf[i] = res[:, k * TS:(k + 1) * TS]
                p_copy(i).start()
            if h == 1:
                @pl.when(t % 2 == 1)
                def _():
                    y_tile(early + t // 2)
            return 0
        lax.fori_loop(0, n_tiles, tile, 0)

    def out_cols(i, on_core):
        return pl.ds(pl.multiple_of(on_core * half + (i % n_sub) * TS, TS), TS)

    def out_rows(i, on_chip):
        return pl.ds(pl.multiple_of(on_chip * chip_rows + (i // n_sub) * part_rows, part_rows), part_rows)

    def out_copy(i, kind):
        rows, cols = out_rows(i, (chip, 1 - chip)[kind % 2]), out_cols(i, (core, 1 - core)[kind // 2])
        return pltpu.make_async_copy(y_ref.at[rows, cols], y_out.at[rows, cols], yo_sem.at[kind, i])

    def y_tile(i):
        p_copy(i).wait_recv()
        res = hid[pl.ds(pl.multiple_of((i // n_sub) * part_rows, part_rows), part_rows),
                  pl.ds(pl.multiple_of((i % n_sub) * TS, TS), TS)].astype(jnp.float32)
        y = (res + (p_buf[i] + p_recv[i])).astype(jnp.bfloat16)
        p_copy(i).wait_send()
        p_buf[i] = y.astype(jnp.float32)
        y_ref[out_rows(i, chip), out_cols(i, core)] = y
        yx_copy(i).start()
        yc_copy(i).start()
        out_copy(i, 0).start()

    def y_from_chip(i):
        yx_copy(i).wait_recv()
        yf_copy(i).start()
        y_ref[out_rows(i, 1 - chip), out_cols(i, core)] = y_chip[i].astype(jnp.bfloat16)
        out_copy(i, 1).start()
        yc_copy(i).wait_recv()
        y_ref[out_rows(i, chip), out_cols(i, 1 - core)] = y_core[i].astype(jnp.bfloat16)
        out_copy(i, 2).start()

    def y_from_fwd(i):
        yf_copy(i).wait_recv()
        y_ref[out_rows(i, 1 - chip), out_cols(i, 1 - core)] = y_fwd[i].astype(jnp.bfloat16)
        out_copy(i, 3).start()

    total = NH * n_sub
    last = (n_blk + 2) // 2
    lax.fori_loop(0, G_FINISH, two_blocks, 0)
    for n in range(NC):
        new_scores(n)
    finish_part(0)
    lax.fori_loop(G_FINISH, G_PROJECT, two_blocks, 0)
    early = last - G_PROJECT + 2
    project_part(0)
    hid_copy.wait()

    def two_blocks_and_tile(g, _):
        two_blocks(g, 0)
        y_tile(g - G_PROJECT)
        return 0
    lax.fori_loop(G_PROJECT, last, two_blocks_and_tile, 0)
    finish_part(1)
    y_tile(early - 2)
    y_tile(early - 1)
    project_part(1)
    early = early + n_tiles // 2

    def step(s, _):
        @pl.when(s + early < total)
        def _():
            y_tile(s + early)

        @pl.when(s < total)
        def _():
            y_from_chip(s)

        @pl.when(s >= 1)
        def _():
            y_from_fwd(s - 1)
        return 0
    lax.fori_loop(0, total + 1, step, 0)

    for t in range(n_q):
        q_copy(t).wait_send()
    for k in range(2 * NC):
        d2d(k).wait_send()
    for n in range(NC):
        xsend(n).wait_send()
        at_copy(n).wait_send()

    def drain(i, _):
        yc_copy(i).wait_send()
        yx_copy(i).wait_send()
        yf_copy(i).wait_send()
        for kind in range(4):
            out_copy(i, kind).wait()
        return 0
    lax.fori_loop(0, total, drain, 0)


def attention(seq_lens, cos_t, sin_t, norm_w, b_q, b_k, b_v, hidden, w_q, w_k, w_v, k_cache, v_cache, w_o):
    n_rows, d_model = hidden.shape
    s_dev, head_dim = k_cache.shape[1], k_cache.shape[2]
    heads = w_q.shape[1] // head_dim
    half = d_model // 2
    n_tiles = half // TN
    n_q = w_q.shape[1] // (2 * TN)
    quarter = n_rows // (4 * NC)
    msg = quarter * heads + heads
    total = NH * n_tiles * (TN // TS)
    vmem = pl.BlockSpec(memory_space=pltpu.VMEM)
    hbm = pl.BlockSpec(memory_space=pl.ANY)
    f32, bf16 = jnp.float32, jnp.bfloat16
    dma = pltpu.SemaphoreType.DMA
    tile_f32 = pltpu.VMEM((total, n_rows // (2 * NH), TS), f32)
    return pl.pallas_call(
        attn_kernel,
        out_shape=[jax.ShapeDtypeStruct((n_rows, d_model), bf16)] + [jax.ShapeDtypeStruct((n_rows, head_dim), bf16)] * 2,
        in_specs=[pl.BlockSpec(memory_space=pltpu.SMEM)] + [vmem] * 6 + [hbm] * 7,
        out_specs=[hbm, vmem, vmem],
        scratch_shapes=[
            pltpu.VMEM((n_rows, d_model), bf16), dma((4, total)),
            pltpu.VMEM((n_rows * heads, head_dim), f32),
            pltpu.VMEM((n_q, n_rows * TN // head_dim, head_dim), f32),
            pltpu.VMEM((n_q, n_rows * TN // head_dim, head_dim), f32),
            pltpu.VMEM((heads, head_dim), f32),
            pltpu.VMEM((n_rows, head_dim), f32), pltpu.VMEM((n_rows, head_dim), f32),
            dma((n_rows // NORM_ROWS,)), dma((4,)), dma((n_q,)), dma((n_q,)),
            pltpu.VMEM((NC * 4, msg, head_dim), f32),
            pltpu.VMEM((NC * 2, msg, head_dim), f32),
            pltpu.VMEM((NC, msg, head_dim), f32),
            pltpu.VMEM((NC * 2, quarter * heads, head_dim), f32),
            pltpu.VMEM((n_rows // (2 * NH), heads * head_dim), bf16),
            pltpu.VMEM((2, BR // 2, 2 * heads, s_dev), f32),
            pltpu.VMEM((2, BR // 2, 2 * heads, s_dev), bf16),
            pltpu.VMEM((NC, heads, head_dim), f32),
            tile_f32, tile_f32, tile_f32, tile_f32, tile_f32,
            pltpu.VMEM((n_tiles, heads * head_dim, TN), bf16),
            pltpu.VMEM((n_rows // 2, half), bf16),
            pltpu.VMEM((NBK, BR, s_dev, head_dim), bf16),
            pltpu.VMEM((NBV, BR, s_dev, head_dim), bf16),
            dma((NBK,)), dma((NBV,)), dma((n_tiles,)), dma,
            dma((NC * 2,)), dma((NC * 2,)), dma((NC,)), dma((NC,)), dma((NC,)), dma((NC,)),
            dma((total,)), dma((total,)), dma((total,)), dma((total,)), dma((total,)), dma((total,)),
            dma((total,)), dma((total,)),
        ],
        compiler_params=pltpu.CompilerParams(
            collective_id=0, has_side_effects=True, vmem_limit_bytes=VMEM_LIMIT),
        name="attend",
    )(seq_lens, cos_t, sin_t, norm_w.reshape(-1, 128), b_q.reshape(heads, head_dim), b_k[None], b_v[None], hidden,
      w_q, w_k, w_v, k_cache, v_cache, w_o)


def copy_kernel(parts, y_in, k_in, v_in, y_out, k_out, v_out, buf, kv_buf, in_sem, out_sem):
    rows = y_in.shape[0] // parts
    pairs = [(y_in.at[pl.ds(p * rows, rows)], buf.at[p], y_out.at[pl.ds(p * rows, rows)]) for p in range(parts)]
    pairs += [(k_in, kv_buf.at[0], k_out), (v_in, kv_buf.at[1], v_out)]
    loads = [pltpu.make_async_copy(a, m, in_sem.at[i]) for i, (a, m, _) in enumerate(pairs)]
    stores = [pltpu.make_async_copy(m, z, out_sem.at[i]) for i, (_, m, z) in enumerate(pairs)]
    for c in loads:
        c.start()
    for c, d in zip(loads, stores):
        c.wait()
        d.start()
    for d in stores:
        d.wait()


def copy_out(y, k, v):
    parts = 8
    hbm = pl.BlockSpec(memory_space=pl.ANY)
    dma = pltpu.SemaphoreType.DMA
    return pl.pallas_call(
        functools.partial(copy_kernel, parts),
        out_shape=[jax.ShapeDtypeStruct(a.shape, a.dtype) for a in (y, k, v)],
        in_specs=[hbm] * 3, out_specs=[hbm] * 3,
        scratch_shapes=[pltpu.VMEM((parts, y.shape[0] // parts, y.shape[1]), y.dtype),
                        pltpu.VMEM((2,) + k.shape, k.dtype), dma((parts + 2,)), dma((parts + 2,))],
        name="copy_out",
    )(y, k, v)


def solution(mesh):
    def device_step(hidden, norm_w, w_q, b_q, w_k, b_k, w_v, b_v, w_o, k_cache, v_cache, positions, seq_lens):
        n_rows = hidden.shape[0]
        s_dev, head_dim = k_cache.shape[1], k_cache.shape[3]
        cos_t, sin_t = rope_tables(positions, head_dim)
        outs = attention(seq_lens, cos_t, sin_t, norm_w, b_q, b_k, b_v, hidden, w_q, w_k, w_v,
                         k_cache.reshape(n_rows, s_dev, head_dim), v_cache.reshape(n_rows, s_dev, head_dim), w_o)
        y_out, kb, vb = copy_out(*outs)
        return y_out, kb.reshape(n_rows, 1, head_dim), vb.reshape(n_rows, 1, head_dim)

    col_spec = P(None, 'tp')
    vec_spec = P('tp')
    cache_spec = P('dp', 'sp', 'tp', None)
    group_spec = P('dp', 'tp', None)
    in_specs = (P('dp', None), P(None), col_spec, vec_spec, col_spec, vec_spec, col_spec, vec_spec,
                P('tp', None), cache_spec, cache_spec, P('dp'), P('dp'))
    out_specs = (P('dp', None), group_spec, group_spec)
    return jax.shard_map(device_step, mesh=mesh, in_specs=in_specs, out_specs=out_specs, check_vma=False)
```
